64 devices in a mesh: dp: 4 (over x, y), cp: 16 (over z, core).
Axes of the slice: x: 2, y: 2, z: 8, core: 2. Of those that a mesh axis runs over, the one named last changes fastest.
The devices are a block of a 4x4x8 slice.
Arguments:
- x_tok: bfloat16 [128, 5120], P(('dp', 'cp')), parts along dimension 0
- prompt_lens: int32 [128], P('dp'), parts along dimension 0
- k_cache: bfloat16 [128, 1024, 8, 128], P('dp', 'cp'), parts along dimension 0
- v_cache: bfloat16 [128, 1024, 8, 128], P('dp', 'cp'), parts along dimension 0
- norm_gain: bfloat16 [5120], replicated
- w_q: bfloat16 [5120, 5120], replicated
- b_q: bfloat16 [5120], replicated
- w_k: bfloat16 [5120, 1024], replicated
- b_k: bfloat16 [1024], replicated
- w_v: bfloat16 [5120, 1024], replicated
- b_v: bfloat16 [1024], replicated
- w_o: bfloat16 [5120, 5120], replicated
Outputs:
- output 1: bfloat16 [128, 5120], P(('dp', 'cp')), parts along dimension 0
- output 2: bfloat16 [128, 1024, 8, 128], P(('dp', 'cp')), parts along dimension 0
- output 3: bfloat16 [128, 1024, 8, 128], P(('dp', 'cp')), parts along dimension 0
There are 4 independent parts. The reference program is written for one: setup_inputs(seed, part) draws one part's arguments, and reference() takes and returns one part's arrays. A program takes and returns all parts, laid end to end along the dimension named above; an argument that names none is the same for every part.
All inputs are finite; a program needn't handle non-finite values.
Results may differ from the reference program's by a relative error of at most 0.00629694.
Values are sent between devices in bfloat16 or wider.
A program may use at most 768 MiB of HBM per device.

```python
import math
import jax
import jax.numpy as jnp
from jax import lax

D = 5120
HEADS = 40
KV_HEADS = 8
HEAD = 128
BATCH = 32
SEQ = 1024

GROUP = HEADS // KV_HEADS
HALF = HEAD // 2
RMS_EPS = 1e-6
ROPE_THETA = 1000000.0
SCORE_SCALE = HEAD ** -0.5


def normal_draw(draw_key, shape, scale):
    return (jax.random.normal(draw_key, shape, jnp.float32) * scale).astype(jnp.bfloat16)


def setup_inputs(seed: int = 0, part: int = 0) -> dict:
    base_key = jax.random.key(seed)
    part_keys = jax.random.split(jax.random.fold_in(base_key, part), 5)
    weight_keys = jax.random.split(base_key, 8)
    gain = math.sqrt(SEQ) / 4.0
    low_len = SEQ // 16
    prompt_lens = jax.random.randint(part_keys[1], (BATCH,), low_len, SEQ, jnp.int32)
    order = jax.random.permutation(part_keys[2], BATCH)
    prompt_lens = prompt_lens.at[order[0]].set(SEQ - 1).at[order[1]].set(low_len)
    norm_gain = (1.0 + 0.3 * jax.random.normal(weight_keys[0], (D,), jnp.float32)).astype(jnp.bfloat16)
    return {
        'x_tok': normal_draw(part_keys[0], (BATCH, D), 1.0),
        'prompt_lens': prompt_lens,
        'k_cache': normal_draw(part_keys[3], (BATCH, SEQ, KV_HEADS, HEAD), 1.0),
        'v_cache': normal_draw(part_keys[4], (BATCH, SEQ, KV_HEADS, HEAD), 1.0),
        'norm_gain': norm_gain,
        'w_q': normal_draw(weight_keys[1], (D, HEADS * HEAD), D ** -0.5),
        'b_q': normal_draw(weight_keys[2], (HEADS * HEAD,), 0.5),
        'w_k': normal_draw(weight_keys[3], (D, KV_HEADS * HEAD), D ** -0.5),
        'b_k': normal_draw(weight_keys[4], (KV_HEADS * HEAD,), 1.0),
        'w_v': normal_draw(weight_keys[5], (D, KV_HEADS * HEAD), gain * D ** -0.5),
        'b_v': normal_draw(weight_keys[6], (KV_HEADS * HEAD,), 0.5 * gain),
        'w_o': normal_draw(weight_keys[7], (HEADS * HEAD, D), gain * (HEADS * HEAD) ** -0.5),
    }


def rotary(vectors, positions):
    inv_freq = jnp.power(ROPE_THETA, -(jnp.arange(HALF).astype(jnp.float32) * 2.0 / HEAD))
    angle = positions.astype(jnp.float32)[:, None, None] * inv_freq
    cos_t = jnp.cos(angle)
    sin_t = jnp.sin(angle)
    first = vectors[..., :HALF]
    second = vectors[..., HALF:]
    return jnp.concatenate([first * cos_t - second * sin_t, second * cos_t + first * sin_t], axis=-1)


def reference(x_tok, prompt_lens, k_cache, v_cache, norm_gain, w_q, b_q, w_k, b_k, w_v, b_v, w_o):
    x_wide = x_tok.astype(jnp.float32)
    mean_sq = jnp.mean(x_wide * x_wide, axis=-1, keepdims=True)
    normed = (x_wide * lax.rsqrt(mean_sq + RMS_EPS) * norm_gain.astype(jnp.float32)).astype(jnp.bfloat16)
    query = jnp.dot(normed, w_q, preferred_element_type=jnp.float32) + b_q.astype(jnp.float32)
    query = rotary(query.reshape(BATCH, HEADS, HEAD), prompt_lens).astype(jnp.bfloat16)
    key_new = jnp.dot(normed, w_k, preferred_element_type=jnp.float32) + b_k.astype(jnp.float32)
    key_new = rotary(key_new.reshape(BATCH, KV_HEADS, HEAD), prompt_lens).astype(jnp.bfloat16)
    value_new = jnp.dot(normed, w_v, preferred_element_type=jnp.float32) + b_v.astype(jnp.float32)
    value_new = value_new.reshape(BATCH, KV_HEADS, HEAD).astype(jnp.bfloat16)
    slot_idx = jnp.arange(SEQ)

    def one_sequence(operands):
        keys_old, vals_old, query_one, key_one, value_one, length = operands
        before = (slot_idx < length)[:, None, None]
        at_new = (slot_idx == length)[:, None, None]
        keys_all = jnp.where(at_new, key_one[None], jnp.where(before, keys_old, jnp.zeros_like(keys_old)))
        vals_all = jnp.where(at_new, value_one[None], jnp.where(before, vals_old, jnp.zeros_like(vals_old)))
        scores = jnp.einsum('kgd,skd->kgs', query_one.reshape(KV_HEADS, GROUP, HEAD).astype(jnp.float32), keys_all.astype(jnp.float32)) * SCORE_SCALE
        scores = jnp.where(slot_idx <= length, scores, -1e30)
        row_max = jnp.max(scores, axis=-1, keepdims=True)
        weights = jnp.exp(scores - row_max)
        weight_sum = jnp.sum(weights, axis=-1, keepdims=True)
        mixed = jnp.einsum('kgs,skd->kgd', weights.astype(jnp.bfloat16).astype(jnp.float32), vals_all.astype(jnp.float32)) / weight_sum
        return keys_all, vals_all, mixed.reshape(HEADS * HEAD).astype(jnp.bfloat16)

    k_out, v_out, attended = lax.map(one_sequence, (k_cache, v_cache, query, key_new, value_new, prompt_lens))
    y_out = (x_wide + jnp.dot(attended, w_o, preferred_element_type=jnp.float32)).astype(jnp.bfloat16)
    return y_out, k_out, v_out
```

```python
import functools
import math
import jax
import jax.numpy as jnp
from jax import lax
from jax.experimental import pallas as pl
from jax.experimental.pallas import tpu as pltpu
from jax.sharding import PartitionSpec as P

RMS_EPS = 1e-6
ROPE_THETA = 1000000.0
MASKED = -1e30
RING = 8
PACK = 5
TILE = 512
LHS_ROWS = 16
MESH = pl.DeviceIdType.MESH


def decode_kernel(dims, lens_ref, x_ref, gain_ref, bq_ref, bk_ref, bv_ref, k_ref, v_ref, wq_ref, wk_ref, wv_ref, wo_ref,
                  y_ref, k_land, v_land,
                  ring, scores, h_ref, acc, acc_kv, q_raw, q_rot, k_raw, v_raw, o_acc, m_acc, l_acc, o_row,
                  ring_sem, own_sem, send_sem, recv_sem):
    n, rows, span, kv_heads, head_dim, heads = dims
    group = heads // kv_heads
    width = heads * head_dim
    kv_width = kv_heads * head_dim
    chunk = span * kv_heads
    depth = x_ref.shape[1]
    half_dim = head_dim // 2
    block = depth // 10
    group_id = lax.axis_index("dp")
    me = lax.axis_index("cp")

    barrier = pltpu.get_barrier_semaphore()

    def greet(d, carry):
        peer = lax.rem(me + d, n)
        pl.semaphore_signal(barrier, inc=1, device_id=(group_id, peer), device_id_type=MESH)
        return carry

    lax.fori_loop(1, n, greet, 0)

    def weight_copies(b):
        slot = ring.at[b % RING]
        if b < 4:
            src = wk_ref if b < 2 else wv_ref
            base = (b % 2) * PACK
            return [pltpu.make_async_copy(src.at[pl.ds((base + c) * block, block)],
                                          slot.at[:, pl.ds(c * kv_width, kv_width)], ring_sem.at[b % RING, c])
                    for c in range(PACK)]
        src, r = (wq_ref, b - 4) if b < 14 else (wo_ref, b - 14)
        return [pltpu.make_async_copy(src.at[pl.ds(r * block, block)], slot, ring_sem.at[b % RING, 0])]

    def start_weights(b):
        for copy in weight_copies(b):
            copy.start()

    def wait_weights(b):
        for copy in weight_copies(b):
            copy.wait()

    def own_copy(c, src, land):
        return pltpu.make_async_copy(src.at[pl.ds(me * rows, rows)], land.at[:, pl.ds(me * chunk, chunk)], own_sem.at[c])

    def push(c, src, land, d):
        peer = lax.rem(me + d, n)
        return pltpu.make_async_remote_copy(
            src_ref=src.at[pl.ds(peer * rows, rows)],
            dst_ref=land.at[:, pl.ds(me * chunk, chunk)],
            send_sem=send_sem.at[c, d], recv_sem=recv_sem.at[c, me],
            device_id=(group_id, peer), device_id_type=MESH)

    def arrival(c, land, source):
        return pltpu.make_async_remote_copy(
            src_ref=land.at[:, pl.ds(source * chunk, chunk)],
            dst_ref=land.at[:, pl.ds(source * chunk, chunk)],
            send_sem=send_sem.at[c, 0], recv_sem=recv_sem.at[c, source],
            device_id=(group_id, me), device_id_type=MESH)

    pl.semaphore_wait(barrier, n - 1)
    order = []
    for d in range(n // 2, 0, -1):
        order.append(d)
        if n - d != d:
            order.append(n - d)
    for c, (src, land) in enumerate(((k_ref, k_land), (v_ref, v_land))):
        for d in order:
            push(c, src, land, d).start()
    own_copy(0, k_ref, k_land).start()
    own_copy(1, v_ref, v_land).start()
    for b in range(RING):
        start_weights(b)

    x_wide = x_ref[...].astype(jnp.float32)
    mean_sq = jnp.mean(x_wide * x_wide, axis=-1, keepdims=True)
    normed = x_wide * lax.rsqrt(mean_sq + RMS_EPS) * gain_ref[...].astype(jnp.float32)
    h_ref[...] = jnp.concatenate([normed, jnp.zeros((LHS_ROWS - rows, depth), jnp.float32)], axis=0).astype(jnp.bfloat16)
    acc[...] = jnp.zeros_like(acc)
    acc_kv[...] = jnp.zeros_like(acc_kv)

    def multiply(lhs, slot, out, tile_count):
        def tile(t, carry):
            cols = pl.ds(pl.multiple_of(t * TILE, TILE), TILE)
            out[:, cols] += jnp.dot(lhs, ring[slot, :, cols], preferred_element_type=jnp.float32)
            return carry
        lax.fori_loop(0, tile_count, tile, 0)

    def multiply_kv(b):
        base = (b % 2) * PACK
        out = (b // 2) * kv_width
        slot = b % RING
        def part(c, carry):
            lhs = h_ref[:, pl.ds(pl.multiple_of((base + c) * block, block), block)]
            for t in range(kv_width // TILE):
                cols = pl.ds(out + t * TILE, TILE)
                src = pl.ds(pl.multiple_of(c * kv_width + t * TILE, TILE), TILE)
                acc_kv[:, cols] += jnp.dot(lhs, ring[slot, :, src], preferred_element_type=jnp.float32)
            return carry
        lax.fori_loop(0, PACK, part, 0)

    for b in range(4):
        wait_weights(b)
        multiply_kv(b)
        start_weights(b + RING)
    for b in range(4, 14):
        wait_weights(b)
        multiply(h_ref[:, pl.ds((b - 4) * block, block)], b % RING, acc, width // TILE)
        if b + RING < 22:
            start_weights(b + RING)

    lane = lax.broadcasted_iota(jnp.int32, (1, head_dim), 1)
    freq_idx = jnp.where(lane < half_dim, lane, lane - half_dim).astype(jnp.float32)
    inv_freq = jnp.exp(freq_idx * (-2.0 * math.log(ROPE_THETA) / head_dim))
    sign = jnp.where(lane < half_dim, -1.0, 1.0)
    for s in range(rows):
        for j in range(heads):
            cols = slice(j * head_dim, (j + 1) * head_dim)
            q_raw[s, pl.ds(j, 1), :] = acc[pl.ds(s, 1), cols] + bq_ref[:, cols].astype(jnp.float32)
        for j in range(kv_heads):
            cols = slice(j * head_dim, (j + 1) * head_dim)
            v_cols = slice(kv_width + j * head_dim, kv_width + (j + 1) * head_dim)
            k_raw[s, pl.ds(j, 1), :] = acc_kv[pl.ds(s, 1), cols] + bk_ref[:, cols].astype(jnp.float32)
            v_raw[s, pl.ds(j, 1), :] = acc_kv[pl.ds(s, 1), v_cols] + bv_ref[:, cols].astype(jnp.float32)
    for s in range(rows):
        angle = lens_ref[me * rows + s].astype(jnp.float32) * inv_freq
        cos_t = jnp.cos(angle)
        sin_t = jnp.sin(angle) * sign
        q_one = q_raw[s]
        q_rot[s] = (q_one * cos_t + pltpu.roll(q_one, half_dim, 1) * sin_t).astype(jnp.bfloat16)
        k_one = k_raw[s]
        k_raw[s] = (k_one * cos_t + pltpu.roll(k_one, half_dim, 1) * sin_t).astype(jnp.bfloat16).astype(jnp.float32)
        v_raw[s] = v_raw[s].astype(jnp.bfloat16).astype(jnp.float32)

    row_idx = lax.broadcasted_iota(jnp.int32, (span, kv_heads, head_dim), 0)
    col = lax.broadcasted_iota(jnp.int32, (heads, chunk), 1)
    head = lax.broadcasted_iota(jnp.int32, (heads, chunk), 0)
    own_head = (col % kv_heads) == (head // group)
    col_slot = col // kv_heads
    scale = head_dim ** -0.5

    def settle(land, s, source, fresh):
        place = pl.ds(pl.multiple_of(source * chunk, chunk), chunk)
        limit = lens_ref[me * rows + s] - source * span
        old = land[s, place, :].astype(jnp.float32).reshape(span, kv_heads, head_dim)
        kept = jnp.where(row_idx < limit, old, jnp.where(row_idx == limit, fresh[s][None], 0.0))
        kept = kept.reshape(chunk, head_dim).astype(jnp.bfloat16)
        land[s, place, :] = kept
        return kept, place, limit

    def lane_fold(op, values):
        out = values[:, :head_dim]
        for t in range(1, chunk // head_dim):
            out = op(out, values[:, t * head_dim:(t + 1) * head_dim])
        return out

    def score_chunk(source):
        for s in range(rows):
            keys, place, limit = settle(k_land, s, source, k_raw)
            sc = lax.dot_general(q_rot[s], keys, (((1,), (1,)), ((), ())), preferred_element_type=jnp.float32) * scale
            sc = jnp.where(own_head & (col_slot <= limit), sc, MASKED)
            scores[s, :, place] = sc
            m_acc[s] = jnp.maximum(m_acc[s], lane_fold(jnp.maximum, sc))

    def value_chunk(source):
        for s in range(rows):
            vals, place, limit = settle(v_land, s, source, v_raw)
            e = jnp.exp(scores[s, :, place] - m_acc[s][:, :1])
            l_acc[s] += lane_fold(jnp.add, e)
            o_acc[s] += jnp.dot(e.astype(jnp.bfloat16), vals, preferred_element_type=jnp.float32)

    m_acc[...] = jnp.full_like(m_acc, MASKED)
    l_acc[...] = jnp.zeros_like(l_acc)
    o_acc[...] = jnp.zeros_like(o_acc)

    own_copy(0, k_ref, k_land).wait()
    score_chunk(me)
    for d in order:
        source = lax.rem(me - d + n, n)
        arrival(0, k_land, source).wait_recv()
        score_chunk(source)
    for s in range(rows):
        m_acc[s] = jnp.broadcast_to(jnp.max(m_acc[s], axis=-1, keepdims=True), (heads, head_dim))
    own_copy(1, v_ref, v_land).wait()
    value_chunk(me)
    for d in order:
        source = lax.rem(me - d + n, n)
        arrival(1, v_land, source).wait_recv()
        value_chunk(source)

    o_row[...] = jnp.zeros_like(o_row)
    for s in range(rows):
        l_all = jnp.sum(l_acc[s], axis=-1, keepdims=True)
        q_raw[s] = o_acc[s] / l_all
        for j in range(heads):
            o_row[pl.ds(s, 1), j * head_dim:(j + 1) * head_dim] = q_raw[s, pl.ds(j, 1), :]
    h_ref[...] = o_row[...].astype(jnp.bfloat16)
    acc[...] = jnp.zeros_like(acc)
    for b in range(14, 24):
        wait_weights(b)
        multiply(h_ref[:, pl.ds((b - 14) * block, block)], b % RING, acc, width // TILE)
        if b + RING < 24:
            start_weights(b + RING)
    y_ref[...] = (x_ref[...].astype(jnp.float32) + acc[:rows, :]).astype(jnp.bfloat16)
    for c, (src, land) in enumerate(((k_ref, k_land), (v_ref, v_land))):
        for d in order:
            push(c, src, land, d).wait_send()


def solution(mesh):
    batch_spec = P(('dp', 'cp'))
    seq_spec = P('dp', 'cp')
    whole = P()
    n = mesh.shape['cp']

    def per_device(x_tok, prompt_lens, k_cache, v_cache, norm_gain, w_q, b_q, w_k, b_k, w_v, b_v, w_o):
        rows, depth = x_tok.shape
        batch, span, kv_heads, head_dim = k_cache.shape
        width = w_q.shape[1]
        heads = width // head_dim
        chunk = span * kv_heads
        kv_width = kv_heads * head_dim
        block = depth // 10
        dims = (n, rows, span, kv_heads, head_dim, heads)
        vmem = pl.BlockSpec(memory_space=pltpu.VMEM)
        smem = pl.BlockSpec(memory_space=pltpu.SMEM)
        hbm = pl.BlockSpec(memory_space=pl.ANY)
        bf16, f32 = jnp.bfloat16, jnp.float32
        y, k_all, v_all = pl.pallas_call(
            functools.partial(decode_kernel, dims),
            out_shape=(jax.ShapeDtypeStruct((rows, depth), bf16),
                       pltpu.VMEM((rows, n * chunk, head_dim), bf16),
                       pltpu.VMEM((rows, n * chunk, head_dim), bf16)),
            in_specs=[smem] + [vmem] * 5 + [hbm] * 6,
            out_specs=(vmem, vmem, vmem),
            scratch_shapes=[
                pltpu.VMEM((RING, block, width), bf16),
                pltpu.VMEM((rows, heads, n * chunk), f32),
                pltpu.VMEM((LHS_ROWS, depth), bf16),
                pltpu.VMEM((LHS_ROWS, width), f32),
                pltpu.VMEM((LHS_ROWS, 2 * kv_width), f32),
                pltpu.VMEM((rows, heads, head_dim), f32),
                pltpu.VMEM((rows, heads, head_dim), bf16),
                pltpu.VMEM((rows, kv_heads, head_dim), f32),
                pltpu.VMEM((rows, kv_heads, head_dim), f32),
                pltpu.VMEM((rows, heads, head_dim), f32),
                pltpu.VMEM((rows, heads, head_dim), f32),
                pltpu.VMEM((rows, heads, head_dim), f32),
                pltpu.VMEM((LHS_ROWS, width), f32),
                pltpu.SemaphoreType.DMA((RING, PACK)),
                pltpu.SemaphoreType.DMA((2,)),
                pltpu.SemaphoreType.DMA((2, n)),
                pltpu.SemaphoreType.DMA((2, n)),
            ],
            compiler_params=pltpu.CompilerParams(collective_id=0, has_side_effects=True, vmem_limit_bytes=50 * 1024 * 1024),
            cost_estimate=pl.CostEstimate(flops=1 << 30, bytes_accessed=1 << 27, transcendentals=0),
        )(prompt_lens, x_tok, norm_gain[None], b_q[None], b_k[None], b_v[None],
          k_cache.reshape(batch, chunk, head_dim), v_cache.reshape(batch, chunk, head_dim), w_q, w_k, w_v, w_o)
        shape = (rows, n * span, kv_heads, head_dim)
        return y, k_all.reshape(shape), v_all.reshape(shape)

    return jax.shard_map(per_device, mesh=mesh, in_specs=(batch_spec, P('dp'), seq_spec, seq_spec, whole, whole, whole, whole, whole, whole, whole, whole), out_specs=(batch_spec, batch_spec, batch_spec), check_vma=False)
```

```python
import functools
import math
import jax
import jax.numpy as jnp
from jax import lax
from jax.experimental import pallas as pl
from jax.experimental.pallas import tpu as pltpu
from jax.sharding import PartitionSpec as P

RMS_EPS = 1e-6
ROPE_THETA = 1000000.0
MASKED = -1e30
RING = 9
PACK = 5
TILE = 512
LHS_ROWS = 16
MESH = pl.DeviceIdType.MESH


def exchange_kernel(dims, lens_hbm, x_hbm, gain_hbm, bq_hbm, bk_hbm, bv_hbm, k_ref, v_ref, wq_ref, wk_ref, wv_ref, wo_ref,
                    o_ref, k_land, v_land, ring,
                    lens_ref, x_ref, gain_ref, bq_ref, bk_ref, bv_ref,
                    scores, h_ref, acc, acc_kv, q_raw, q_rot, k_raw, v_raw, o_acc, m_acc, l_acc, o_row,
                    small_sem, ring_sem, own_sem, send_sem, recv_sem):
    n, rows, span, kv_heads, head_dim, heads = dims
    group = heads // kv_heads
    width = heads * head_dim
    kv_width = kv_heads * head_dim
    chunk = span * kv_heads
    depth = x_ref.shape[1]
    half_dim = head_dim // 2
    block = depth // 10
    group_id = lax.axis_index("dp")
    me = lax.axis_index("cp")

    barrier = pltpu.get_barrier_semaphore()

    def greet(d, carry):
        peer = lax.rem(me + d, n)
        pl.semaphore_signal(barrier, inc=1, device_id=(group_id, peer), device_id_type=MESH)
        return carry

    lax.fori_loop(1, n, greet, 0)

    def weight_copies(b):
        slot = ring.at[b % RING]
        if b < 4:
            src = wk_ref if b < 2 else wv_ref
            base = (b % 2) * PACK
            return [pltpu.make_async_copy(src.at[pl.ds((base + c) * block, block)],
                                          slot.at[:, pl.ds(c * kv_width, kv_width)], ring_sem.at[b % RING, c])
                    for c in range(PACK)]
        src, r = (wq_ref, b - 4) if b < 14 else (wo_ref, b - 14)
        return [pltpu.make_async_copy(src.at[pl.ds(r * block, block)], slot, ring_sem.at[b % RING, 0])]

    def start_weights(b):
        for copy in weight_copies(b):
            copy.start()

    def wait_weights(b):
        for copy in weight_copies(b):
            copy.wait()

    def own_copy(c, src, land):
        return pltpu.make_async_copy(src.at[pl.ds(me * rows, rows)], land.at[:, pl.ds(me * chunk, chunk)], own_sem.at[c])

    def push(c, src, land, d):
        peer = lax.rem(me + d, n)
        return pltpu.make_async_remote_copy(
            src_ref=src.at[pl.ds(peer * rows, rows)],
            dst_ref=land.at[:, pl.ds(me * chunk, chunk)],
            send_sem=send_sem.at[c, d], recv_sem=recv_sem.at[c, me],
            device_id=(group_id, peer), device_id_type=MESH)

    def arrival(c, land, source):
        return pltpu.make_async_remote_copy(
            src_ref=land.at[:, pl.ds(source * chunk, chunk)],
            dst_ref=land.at[:, pl.ds(source * chunk, chunk)],
            send_sem=send_sem.at[c, 0], recv_sem=recv_sem.at[c, source],
            device_id=(group_id, me), device_id_type=MESH)

    pl.semaphore_wait(barrier, n - 1)
    order = []
    for d in range(n // 2, 0, -1):
        order.append(d)
        if n - d != d:
            order.append(n - d)
    for c, (src, land) in enumerate(((k_ref, k_land), (v_ref, v_land))):
        for d in order:
            push(c, src, land, d).start()
    own_copy(0, k_ref, k_land).start()
    own_copy(1, v_ref, v_land).start()
    small = [pltpu.make_async_copy(src, dst, small_sem.at[i]) for i, (src, dst) in enumerate((
        (lens_hbm, lens_ref), (x_hbm, x_ref), (gain_hbm, gain_ref), (bq_hbm, bq_ref), (bk_hbm, bk_ref), (bv_hbm, bv_ref)))]
    for copy in small:
        copy.start()
    for b in range(RING):
        start_weights(b)
    for copy in small:
        copy.wait()

    x_wide = x_ref[...].astype(jnp.float32)
    mean_sq = jnp.mean(x_wide * x_wide, axis=-1, keepdims=True)
    normed = x_wide * lax.rsqrt(mean_sq + RMS_EPS) * gain_ref[...].astype(jnp.float32).reshape(1, depth)
    h_ref[...] = jnp.concatenate([normed, jnp.zeros((LHS_ROWS - rows, depth), jnp.float32)], axis=0).astype(jnp.bfloat16)
    acc[...] = jnp.zeros_like(acc)
    acc_kv[...] = jnp.zeros_like(acc_kv)

    def multiply(lhs, slot, out, tile_count):
        def tile(t, carry):
            cols = pl.ds(pl.multiple_of(t * TILE, TILE), TILE)
            out[:, cols] += jnp.dot(lhs, ring[slot, :, cols], preferred_element_type=jnp.float32)
            return carry
        lax.fori_loop(0, tile_count, tile, 0)

    def multiply_kv(b):
        base = (b % 2) * PACK
        out = (b // 2) * kv_width
        slot = b % RING
        def part(c, carry):
            lhs = h_ref[:, pl.ds(pl.multiple_of((base + c) * block, block), block)]
            for t in range(kv_width // TILE):
                cols = pl.ds(out + t * TILE, TILE)
                src = pl.ds(pl.multiple_of(c * kv_width + t * TILE, TILE), TILE)
                acc_kv[:, cols] += jnp.dot(lhs, ring[slot, :, src], preferred_element_type=jnp.float32)
            return carry
        lax.fori_loop(0, PACK, part, 0)

    for b in range(4):
        wait_weights(b)
        multiply_kv(b)
        start_weights(b + RING)
    for b in range(4, 14):
        wait_weights(b)
        multiply(h_ref[:, pl.ds((b - 4) * block, block)], b % RING, acc, width // TILE)
        if b + RING < 14 + RING:
            start_weights(b + RING)

    lane = lax.broadcasted_iota(jnp.int32, (1, head_dim), 1)
    freq_idx = jnp.where(lane < half_dim, lane, lane - half_dim).astype(jnp.float32)
    inv_freq = jnp.exp(freq_idx * (-2.0 * math.log(ROPE_THETA) / head_dim))
    sign = jnp.where(lane < half_dim, -1.0, 1.0)
    q_bias = bq_ref[...].astype(jnp.float32).reshape(heads, head_dim)
    k_bias = bk_ref[...].astype(jnp.float32).reshape(kv_heads, head_dim)
    v_bias = bv_ref[...].astype(jnp.float32).reshape(kv_heads, head_dim)
    for s in range(rows):
        for j in range(heads):
            q_raw[s, pl.ds(j, 1), :] = acc[pl.ds(s, 1), j * head_dim:(j + 1) * head_dim]
        for j in range(kv_heads):
            k_raw[s, pl.ds(j, 1), :] = acc_kv[pl.ds(s, 1), j * head_dim:(j + 1) * head_dim]
            v_raw[s, pl.ds(j, 1), :] = acc_kv[pl.ds(s, 1), kv_width + j * head_dim:kv_width + (j + 1) * head_dim]
    for s in range(rows):
        angle = lens_ref[me * rows + s].astype(jnp.float32) * inv_freq
        cos_t = jnp.cos(angle)
        sin_t = jnp.sin(angle) * sign
        q_one = q_raw[s] + q_bias
        q_rot[s] = (q_one * cos_t + pltpu.roll(q_one, half_dim, 1) * sin_t).astype(jnp.bfloat16)
        k_one = k_raw[s] + k_bias
        k_raw[s] = (k_one * cos_t + pltpu.roll(k_one, half_dim, 1) * sin_t).astype(jnp.bfloat16).astype(jnp.float32)
        v_raw[s] = (v_raw[s] + v_bias).astype(jnp.bfloat16).astype(jnp.float32)

    row_idx = lax.broadcasted_iota(jnp.int32, (span, kv_heads, head_dim), 0)
    col = lax.broadcasted_iota(jnp.int32, (heads, chunk), 1)
    head = lax.broadcasted_iota(jnp.int32, (heads, chunk), 0)
    own_head = (col % kv_heads) == (head // group)
    col_slot = col // kv_heads
    scale = head_dim ** -0.5

    def settle(land, s, source, fresh):
        place = pl.ds(pl.multiple_of(source * chunk, chunk), chunk)
        limit = lens_ref[me * rows + s] - source * span
        old = land[s, place, :].astype(jnp.float32).reshape(span, kv_heads, head_dim)
        kept = jnp.where(row_idx < limit, old, jnp.where(row_idx == limit, fresh[s][None], 0.0))
        kept = kept.reshape(chunk, head_dim).astype(jnp.bfloat16)
        land[s, place, :] = kept
        return kept, place, limit

    def lane_fold(op, values):
        out = values[:, :head_dim]
        for t in range(1, chunk // head_dim):
            out = op(out, values[:, t * head_dim:(t + 1) * head_dim])
        return out

    def score_chunk(source):
        for s in range(rows):
            keys, place, limit = settle(k_land, s, source, k_raw)
            sc = lax.dot_general(q_rot[s], keys, (((1,), (1,)), ((), ())), preferred_element_type=jnp.float32) * scale
            sc = jnp.where(own_head & (col_slot <= limit), sc, MASKED)
            scores[s, :, place] = sc
            m_acc[s] = jnp.maximum(m_acc[s], lane_fold(jnp.maximum, sc))

    def value_chunk(source):
        for s in range(rows):
            vals, place, limit = settle(v_land, s, source, v_raw)
            e = jnp.exp(scores[s, :, place] - m_acc[s][:, :1])
            l_acc[s] += lane_fold(jnp.add, e)
            o_acc[s] += jnp.dot(e.astype(jnp.bfloat16), vals, preferred_element_type=jnp.float32)

    m_acc[...] = jnp.full_like(m_acc, MASKED)
    l_acc[...] = jnp.zeros_like(l_acc)
    o_acc[...] = jnp.zeros_like(o_acc)

    own_copy(0, k_ref, k_land).wait()
    score_chunk(me)
    for d in order:
        source = lax.rem(me - d + n, n)
        arrival(0, k_land, source).wait_recv()
        score_chunk(source)
    for s in range(rows):
        m_acc[s] = jnp.broadcast_to(jnp.max(m_acc[s], axis=-1, keepdims=True), (heads, head_dim))
    own_copy(1, v_ref, v_land).wait()
    value_chunk(me)
    for d in order:
        source = lax.rem(me - d + n, n)
        arrival(1, v_land, source).wait_recv()
        value_chunk(source)

    o_row[...] = jnp.zeros_like(o_row)
    for s in range(rows):
        l_all = jnp.sum(l_acc[s], axis=-1, keepdims=True)
        q_raw[s] = o_acc[s] / l_all
        for j in range(heads):
            o_row[pl.ds(s, 1), j * head_dim:(j + 1) * head_dim] = q_raw[s, pl.ds(j, 1), :]
    o_ref[...] = o_row[...].astype(jnp.bfloat16)
    for b in range(14, 14 + RING):
        wait_weights(b)
    for c, (src, land) in enumerate(((k_ref, k_land), (v_ref, v_land))):
        for d in order:
            push(c, src, land, d).wait_send()


def output_kernel(first, o_ref, k_land, v_land, ring, x_hbm, wo_ref, y_ref, k_out, v_out, x_ref, extra, acc, sem):
    rows, depth = x_ref.shape
    block, width = extra.shape[1:]
    resident = ring.shape[0]
    tail = [pltpu.make_async_copy(wo_ref.at[pl.ds((resident + i) * block, block)], extra.at[i], sem.at[i])
            for i in range(extra.shape[0])]
    rest = [pltpu.make_async_copy(x_hbm, x_ref, sem.at[len(tail)]),
            pltpu.make_async_copy(k_land, k_out, sem.at[len(tail) + 1]),
            pltpu.make_async_copy(v_land, v_out, sem.at[len(tail) + 2])]
    for copy in tail + rest:
        copy.start()
    acc[...] = jnp.zeros_like(acc)

    def multiply(r, weights):
        lhs = o_ref[:, r * block:(r + 1) * block]

        def tile(t, carry):
            cols = pl.ds(pl.multiple_of(t * TILE, TILE), TILE)
            acc[:, cols] += jnp.dot(lhs, weights[:, cols], preferred_element_type=jnp.float32)
            return carry
        lax.fori_loop(0, width // TILE, tile, 0)

    for r in range(resident):
        multiply(r, ring.at[(first + r) % resident])
    for i, copy in enumerate(tail):
        copy.wait()
        multiply(resident + i, extra.at[i])
    for copy in rest:
        copy.wait()
    y_ref[...] = (x_ref[...].astype(jnp.float32) + acc[:rows, :]).astype(jnp.bfloat16)


def solution(mesh):
    batch_spec = P(('dp', 'cp'))
    seq_spec = P('dp', 'cp')
    whole = P()
    n = mesh.shape['cp']

    def per_device(x_tok, prompt_lens, k_cache, v_cache, norm_gain, w_q, b_q, w_k, b_k, w_v, b_v, w_o):
        rows, depth = x_tok.shape
        batch, span, kv_heads, head_dim = k_cache.shape
        width = w_q.shape[1]
        heads = width // head_dim
        chunk = span * kv_heads
        kv_width = kv_heads * head_dim
        block = depth // 10
        dims = (n, rows, span, kv_heads, head_dim, heads)
        vmem = pl.BlockSpec(memory_space=pltpu.VMEM)
        smem = pl.BlockSpec(memory_space=pltpu.SMEM)
        hbm = pl.BlockSpec(memory_space=pl.ANY)
        bf16, f32 = jnp.bfloat16, jnp.float32
        land = (rows, n * chunk, head_dim)
        o_rows, k_all, v_all, ring = pl.pallas_call(
            functools.partial(exchange_kernel, dims),
            out_shape=(pltpu.VMEM((LHS_ROWS, width), bf16), pltpu.VMEM(land, bf16), pltpu.VMEM(land, bf16),
                       pltpu.VMEM((RING, block, width), bf16)),
            in_specs=[hbm] * 12,
            out_specs=(vmem,) * 4,
            scratch_shapes=[
                pltpu.SMEM((batch,), jnp.int32),
                pltpu.VMEM((rows, depth), bf16),
                pltpu.VMEM((depth,), bf16),
                pltpu.VMEM((width,), bf16),
                pltpu.VMEM((kv_width,), bf16),
                pltpu.VMEM((kv_width,), bf16),
                pltpu.VMEM((rows, heads, n * chunk), f32),
                pltpu.VMEM((LHS_ROWS, depth), bf16),
                pltpu.VMEM((LHS_ROWS, width), f32),
                pltpu.VMEM((LHS_ROWS, 2 * kv_width), f32),
                pltpu.VMEM((rows, heads, head_dim), f32),
                pltpu.VMEM((rows, heads, head_dim), bf16),
                pltpu.VMEM((rows, kv_heads, head_dim), f32),
                pltpu.VMEM((rows, kv_heads, head_dim), f32),
                pltpu.VMEM((rows, heads, head_dim), f32),
                pltpu.VMEM((rows, heads, head_dim), f32),
                pltpu.VMEM((rows, heads, head_dim), f32),
                pltpu.VMEM((LHS_ROWS, width), f32),
                pltpu.SemaphoreType.DMA((6,)),
                pltpu.SemaphoreType.DMA((RING, PACK)),
                pltpu.SemaphoreType.DMA((2,)),
                pltpu.SemaphoreType.DMA((2, n)),
                pltpu.SemaphoreType.DMA((2, n)),
            ],
            compiler_params=pltpu.CompilerParams(collective_id=0, has_side_effects=True, vmem_limit_bytes=8 * 1024 * 1024),
            cost_estimate=pl.CostEstimate(flops=1 << 30, bytes_accessed=1 << 27, transcendentals=0),
        )(prompt_lens, x_tok, norm_gain, b_q, b_k, b_v,
          k_cache.reshape(batch, chunk, head_dim), v_cache.reshape(batch, chunk, head_dim), w_q, w_k, w_v, w_o)
        extra = depth // block - RING
        y, k_out, v_out = pl.pallas_call(
            functools.partial(output_kernel, 14),
            out_shape=(jax.ShapeDtypeStruct((rows, depth), bf16), jax.ShapeDtypeStruct(land, bf16), jax.ShapeDtypeStruct(land, bf16)),
            in_specs=[vmem] * 4 + [hbm] * 2,
            out_specs=(vmem, hbm, hbm),
            scratch_shapes=[
                pltpu.VMEM((rows, depth), bf16),
                pltpu.VMEM((extra, block, width), bf16),
                pltpu.VMEM((LHS_ROWS, depth), f32),
                pltpu.SemaphoreType.DMA((extra + 3,)),
            ],
            compiler_params=pltpu.CompilerParams(vmem_limit_bytes=(extra * 6 + 2) * 1024 * 1024),
            cost_estimate=pl.CostEstimate(flops=1 << 30, bytes_accessed=1 << 25, transcendentals=0),
        )(*[pltpu.with_memory_space_constraint(a, pltpu.VMEM) for a in (o_rows, k_all, v_all, ring)], x_tok, w_o)
        shape = (rows, n * span, kv_heads, head_dim)
        return y, k_out.reshape(shape), v_out.reshape(shape)

    return jax.shard_map(per_device, mesh=mesh, in_specs=(batch_spec, P('dp'), seq_spec, seq_spec, whole, whole, whole, whole, whole, whole, whole, whole), out_specs=(batch_spec, batch_spec, batch_spec), check_vma=False)
```

```python
import functools
import math
import jax
import jax.numpy as jnp
from jax import lax
from jax.experimental import pallas as pl
from jax.experimental.pallas import tpu as pltpu
from jax.sharding import PartitionSpec as P

RMS_EPS = 1e-6
ROPE_THETA = 1000000.0
MASKED = -1e30
RING = 9
PACK = 5
TILE = 512
OUT_TILE = 512
LHS_ROWS = 16
MESH = pl.DeviceIdType.MESH


def exchange_kernel(dims, lens_hbm, x_hbm, gain_hbm, bq_hbm, bk_hbm, bv_hbm, k_ref, v_ref, wq_ref, wk_ref, wv_ref, wo_ref,
                    o_ref, k_land, v_land, ring,
                    lens_ref, x_ref, gain_ref, bq_ref, bk_ref, bv_ref,
                    scores, h_ref, acc, acc_kv, q_raw, q_rot, k_raw, v_raw, o_acc, m_acc, l_acc, o_row,
                    small_sem, ring_sem, own_sem, send_sem, recv_sem):
    n, rows, span, kv_heads, head_dim, heads = dims
    group = heads // kv_heads
    width = heads * head_dim
    kv_width = kv_heads * head_dim
    chunk = span * kv_heads
    depth = x_ref.shape[1]
    half_dim = head_dim // 2
    block = depth // 10
    group_id = lax.axis_index("dp")
    me = lax.axis_index("cp")

    barrier = pltpu.get_barrier_semaphore()

    def greet(d, carry):
        peer = lax.rem(me + d, n)
        pl.semaphore_signal(barrier, inc=1, device_id=(group_id, peer), device_id_type=MESH)
        return carry

    lax.fori_loop(1, n, greet, 0)

    def weight_copies(b):
        slot = ring.at[b % RING]
        if b < 4:
            src = wk_ref if b < 2 else wv_ref
            base = (b % 2) * PACK
            return [pltpu.make_async_copy(src.at[pl.ds((base + c) * block, block)],
                                          slot.at[:, pl.ds(c * kv_width, kv_width)], ring_sem.at[b % RING, c])
                    for c in range(PACK)]
        src, r = (wq_ref, b - 4) if b < 14 else (wo_ref, b - 14)
        return [pltpu.make_async_copy(src.at[pl.ds(r * block, block)], slot, ring_sem.at[b % RING, 0])]

    def start_weights(b):
        for copy in weight_copies(b):
            copy.start()

    def wait_weights(b):
        for copy in weight_copies(b):
            copy.wait()

    def own_copy(c, src, land):
        return pltpu.make_async_copy(src.at[pl.ds(me * rows, rows)], land.at[:, pl.ds(me * chunk, chunk)], own_sem.at[c])

    def push(c, src, land, d):
        peer = lax.rem(me + d, n)
        return pltpu.make_async_remote_copy(
            src_ref=src.at[pl.ds(peer * rows, rows)],
            dst_ref=land.at[:, pl.ds(me * chunk, chunk)],
            send_sem=send_sem.at[c, d], recv_sem=recv_sem.at[c, me],
            device_id=(group_id, peer), device_id_type=MESH)

    def arrival(c, land, source):
        return pltpu.make_async_remote_copy(
            src_ref=land.at[:, pl.ds(source * chunk, chunk)],
            dst_ref=land.at[:, pl.ds(source * chunk, chunk)],
            send_sem=send_sem.at[c, 0], recv_sem=recv_sem.at[c, source],
            device_id=(group_id, me), device_id_type=MESH)

    pl.semaphore_wait(barrier, n - 1)
    order = []
    for d in range(n // 2, 0, -1):
        order.append(d)
        if n - d != d:
            order.append(n - d)
    for c, (src, land) in enumerate(((k_ref, k_land), (v_ref, v_land))):
        for d in order:
            push(c, src, land, d).start()
    own_copy(0, k_ref, k_land).start()
    own_copy(1, v_ref, v_land).start()
    small = [pltpu.make_async_copy(src, dst, small_sem.at[i]) for i, (src, dst) in enumerate((
        (lens_hbm, lens_ref), (x_hbm, x_ref), (gain_hbm, gain_ref), (bq_hbm, bq_ref), (bk_hbm, bk_ref), (bv_hbm, bv_ref)))]
    for copy in small:
        copy.start()
    for b in range(RING):
        start_weights(b)
    for copy in small:
        copy.wait()

    x_wide = x_ref[...].astype(jnp.float32)
    mean_sq = jnp.mean(x_wide * x_wide, axis=-1, keepdims=True)
    normed = x_wide * lax.rsqrt(mean_sq + RMS_EPS) * gain_ref[...].astype(jnp.float32).reshape(1, depth)
    h_ref[...] = jnp.concatenate([normed, jnp.zeros((LHS_ROWS - rows, depth), jnp.float32)], axis=0).astype(jnp.bfloat16)
    acc[...] = jnp.zeros_like(acc)
    acc_kv[...] = jnp.zeros_like(acc_kv)

    def multiply(lhs, slot, out, tile_count):
        def tile(t, carry):
            cols = pl.ds(pl.multiple_of(t * TILE, TILE), TILE)
            out[:, cols] += jnp.dot(lhs, ring[slot, :, cols], preferred_element_type=jnp.float32)
            return carry
        lax.fori_loop(0, tile_count, tile, 0)

    def multiply_kv(b):
        base = (b % 2) * PACK
        out = (b // 2) * kv_width
        slot = b % RING
        def part(c, carry):
            lhs = h_ref[:, pl.ds(pl.multiple_of((base + c) * block, block), block)]
            for t in range(kv_width // TILE):
                cols = pl.ds(out + t * TILE, TILE)
                src = pl.ds(pl.multiple_of(c * kv_width + t * TILE, TILE), TILE)
                acc_kv[:, cols] += jnp.dot(lhs, ring[slot, :, src], preferred_element_type=jnp.float32)
            return carry
        lax.fori_loop(0, PACK, part, 0)

    for b in range(4):
        wait_weights(b)
        multiply_kv(b)
        start_weights(b + RING)
    for b in range(4, 14):
        wait_weights(b)
        multiply(h_ref[:, pl.ds((b - 4) * block, block)], b % RING, acc, width // TILE)
        if b + RING < 14 + RING:
            start_weights(b + RING)

    lane = lax.broadcasted_iota(jnp.int32, (1, head_dim), 1)
    freq_idx = jnp.where(lane < half_dim, lane, lane - half_dim).astype(jnp.float32)
    inv_freq = jnp.exp(freq_idx * (-2.0 * math.log(ROPE_THETA) / head_dim))
    sign = jnp.where(lane < half_dim, -1.0, 1.0)
    q_bias = bq_ref[...].astype(jnp.float32).reshape(heads, head_dim)
    k_bias = bk_ref[...].astype(jnp.float32).reshape(kv_heads, head_dim)
    v_bias = bv_ref[...].astype(jnp.float32).reshape(kv_heads, head_dim)
    for s in range(rows):
        for j in range(heads):
            q_raw[s, pl.ds(j, 1), :] = acc[pl.ds(s, 1), j * head_dim:(j + 1) * head_dim]
        for j in range(kv_heads):
            k_raw[s, pl.ds(j, 1), :] = acc_kv[pl.ds(s, 1), j * head_dim:(j + 1) * head_dim]
            v_raw[s, pl.ds(j, 1), :] = acc_kv[pl.ds(s, 1), kv_width + j * head_dim:kv_width + (j + 1) * head_dim]
    for s in range(rows):
        angle = lens_ref[me * rows + s].astype(jnp.float32) * inv_freq
        cos_t = jnp.cos(angle)
        sin_t = jnp.sin(angle) * sign
        q_one = q_raw[s] + q_bias
        q_rot[s] = (q_one * cos_t + pltpu.roll(q_one, half_dim, 1) * sin_t).astype(jnp.bfloat16)
        k_one = k_raw[s] + k_bias
        k_raw[s] = (k_one * cos_t + pltpu.roll(k_one, half_dim, 1) * sin_t).astype(jnp.bfloat16).astype(jnp.float32)
        v_raw[s] = (v_raw[s] + v_bias).astype(jnp.bfloat16).astype(jnp.float32)

    row_idx = lax.broadcasted_iota(jnp.int32, (span, kv_heads, head_dim), 0)
    col = lax.broadcasted_iota(jnp.int32, (heads, chunk), 1)
    head = lax.broadcasted_iota(jnp.int32, (heads, chunk), 0)
    own_head = (col % kv_heads) == (head // group)
    col_slot = col // kv_heads
    scale = head_dim ** -0.5

    def settle(land, s, source, fresh):
        place = pl.ds(pl.multiple_of(source * chunk, chunk), chunk)
        limit = lens_ref[me * rows + s] - source * span
        old = land[s, place, :].astype(jnp.float32).reshape(span, kv_heads, head_dim)
        kept = jnp.where(row_idx < limit, old, jnp.where(row_idx == limit, fresh[s][None], 0.0))
        kept = kept.reshape(chunk, head_dim).astype(jnp.bfloat16)
        land[s, place, :] = kept
        return kept, place, limit

    def lane_fold(op, values):
        out = values[:, :head_dim]
        for t in range(1, chunk // head_dim):
            out = op(out, values[:, t * head_dim:(t + 1) * head_dim])
        return out

    def score_chunk(source):
        for s in range(rows):
            keys, place, limit = settle(k_land, s, source, k_raw)
            sc = lax.dot_general(q_rot[s], keys, (((1,), (1,)), ((), ())), preferred_element_type=jnp.float32) * scale
            sc = jnp.where(own_head & (col_slot <= limit), sc, MASKED)
            scores[s, :, place] = sc
            m_acc[s] = jnp.maximum(m_acc[s], lane_fold(jnp.maximum, sc))

    def value_chunk(source):
        for s in range(rows):
            vals, place, limit = settle(v_land, s, source, v_raw)
            e = jnp.exp(scores[s, :, place] - m_acc[s][:, :1])
            l_acc[s] += lane_fold(jnp.add, e)
            o_acc[s] += jnp.dot(e.astype(jnp.bfloat16), vals, preferred_element_type=jnp.float32)

    m_acc[...] = jnp.full_like(m_acc, MASKED)
    l_acc[...] = jnp.zeros_like(l_acc)
    o_acc[...] = jnp.zeros_like(o_acc)

    own_copy(0, k_ref, k_land).wait()
    score_chunk(me)
    for d in order:
        source = lax.rem(me - d + n, n)
        arrival(0, k_land, source).wait_recv()
        score_chunk(source)
    for s in range(rows):
        m_acc[s] = jnp.broadcast_to(jnp.max(m_acc[s], axis=-1, keepdims=True), (heads, head_dim))
    own_copy(1, v_ref, v_land).wait()
    value_chunk(me)
    for d in order:
        source = lax.rem(me - d + n, n)
        arrival(1, v_land, source).wait_recv()
        value_chunk(source)

    o_row[...] = jnp.zeros_like(o_row)
    for s in range(rows):
        l_all = jnp.sum(l_acc[s], axis=-1, keepdims=True)
        q_raw[s] = o_acc[s] / l_all
        for j in range(heads):
            o_row[pl.ds(s, 1), j * head_dim:(j + 1) * head_dim] = q_raw[s, pl.ds(j, 1), :]
    o_ref[...] = o_row[...].astype(jnp.bfloat16)
    for b in range(14, 14 + RING):
        wait_weights(b)
    for c, (src, land) in enumerate(((k_ref, k_land), (v_ref, v_land))):
        for d in order:
            push(c, src, land, d).wait_send()


def output_kernel(first, o_ref, k_land, v_land, ring, x_hbm, wo_ref, y_ref, k_out, v_out, x_ref, extra, acc, sem):
    rows, depth = x_ref.shape
    block, width = extra.shape[1:]
    resident = ring.shape[0]
    tail = [pltpu.make_async_copy(wo_ref.at[pl.ds((resident + i) * block, block)], extra.at[i], sem.at[i])
            for i in range(extra.shape[0])]
    rest = [pltpu.make_async_copy(x_hbm, x_ref, sem.at[len(tail)]),
            pltpu.make_async_copy(k_land, k_out, sem.at[len(tail) + 1]),
            pltpu.make_async_copy(v_land, v_out, sem.at[len(tail) + 2])]
    for copy in tail + rest:
        copy.start()
    acc[...] = jnp.zeros_like(acc)

    def multiply(r, weights):
        lhs = o_ref[:, r * block:(r + 1) * block]

        for t in range(width // OUT_TILE):
            cols = slice(t * OUT_TILE, (t + 1) * OUT_TILE)
            acc[:, cols] += jnp.dot(lhs, weights[:, cols], preferred_element_type=jnp.float32)

    for r in range(resident):
        multiply(r, ring.at[(first + r) % resident])
    for i, copy in enumerate(tail):
        copy.wait()
        multiply(resident + i, extra.at[i])
    for copy in rest:
        copy.wait()
    y_ref[...] = (x_ref[...].astype(jnp.float32) + acc[:rows, :]).astype(jnp.bfloat16)


def solution(mesh):
    batch_spec = P(('dp', 'cp'))
    seq_spec = P('dp', 'cp')
    whole = P()
    n = mesh.shape['cp']

    def per_device(x_tok, prompt_lens, k_cache, v_cache, norm_gain, w_q, b_q, w_k, b_k, w_v, b_v, w_o):
        rows, depth = x_tok.shape
        batch, span, kv_heads, head_dim = k_cache.shape
        width = w_q.shape[1]
        heads = width // head_dim
        chunk = span * kv_heads
        kv_width = kv_heads * head_dim
        block = depth // 10
        dims = (n, rows, span, kv_heads, head_dim, heads)
        vmem = pl.BlockSpec(memory_space=pltpu.VMEM)
        smem = pl.BlockSpec(memory_space=pltpu.SMEM)
        hbm = pl.BlockSpec(memory_space=pl.ANY)
        bf16, f32 = jnp.bfloat16, jnp.float32
        land = (rows, n * chunk, head_dim)
        o_rows, k_all, v_all, ring = pl.pallas_call(
            functools.partial(exchange_kernel, dims),
            out_shape=(pltpu.VMEM((LHS_ROWS, width), bf16), pltpu.VMEM(land, bf16), pltpu.VMEM(land, bf16),
                       pltpu.VMEM((RING, block, width), bf16)),
            in_specs=[hbm] * 12,
            out_specs=(vmem,) * 4,
            scratch_shapes=[
                pltpu.SMEM((batch,), jnp.int32),
                pltpu.VMEM((rows, depth), bf16),
                pltpu.VMEM((depth,), bf16),
                pltpu.VMEM((width,), bf16),
                pltpu.VMEM((kv_width,), bf16),
                pltpu.VMEM((kv_width,), bf16),
                pltpu.VMEM((rows, heads, n * chunk), f32),
                pltpu.VMEM((LHS_ROWS, depth), bf16),
                pltpu.VMEM((LHS_ROWS, width), f32),
                pltpu.VMEM((LHS_ROWS, 2 * kv_width), f32),
                pltpu.VMEM((rows, heads, head_dim), f32),
                pltpu.VMEM((rows, heads, head_dim), bf16),
                pltpu.VMEM((rows, kv_heads, head_dim), f32),
                pltpu.VMEM((rows, kv_heads, head_dim), f32),
                pltpu.VMEM((rows, heads, head_dim), f32),
                pltpu.VMEM((rows, heads, head_dim), f32),
                pltpu.VMEM((rows, heads, head_dim), f32),
                pltpu.VMEM((LHS_ROWS, width), f32),
                pltpu.SemaphoreType.DMA((6,)),
                pltpu.SemaphoreType.DMA((RING, PACK)),
                pltpu.SemaphoreType.DMA((2,)),
                pltpu.SemaphoreType.DMA((2, n)),
                pltpu.SemaphoreType.DMA((2, n)),
            ],
            compiler_params=pltpu.CompilerParams(collective_id=0, has_side_effects=True, vmem_limit_bytes=8 * 1024 * 1024),
            cost_estimate=pl.CostEstimate(flops=1 << 30, bytes_accessed=1 << 27, transcendentals=0),
        )(prompt_lens, x_tok, norm_gain, b_q, b_k, b_v,
          k_cache.reshape(batch, chunk, head_dim), v_cache.reshape(batch, chunk, head_dim), w_q, w_k, w_v, w_o)
        extra = depth // block - RING
        y, k_out, v_out = pl.pallas_call(
            functools.partial(output_kernel, 14),
            out_shape=(jax.ShapeDtypeStruct((rows, depth), bf16), jax.ShapeDtypeStruct(land, bf16), jax.ShapeDtypeStruct(land, bf16)),
            in_specs=[vmem] * 4 + [hbm] * 2,
            out_specs=(vmem, hbm, hbm),
            scratch_shapes=[
                pltpu.VMEM((rows, depth), bf16),
                pltpu.VMEM((extra, block, width), bf16),
                pltpu.VMEM((LHS_ROWS, depth), f32),
                pltpu.SemaphoreType.DMA((extra + 3,)),
            ],
            compiler_params=pltpu.CompilerParams(vmem_limit_bytes=(extra * 6 + 2) * 1024 * 1024),
            cost_estimate=pl.CostEstimate(flops=1 << 30, bytes_accessed=1 << 25, transcendentals=0),
        )(*[pltpu.with_memory_space_constraint(a, pltpu.VMEM) for a in (o_rows, k_all, v_all, ring)], x_tok, w_o)
        shape = (rows, n * span, kv_heads, head_dim)
        return y, k_out.reshape(shape), v_out.reshape(shape)

    return jax.shard_map(per_device, mesh=mesh, in_specs=(batch_spec, P('dp'), seq_spec, seq_spec, whole, whole, whole, whole, whole, whole, whole, whole), out_specs=(batch_spec, batch_spec, batch_spec), check_vma=False)
```

```python
import functools
import math
import jax
import jax.numpy as jnp
from jax import lax
from jax.experimental import pallas as pl
from jax.experimental.pallas import tpu as pltpu
from jax.sharding import PartitionSpec as P

RMS_EPS = 1e-6
ROPE_THETA = 1000000.0
MASKED = -1e30
RING = 9
PACK = 5
TILE = 512
OUT_TILE = 512
LHS_ROWS = 16
CORES = 2
MESH = pl.DeviceIdType.MESH


def exchange_kernel(dims, lens_hbm, x_hbm, gain_hbm, bq_hbm, bk_hbm, bv_hbm, k_ref, v_ref, wq_ref, wk_ref, wv_ref, wo_ref,
                    o_ref, k_land, v_land, ring,
                    lens_ref, x_ref, gain_ref, bq_ref, bk_ref, bv_ref,
                    scores, h_ref, acc, acc_kv, q_raw, q_rot, k_raw, v_raw, o_acc, m_acc, l_acc, o_row,
                    small_sem, ring_sem, own_sem, send_sem, recv_sem):
    n, rows, span, kv_heads, head_dim, heads = dims
    group = heads // kv_heads
    width = heads * head_dim
    kv_width = kv_heads * head_dim
    chunk = span * kv_heads
    depth = x_ref.shape[1]
    half_dim = head_dim // 2
    block = depth // 10
    group_id = lax.axis_index("dp")
    me = lax.axis_index("cp")

    barrier = pltpu.get_barrier_semaphore()

    def greet(d, carry):
        peer = lax.rem(me + d, n)
        pl.semaphore_signal(barrier, inc=1, device_id=(group_id, peer), device_id_type=MESH)
        return carry

    lax.fori_loop(1, n, greet, 0)

    def weight_copies(b):
        slot = ring.at[b % RING]
        if b < 4:
            src = wk_ref if b < 2 else wv_ref
            base = (b % 2) * PACK
            return [pltpu.make_async_copy(src.at[pl.ds((base + c) * block, block)],
                                          slot.at[:, pl.ds(c * kv_width, kv_width)], ring_sem.at[b % RING, c])
                    for c in range(PACK)]
        src, r = (wq_ref, b - 4) if b < 14 else (wo_ref, b - 14)
        return [pltpu.make_async_copy(src.at[pl.ds(r * block, block)], slot, ring_sem.at[b % RING, 0])]

    def start_weights(b):
        for copy in weight_copies(b):
            copy.start()

    def wait_weights(b):
        for copy in weight_copies(b):
            copy.wait()

    def partner(i):
        offset, flip = pairs[i]
        chip = lax.rem(lax.div(me, CORES) + offset + n // CORES, n // CORES)
        return chip * CORES + lax.rem(lax.rem(me, CORES) + flip, CORES)

    def own_copy(c, src, land):
        return pltpu.make_async_copy(src.at[pl.ds(me * rows, rows)], land.at[:, pl.ds(me * chunk, chunk)], own_sem.at[c])

    def push(c, src, land, i):
        peer = partner(i)
        return pltpu.make_async_remote_copy(
            src_ref=src.at[pl.ds(peer * rows, rows)],
            dst_ref=land.at[:, pl.ds(me * chunk, chunk)],
            send_sem=send_sem.at[c, i], recv_sem=recv_sem.at[c, me],
            device_id=(group_id, peer), device_id_type=MESH)

    def arrival(c, land, source):
        return pltpu.make_async_remote_copy(
            src_ref=land.at[:, pl.ds(source * chunk, chunk)],
            dst_ref=land.at[:, pl.ds(source * chunk, chunk)],
            send_sem=send_sem.at[c, 0], recv_sem=recv_sem.at[c, source],
            device_id=(group_id, me), device_id_type=MESH)

    pl.semaphore_wait(barrier, n - 1)
    chips = n // CORES
    pairs = [(0, 1)]
    for d in range(1, (chips - 1) // 2 + 1):
        pairs += [(d, 0), (-d, 0), (d, 1), (-d, 1)]
    near = len(pairs)
    if chips % 2 == 0:
        pairs += [(chips // 2, 0), (chips // 2, 1)]
    for c, src, land, peers in ((0, k_ref, k_land, range(near)), (1, v_ref, v_land, range(near)),
                                (0, k_ref, k_land, range(near, n - 1)), (1, v_ref, v_land, range(near, n - 1))):
        for i in peers:
            push(c, src, land, i).start()
    own_copy(0, k_ref, k_land).start()
    own_copy(1, v_ref, v_land).start()
    small = [pltpu.make_async_copy(src, dst, small_sem.at[i]) for i, (src, dst) in enumerate((
        (lens_hbm, lens_ref), (x_hbm, x_ref), (gain_hbm, gain_ref), (bq_hbm, bq_ref), (bk_hbm, bk_ref), (bv_hbm, bv_ref)))]
    for copy in small:
        copy.start()
    for b in range(RING):
        start_weights(b)
    for copy in small:
        copy.wait()

    x_wide = x_ref[...].astype(jnp.float32)
    mean_sq = jnp.mean(x_wide * x_wide, axis=-1, keepdims=True)
    normed = x_wide * lax.rsqrt(mean_sq + RMS_EPS) * gain_ref[...].astype(jnp.float32).reshape(1, depth)
    h_ref[...] = jnp.concatenate([normed, jnp.zeros((LHS_ROWS - rows, depth), jnp.float32)], axis=0).astype(jnp.bfloat16)
    acc[...] = jnp.zeros_like(acc)
    acc_kv[...] = jnp.zeros_like(acc_kv)

    def multiply(lhs, slot, out, tile_count):
        def tile(t, carry):
            cols = pl.ds(pl.multiple_of(t * TILE, TILE), TILE)
            out[:, cols] += jnp.dot(lhs, ring[slot, :, cols], preferred_element_type=jnp.float32)
            return carry
        lax.fori_loop(0, tile_count, tile, 0)

    def multiply_kv(b):
        base = (b % 2) * PACK
        out = (b // 2) * kv_width
        slot = b % RING
        def part(c, carry):
            lhs = h_ref[:, pl.ds(pl.multiple_of((base + c) * block, block), block)]
            for t in range(kv_width // TILE):
                cols = pl.ds(out + t * TILE, TILE)
                src = pl.ds(pl.multiple_of(c * kv_width + t * TILE, TILE), TILE)
                acc_kv[:, cols] += jnp.dot(lhs, ring[slot, :, src], preferred_element_type=jnp.float32)
            return carry
        lax.fori_loop(0, PACK, part, 0)

    for b in range(4):
        wait_weights(b)
        multiply_kv(b)
        start_weights(b + RING)
    for b in range(4, 14):
        wait_weights(b)
        multiply(h_ref[:, pl.ds((b - 4) * block, block)], b % RING, acc, width // TILE)
        if b + RING < 14 + RING:
            start_weights(b + RING)

    lane = lax.broadcasted_iota(jnp.int32, (1, head_dim), 1)
    freq_idx = jnp.where(lane < half_dim, lane, lane - half_dim).astype(jnp.float32)
    inv_freq = jnp.exp(freq_idx * (-2.0 * math.log(ROPE_THETA) / head_dim))
    sign = jnp.where(lane < half_dim, -1.0, 1.0)
    q_bias = bq_ref[...].astype(jnp.float32).reshape(heads, head_dim)
    k_bias = bk_ref[...].astype(jnp.float32).reshape(kv_heads, head_dim)
    v_bias = bv_ref[...].astype(jnp.float32).reshape(kv_heads, head_dim)
    for s in range(rows):
        for j in range(heads):
            q_raw[s, pl.ds(j, 1), :] = acc[pl.ds(s, 1), j * head_dim:(j + 1) * head_dim]
        for j in range(kv_heads):
            k_raw[s, pl.ds(j, 1), :] = acc_kv[pl.ds(s, 1), j * head_dim:(j + 1) * head_dim]
            v_raw[s, pl.ds(j, 1), :] = acc_kv[pl.ds(s, 1), kv_width + j * head_dim:kv_width + (j + 1) * head_dim]
    for s in range(rows):
        angle = lens_ref[me * rows + s].astype(jnp.float32) * inv_freq
        cos_t = jnp.cos(angle)
        sin_t = jnp.sin(angle) * sign
        q_one = q_raw[s] + q_bias
        q_rot[s] = (q_one * cos_t + pltpu.roll(q_one, half_dim, 1) * sin_t).astype(jnp.bfloat16)
        k_one = k_raw[s] + k_bias
        k_raw[s] = (k_one * cos_t + pltpu.roll(k_one, half_dim, 1) * sin_t).astype(jnp.bfloat16).astype(jnp.float32)
        v_raw[s] = (v_raw[s] + v_bias).astype(jnp.bfloat16).astype(jnp.float32)

    row_idx = lax.broadcasted_iota(jnp.int32, (span, kv_heads, head_dim), 0)
    col = lax.broadcasted_iota(jnp.int32, (heads, chunk), 1)
    head = lax.broadcasted_iota(jnp.int32, (heads, chunk), 0)
    own_head = (col % kv_heads) == (head // group)
    col_slot = col // kv_heads
    scale = head_dim ** -0.5

    def settle(land, s, source, fresh):
        place = pl.ds(pl.multiple_of(source * chunk, chunk), chunk)
        limit = lens_ref[me * rows + s] - source * span
        old = land[s, place, :].astype(jnp.float32).reshape(span, kv_heads, head_dim)
        kept = jnp.where(row_idx < limit, old, jnp.where(row_idx == limit, fresh[s][None], 0.0))
        kept = kept.reshape(chunk, head_dim).astype(jnp.bfloat16)
        land[s, place, :] = kept
        return kept, place, limit

    def lane_fold(op, values):
        out = values[:, :head_dim]
        for t in range(1, chunk // head_dim):
            out = op(out, values[:, t * head_dim:(t + 1) * head_dim])
        return out

    def score_chunk(source):
        for s in range(rows):
            keys, place, limit = settle(k_land, s, source, k_raw)
            sc = lax.dot_general(q_rot[s], keys, (((1,), (1,)), ((), ())), preferred_element_type=jnp.float32) * scale
            sc = jnp.where(own_head & (col_slot <= limit), sc, MASKED)
            scores[s, :, place] = sc
            m_acc[s] = jnp.maximum(m_acc[s], lane_fold(jnp.maximum, sc))

    def value_chunk(source):
        for s in range(rows):
            vals, place, limit = settle(v_land, s, source, v_raw)
            e = jnp.exp(scores[s, :, place] - m_acc[s][:, :1])
            l_acc[s] += lane_fold(jnp.add, e)
            o_acc[s] += jnp.dot(e.astype(jnp.bfloat16), vals, preferred_element_type=jnp.float32)

    m_acc[...] = jnp.full_like(m_acc, MASKED)
    l_acc[...] = jnp.zeros_like(l_acc)
    o_acc[...] = jnp.zeros_like(o_acc)

    own_copy(0, k_ref, k_land).wait()
    score_chunk(me)
    for i in range(n - 1):
        source = partner(i)
        arrival(0, k_land, source).wait_recv()
        score_chunk(source)
    for s in range(rows):
        m_acc[s] = jnp.broadcast_to(jnp.max(m_acc[s], axis=-1, keepdims=True), (heads, head_dim))
    own_copy(1, v_ref, v_land).wait()
    value_chunk(me)
    for i in range(n - 1):
        source = partner(i)
        arrival(1, v_land, source).wait_recv()
        value_chunk(source)

    o_row[...] = jnp.zeros_like(o_row)
    for s in range(rows):
        l_all = jnp.sum(l_acc[s], axis=-1, keepdims=True)
        q_raw[s] = o_acc[s] / l_all
        for j in range(heads):
            o_row[pl.ds(s, 1), j * head_dim:(j + 1) * head_dim] = q_raw[s, pl.ds(j, 1), :]
    o_ref[...] = o_row[...].astype(jnp.bfloat16)
    for b in range(14, 14 + RING):
        wait_weights(b)
    for c, (src, land) in enumerate(((k_ref, k_land), (v_ref, v_land))):
        for i in range(n - 1):
            push(c, src, land, i).wait_send()


def output_kernel(first, o_ref, k_land, v_land, ring, x_hbm, wo_ref, y_ref, k_out, v_out, x_ref, extra, acc, sem):
    rows, depth = x_ref.shape
    block, width = extra.shape[1:]
    resident = ring.shape[0]
    tail = [pltpu.make_async_copy(wo_ref.at[pl.ds((resident + i) * block, block)], extra.at[i], sem.at[i])
            for i in range(extra.shape[0])]
    rest = [pltpu.make_async_copy(x_hbm, x_ref, sem.at[len(tail)]),
            pltpu.make_async_copy(k_land, k_out, sem.at[len(tail) + 1]),
            pltpu.make_async_copy(v_land, v_out, sem.at[len(tail) + 2])]
    for copy in tail + rest:
        copy.start()
    acc[...] = jnp.zeros_like(acc)

    def multiply(r, weights):
        lhs = o_ref[:, r * block:(r + 1) * block]

        for t in range(width // OUT_TILE):
            cols = slice(t * OUT_TILE, (t + 1) * OUT_TILE)
            acc[:, cols] += jnp.dot(lhs, weights[:, cols], preferred_element_type=jnp.float32)

    for r in range(resident):
        multiply(r, ring.at[(first + r) % resident])
    for i, copy in enumerate(tail):
        copy.wait()
        multiply(resident + i, extra.at[i])
    for copy in rest:
        copy.wait()
    y_ref[...] = (x_ref[...].astype(jnp.float32) + acc[:rows, :]).astype(jnp.bfloat16)


def solution(mesh):
    batch_spec = P(('dp', 'cp'))
    seq_spec = P('dp', 'cp')
    whole = P()
    n = mesh.shape['cp']

    def per_device(x_tok, prompt_lens, k_cache, v_cache, norm_gain, w_q, b_q, w_k, b_k, w_v, b_v, w_o):
        rows, depth = x_tok.shape
        batch, span, kv_heads, head_dim = k_cache.shape
        width = w_q.shape[1]
        heads = width // head_dim
        chunk = span * kv_heads
        kv_width = kv_heads * head_dim
        block = depth // 10
        dims = (n, rows, span, kv_heads, head_dim, heads)
        vmem = pl.BlockSpec(memory_space=pltpu.VMEM)
        smem = pl.BlockSpec(memory_space=pltpu.SMEM)
        hbm = pl.BlockSpec(memory_space=pl.ANY)
        bf16, f32 = jnp.bfloat16, jnp.float32
        land = (rows, n * chunk, head_dim)
        o_rows, k_all, v_all, ring = pl.pallas_call(
            functools.partial(exchange_kernel, dims),
            out_shape=(pltpu.VMEM((LHS_ROWS, width), bf16), pltpu.VMEM(land, bf16), pltpu.VMEM(land, bf16),
                       pltpu.VMEM((RING, block, width), bf16)),
            in_specs=[hbm] * 12,
            out_specs=(vmem,) * 4,
            scratch_shapes=[
                pltpu.SMEM((batch,), jnp.int32),
                pltpu.VMEM((rows, depth), bf16),
                pltpu.VMEM((depth,), bf16),
                pltpu.VMEM((width,), bf16),
                pltpu.VMEM((kv_width,), bf16),
                pltpu.VMEM((kv_width,), bf16),
                pltpu.VMEM((rows, heads, n * chunk), f32),
                pltpu.VMEM((LHS_ROWS, depth), bf16),
                pltpu.VMEM((LHS_ROWS, width), f32),
                pltpu.VMEM((LHS_ROWS, 2 * kv_width), f32),
                pltpu.VMEM((rows, heads, head_dim), f32),
                pltpu.VMEM((rows, heads, head_dim), bf16),
                pltpu.VMEM((rows, kv_heads, head_dim), f32),
                pltpu.VMEM((rows, kv_heads, head_dim), f32),
                pltpu.VMEM((rows, heads, head_dim), f32),
                pltpu.VMEM((rows, heads, head_dim), f32),
                pltpu.VMEM((rows, heads, head_dim), f32),
                pltpu.VMEM((LHS_ROWS, width), f32),
                pltpu.SemaphoreType.DMA((6,)),
                pltpu.SemaphoreType.DMA((RING, PACK)),
                pltpu.SemaphoreType.DMA((2,)),
                pltpu.SemaphoreType.DMA((2, n)),
                pltpu.SemaphoreType.DMA((2, n)),
            ],
            compiler_params=pltpu.CompilerParams(collective_id=0, has_side_effects=True, vmem_limit_bytes=8 * 1024 * 1024),
            cost_estimate=pl.CostEstimate(flops=1 << 30, bytes_accessed=1 << 27, transcendentals=0),
        )(prompt_lens, x_tok, norm_gain, b_q, b_k, b_v,
          k_cache.reshape(batch, chunk, head_dim), v_cache.reshape(batch, chunk, head_dim), w_q, w_k, w_v, w_o)
        extra = depth // block - RING
        y, k_out, v_out = pl.pallas_call(
            functools.partial(output_kernel, 14),
            out_shape=(jax.ShapeDtypeStruct((rows, depth), bf16), jax.ShapeDtypeStruct(land, bf16), jax.ShapeDtypeStruct(land, bf16)),
            in_specs=[vmem] * 4 + [hbm] * 2,
            out_specs=(vmem, hbm, hbm),
            scratch_shapes=[
                pltpu.VMEM((rows, depth), bf16),
                pltpu.VMEM((extra, block, width), bf16),
                pltpu.VMEM((LHS_ROWS, depth), f32),
                pltpu.SemaphoreType.DMA((extra + 3,)),
            ],
            compiler_params=pltpu.CompilerParams(vmem_limit_bytes=(extra * 6 + 2) * 1024 * 1024),
            cost_estimate=pl.CostEstimate(flops=1 << 30, bytes_accessed=1 << 25, transcendentals=0),
        )(*[pltpu.with_memory_space_constraint(a, pltpu.VMEM) for a in (o_rows, k_all, v_all, ring)], x_tok, w_o)
        shape = (rows, n * span, kv_heads, head_dim)
        return y, k_out.reshape(shape), v_out.reshape(shape)

    return jax.shard_map(per_device, mesh=mesh, in_specs=(batch_spec, P('dp'), seq_spec, seq_spec, whole, whole, whole, whole, whole, whole, whole, whole), out_specs=(batch_spec, batch_spec, batch_spec), check_vma=False)
```

```python
import functools
import math
import jax
import jax.numpy as jnp
from jax import lax
from jax.experimental import pallas as pl
from jax.experimental.pallas import tpu as pltpu
from jax.sharding import PartitionSpec as P

RMS_EPS = 1e-6
ROPE_THETA = 1000000.0
MASKED = -1e30
RING = 9
PACK = 5
TILE = 512
OUT_TILE = 512
LHS_ROWS = 16
CORES = 2
MESH = pl.DeviceIdType.MESH


def exchange_kernel(dims, lens_hbm, x_hbm, gain_hbm, bq_hbm, bk_hbm, bv_hbm, k_ref, v_ref, wq_ref, wk_ref, wv_ref, wo_ref,
                    o_ref, k_land, v_land, ring,
                    lens_ref, x_ref, gain_ref, bq_ref, bk_ref, bv_ref,
                    scores, h_ref, acc, acc_kv, q_raw, q_rot, k_raw, v_raw, o_acc, m_acc, l_acc, o_row,
                    small_sem, ring_sem, own_sem, send_sem, recv_sem, hop_sem):
    n, rows, span, kv_heads, head_dim, heads = dims
    group = heads // kv_heads
    width = heads * head_dim
    kv_width = kv_heads * head_dim
    chunk = span * kv_heads
    depth = x_ref.shape[1]
    half_dim = head_dim // 2
    block = depth // 10
    group_id = lax.axis_index("dp")
    me = lax.axis_index("cp")

    barrier = pltpu.get_barrier_semaphore()

    chips = n // CORES
    reach = (chips - 1) // 2
    pairs = [(0, 1)]
    for d in range(1, reach + 1):
        pairs += [(d, 0), (-d, 0), (d, 1), (-d, 1)]
    near = len(pairs)
    if chips % 2 == 0:
        pairs += [(chips // 2, 0), (chips // 2, 1)]

    def device(offset, flip):
        chip = lax.rem(lax.div(me, CORES) + offset + chips, chips)
        return chip * CORES + lax.rem(lax.rem(me, CORES) + flip, CORES)

    def partner(i):
        return device(*pairs[i])

    first = 1 + 4
    for i in range(first):
        pl.semaphore_signal(barrier, inc=1, device_id=(group_id, partner(i)), device_id_type=MESH)

    def pass_on(stage):
        for way, offset in ((0, -1), (1, 1)):
            pl.semaphore_signal(hop_sem.at[stage, way], inc=1, device_id=(group_id, device(offset, 0)), device_id_type=MESH)

    def await_stage(stage):
        for way in range(2):
            pl.semaphore_wait(hop_sem.at[stage, way], 1)

    def weight_copies(b):
        slot = ring.at[b % RING]
        if b < 4:
            src = wk_ref if b < 2 else wv_ref
            base = (b % 2) * PACK
            return [pltpu.make_async_copy(src.at[pl.ds((base + c) * block, block)],
                                          slot.at[:, pl.ds(c * kv_width, kv_width)], ring_sem.at[b % RING, c])
                    for c in range(PACK)]
        src, r = (wq_ref, b - 4) if b < 14 else (wo_ref, b - 14)
        return [pltpu.make_async_copy(src.at[pl.ds(r * block, block)], slot, ring_sem.at[b % RING, 0])]

    def start_weights(b):
        for copy in weight_copies(b):
            copy.start()

    def wait_weights(b):
        for copy in weight_copies(b):
            copy.wait()

    def own_copy(c, src, land):
        return pltpu.make_async_copy(src.at[pl.ds(me * rows, rows)], land.at[:, pl.ds(me * chunk, chunk)], own_sem.at[c])

    def push(c, src, land, i):
        peer = partner(i)
        return pltpu.make_async_remote_copy(
            src_ref=src.at[pl.ds(peer * rows, rows)],
            dst_ref=land.at[:, pl.ds(me * chunk, chunk)],
            send_sem=send_sem.at[c, i], recv_sem=recv_sem.at[c, me],
            device_id=(group_id, peer), device_id_type=MESH)

    def arrival(c, land, source):
        return pltpu.make_async_remote_copy(
            src_ref=land.at[:, pl.ds(source * chunk, chunk)],
            dst_ref=land.at[:, pl.ds(source * chunk, chunk)],
            send_sem=send_sem.at[c, 0], recv_sem=recv_sem.at[c, source],
            device_id=(group_id, me), device_id_type=MESH)

    def push_all(c, peers):
        src, land = ((k_ref, k_land), (v_ref, v_land))[c]
        for i in peers:
            push(c, src, land, i).start()

    pl.semaphore_wait(barrier, first)
    push_all(0, range(first))
    pass_on(2)
    own_copy(0, k_ref, k_land).start()
    own_copy(1, v_ref, v_land).start()
    small = [pltpu.make_async_copy(src, dst, small_sem.at[i]) for i, (src, dst) in enumerate((
        (lens_hbm, lens_ref), (x_hbm, x_ref), (gain_hbm, gain_ref), (bq_hbm, bq_ref), (bk_hbm, bk_ref), (bv_hbm, bv_ref)))]
    for copy in small:
        copy.start()
    for b in range(RING):
        start_weights(b)
    for stage in range(2, chips // 2 + 1):
        await_stage(stage)
        if stage < chips // 2:
            pass_on(stage + 1)
        if stage <= reach:
            push_all(0, range(1 + 4 * (stage - 1), 1 + 4 * stage))
    push_all(1, range(near))
    push_all(0, range(near, n - 1))
    push_all(1, range(near, n - 1))
    for copy in small:
        copy.wait()

    x_wide = x_ref[...].astype(jnp.float32)
    mean_sq = jnp.mean(x_wide * x_wide, axis=-1, keepdims=True)
    normed = x_wide * lax.rsqrt(mean_sq + RMS_EPS) * gain_ref[...].astype(jnp.float32).reshape(1, depth)
    h_ref[...] = jnp.concatenate([normed, jnp.zeros((LHS_ROWS - rows, depth), jnp.float32)], axis=0).astype(jnp.bfloat16)
    acc[...] = jnp.zeros_like(acc)
    acc_kv[...] = jnp.zeros_like(acc_kv)

    def multiply(lhs, slot, out, tile_count):
        def tile(t, carry):
            cols = pl.ds(pl.multiple_of(t * TILE, TILE), TILE)
            out[:, cols] += jnp.dot(lhs, ring[slot, :, cols], preferred_element_type=jnp.float32)
            return carry
        lax.fori_loop(0, tile_count, tile, 0)

    def multiply_kv(b):
        base = (b % 2) * PACK
        out = (b // 2) * kv_width
        slot = b % RING
        def part(c, carry):
            lhs = h_ref[:, pl.ds(pl.multiple_of((base + c) * block, block), block)]
            for t in range(kv_width // TILE):
                cols = pl.ds(out + t * TILE, TILE)
                src = pl.ds(pl.multiple_of(c * kv_width + t * TILE, TILE), TILE)
                acc_kv[:, cols] += jnp.dot(lhs, ring[slot, :, src], preferred_element_type=jnp.float32)
            return carry
        lax.fori_loop(0, PACK, part, 0)

    for b in range(4):
        wait_weights(b)
        multiply_kv(b)
        start_weights(b + RING)
    for b in range(4, 14):
        wait_weights(b)
        multiply(h_ref[:, pl.ds((b - 4) * block, block)], b % RING, acc, width // TILE)
        if b + RING < 14 + RING:
            start_weights(b + RING)

    lane = lax.broadcasted_iota(jnp.int32, (1, head_dim), 1)
    freq_idx = jnp.where(lane < half_dim, lane, lane - half_dim).astype(jnp.float32)
    inv_freq = jnp.exp(freq_idx * (-2.0 * math.log(ROPE_THETA) / head_dim))
    sign = jnp.where(lane < half_dim, -1.0, 1.0)
    q_bias = bq_ref[...].astype(jnp.float32).reshape(heads, head_dim)
    k_bias = bk_ref[...].astype(jnp.float32).reshape(kv_heads, head_dim)
    v_bias = bv_ref[...].astype(jnp.float32).reshape(kv_heads, head_dim)
    for s in range(rows):
        for j in range(heads):
            q_raw[s, pl.ds(j, 1), :] = acc[pl.ds(s, 1), j * head_dim:(j + 1) * head_dim]
        for j in range(kv_heads):
            k_raw[s, pl.ds(j, 1), :] = acc_kv[pl.ds(s, 1), j * head_dim:(j + 1) * head_dim]
            v_raw[s, pl.ds(j, 1), :] = acc_kv[pl.ds(s, 1), kv_width + j * head_dim:kv_width + (j + 1) * head_dim]
    for s in range(rows):
        angle = lens_ref[me * rows + s].astype(jnp.float32) * inv_freq
        cos_t = jnp.cos(angle)
        sin_t = jnp.sin(angle) * sign
        q_one = q_raw[s] + q_bias
        q_rot[s] = (q_one * cos_t + pltpu.roll(q_one, half_dim, 1) * sin_t).astype(jnp.bfloat16)
        k_one = k_raw[s] + k_bias
        k_raw[s] = (k_one * cos_t + pltpu.roll(k_one, half_dim, 1) * sin_t).astype(jnp.bfloat16).astype(jnp.float32)
        v_raw[s] = (v_raw[s] + v_bias).astype(jnp.bfloat16).astype(jnp.float32)

    row_idx = lax.broadcasted_iota(jnp.int32, (span, kv_heads, head_dim), 0)
    col = lax.broadcasted_iota(jnp.int32, (heads, chunk), 1)
    head = lax.broadcasted_iota(jnp.int32, (heads, chunk), 0)
    own_head = (col % kv_heads) == (head // group)
    col_slot = col // kv_heads
    scale = head_dim ** -0.5

    def settle(land, s, source, fresh):
        place = pl.ds(pl.multiple_of(source * chunk, chunk), chunk)
        limit = lens_ref[me * rows + s] - source * span
        old = land[s, place, :].astype(jnp.float32).reshape(span, kv_heads, head_dim)
        kept = jnp.where(row_idx < limit, old, jnp.where(row_idx == limit, fresh[s][None], 0.0))
        kept = kept.reshape(chunk, head_dim).astype(jnp.bfloat16)
        land[s, place, :] = kept
        return kept, place, limit

    def lane_fold(op, values):
        out = values[:, :head_dim]
        for t in range(1, chunk // head_dim):
            out = op(out, values[:, t * head_dim:(t + 1) * head_dim])
        return out

    def score_chunk(source):
        for s in range(rows):
            keys, place, limit = settle(k_land, s, source, k_raw)
            sc = lax.dot_general(q_rot[s], keys, (((1,), (1,)), ((), ())), preferred_element_type=jnp.float32) * scale
            sc = jnp.where(own_head & (col_slot <= limit), sc, MASKED)
            scores[s, :, place] = sc
            m_acc[s] = jnp.maximum(m_acc[s], lane_fold(jnp.maximum, sc))

    def value_chunk(source):
        for s in range(rows):
            vals, place, limit = settle(v_land, s, source, v_raw)
            e = jnp.exp(scores[s, :, place] - m_acc[s][:, :1])
            l_acc[s] += lane_fold(jnp.add, e)
            o_acc[s] += jnp.dot(e.astype(jnp.bfloat16), vals, preferred_element_type=jnp.float32)

    m_acc[...] = jnp.full_like(m_acc, MASKED)
    l_acc[...] = jnp.zeros_like(l_acc)
    o_acc[...] = jnp.zeros_like(o_acc)

    own_copy(0, k_ref, k_land).wait()
    score_chunk(me)
    for i in range(n - 1):
        source = partner(i)
        arrival(0, k_land, source).wait_recv()
        score_chunk(source)
    for s in range(rows):
        m_acc[s] = jnp.broadcast_to(jnp.max(m_acc[s], axis=-1, keepdims=True), (heads, head_dim))
    own_copy(1, v_ref, v_land).wait()
    value_chunk(me)
    for i in range(n - 1):
        source = partner(i)
        arrival(1, v_land, source).wait_recv()
        value_chunk(source)

    o_row[...] = jnp.zeros_like(o_row)
    for s in range(rows):
        l_all = jnp.sum(l_acc[s], axis=-1, keepdims=True)
        q_raw[s] = o_acc[s] / l_all
        for j in range(heads):
            o_row[pl.ds(s, 1), j * head_dim:(j + 1) * head_dim] = q_raw[s, pl.ds(j, 1), :]
    o_ref[...] = o_row[...].astype(jnp.bfloat16)
    for b in range(14, 14 + RING):
        wait_weights(b)
    for c, (src, land) in enumerate(((k_ref, k_land), (v_ref, v_land))):
        for i in range(n - 1):
            push(c, src, land, i).wait_send()


def output_kernel(first, o_ref, k_land, v_land, ring, x_hbm, wo_ref, y_ref, k_out, v_out, x_ref, extra, acc, sem):
    rows, depth = x_ref.shape
    block, width = extra.shape[1:]
    resident = ring.shape[0]
    tail = [pltpu.make_async_copy(wo_ref.at[pl.ds((resident + i) * block, block)], extra.at[i], sem.at[i])
            for i in range(extra.shape[0])]
    rest = [pltpu.make_async_copy(x_hbm, x_ref, sem.at[len(tail)]),
            pltpu.make_async_copy(k_land, k_out, sem.at[len(tail) + 1]),
            pltpu.make_async_copy(v_land, v_out, sem.at[len(tail) + 2])]
    for copy in tail + rest:
        copy.start()
    acc[...] = jnp.zeros_like(acc)

    def multiply(r, weights):
        lhs = o_ref[:, r * block:(r + 1) * block]

        for t in range(width // OUT_TILE):
            cols = slice(t * OUT_TILE, (t + 1) * OUT_TILE)
            acc[:, cols] += jnp.dot(lhs, weights[:, cols], preferred_element_type=jnp.float32)

    for r in range(resident):
        multiply(r, ring.at[(first + r) % resident])
    for i, copy in enumerate(tail):
        copy.wait()
        multiply(resident + i, extra.at[i])
    for copy in rest:
        copy.wait()
    y_ref[...] = (x_ref[...].astype(jnp.float32) + acc[:rows, :]).astype(jnp.bfloat16)


def solution(mesh):
    batch_spec = P(('dp', 'cp'))
    seq_spec = P('dp', 'cp')
    whole = P()
    n = mesh.shape['cp']

    def per_device(x_tok, prompt_lens, k_cache, v_cache, norm_gain, w_q, b_q, w_k, b_k, w_v, b_v, w_o):
        rows, depth = x_tok.shape
        batch, span, kv_heads, head_dim = k_cache.shape
        width = w_q.shape[1]
        heads = width // head_dim
        chunk = span * kv_heads
        kv_width = kv_heads * head_dim
        block = depth // 10
        dims = (n, rows, span, kv_heads, head_dim, heads)
        vmem = pl.BlockSpec(memory_space=pltpu.VMEM)
        smem = pl.BlockSpec(memory_space=pltpu.SMEM)
        hbm = pl.BlockSpec(memory_space=pl.ANY)
        bf16, f32 = jnp.bfloat16, jnp.float32
        land = (rows, n * chunk, head_dim)
        o_rows, k_all, v_all, ring = pl.pallas_call(
            functools.partial(exchange_kernel, dims),
            out_shape=(pltpu.VMEM((LHS_ROWS, width), bf16), pltpu.VMEM(land, bf16), pltpu.VMEM(land, bf16),
                       pltpu.VMEM((RING, block, width), bf16)),
            in_specs=[hbm] * 12,
            out_specs=(vmem,) * 4,
            scratch_shapes=[
                pltpu.SMEM((batch,), jnp.int32),
                pltpu.VMEM((rows, depth), bf16),
                pltpu.VMEM((depth,), bf16),
                pltpu.VMEM((width,), bf16),
                pltpu.VMEM((kv_width,), bf16),
                pltpu.VMEM((kv_width,), bf16),
                pltpu.VMEM((rows, heads, n * chunk), f32),
                pltpu.VMEM((LHS_ROWS, depth), bf16),
                pltpu.VMEM((LHS_ROWS, width), f32),
                pltpu.VMEM((LHS_ROWS, 2 * kv_width), f32),
                pltpu.VMEM((rows, heads, head_dim), f32),
                pltpu.VMEM((rows, heads, head_dim), bf16),
                pltpu.VMEM((rows, kv_heads, head_dim), f32),
                pltpu.VMEM((rows, kv_heads, head_dim), f32),
                pltpu.VMEM((rows, heads, head_dim), f32),
                pltpu.VMEM((rows, heads, head_dim), f32),
                pltpu.VMEM((rows, heads, head_dim), f32),
                pltpu.VMEM((LHS_ROWS, width), f32),
                pltpu.SemaphoreType.DMA((6,)),
                pltpu.SemaphoreType.DMA((RING, PACK)),
                pltpu.SemaphoreType.DMA((2,)),
                pltpu.SemaphoreType.DMA((2, n)),
                pltpu.SemaphoreType.DMA((2, n)),
                pltpu.SemaphoreType.REGULAR((n // CORES // 2 + 1, 2)),
            ],
            compiler_params=pltpu.CompilerParams(collective_id=0, has_side_effects=True, vmem_limit_bytes=8 * 1024 * 1024),
            cost_estimate=pl.CostEstimate(flops=1 << 30, bytes_accessed=1 << 27, transcendentals=0),
        )(prompt_lens, x_tok, norm_gain, b_q, b_k, b_v,
          k_cache.reshape(batch, chunk, head_dim), v_cache.reshape(batch, chunk, head_dim), w_q, w_k, w_v, w_o)
        extra = depth // block - RING
        y, k_out, v_out = pl.pallas_call(
            functools.partial(output_kernel, 14),
            out_shape=(jax.ShapeDtypeStruct((rows, depth), bf16), jax.ShapeDtypeStruct(land, bf16), jax.ShapeDtypeStruct(land, bf16)),
            in_specs=[vmem] * 4 + [hbm] * 2,
            out_specs=(vmem, hbm, hbm),
            scratch_shapes=[
                pltpu.VMEM((rows, depth), bf16),
                pltpu.VMEM((extra, block, width), bf16),
                pltpu.VMEM((LHS_ROWS, depth), f32),
                pltpu.SemaphoreType.DMA((extra + 3,)),
            ],
            compiler_params=pltpu.CompilerParams(vmem_limit_bytes=(extra * 6 + 2) * 1024 * 1024),
            cost_estimate=pl.CostEstimate(flops=1 << 30, bytes_accessed=1 << 25, transcendentals=0),
        )(*[pltpu.with_memory_space_constraint(a, pltpu.VMEM) for a in (o_rows, k_all, v_all, ring)], x_tok, w_o)
        shape = (rows, n * span, kv_heads, head_dim)
        return y, k_out.reshape(shape), v_out.reshape(shape)

    return jax.shard_map(per_device, mesh=mesh, in_specs=(batch_spec, P('dp'), seq_spec, seq_spec, whole, whole, whole, whole, whole, whole, whole, whole), out_specs=(batch_spec, batch_spec, batch_spec), check_vma=False)
```

```python
import functools
import math
import jax
import jax.numpy as jnp
from jax import lax
from jax.experimental import pallas as pl
from jax.experimental.pallas import tpu as pltpu
from jax.sharding import PartitionSpec as P

RMS_EPS = 1e-6
ROPE_THETA = 1000000.0
MASKED = -1e30
RING = 9
PACK = 5
TILE = 512
OUT_TILE = 512
LHS_ROWS = 16
CORES = 2
MESH = pl.DeviceIdType.MESH


def exchange_kernel(dims, lens_hbm, x_hbm, gain_hbm, bq_hbm, bk_hbm, bv_hbm, k_ref, v_ref, wq_ref, wk_ref, wv_ref, wo_ref,
                    o_ref, k_land, v_land, ring,
                    lens_ref, x_ref, gain_ref, bq_ref, bk_ref, bv_ref,
                    scores, h_ref, acc, acc_kv, q_raw, q_rot, k_raw, v_raw, o_acc, m_acc, l_acc, o_row,
                    small_sem, ring_sem, own_sem, send_sem, recv_sem):
    n, rows, span, kv_heads, head_dim, heads = dims
    group = heads // kv_heads
    width = heads * head_dim
    kv_width = kv_heads * head_dim
    chunk = span * kv_heads
    depth = x_ref.shape[1]
    half_dim = head_dim // 2
    block = depth // 10
    group_id = lax.axis_index("dp")
    me = lax.axis_index("cp")

    barrier = pltpu.get_barrier_semaphore()

    def greet(d, carry):
        peer = lax.rem(me + d, n)
        pl.semaphore_signal(barrier, inc=1, device_id=(group_id, peer), device_id_type=MESH)
        return carry

    lax.fori_loop(1, n, greet, 0)

    def weight_copies(b):
        slot = ring.at[b % RING]
        if b < 4:
            src = wk_ref if b < 2 else wv_ref
            base = (b % 2) * PACK
            return [pltpu.make_async_copy(src.at[pl.ds((base + c) * block, block)],
                                          slot.at[:, pl.ds(c * kv_width, kv_width)], ring_sem.at[b % RING, c])
                    for c in range(PACK)]
        src, r = (wq_ref, b - 4) if b < 14 else (wo_ref, b - 14)
        return [pltpu.make_async_copy(src.at[pl.ds(r * block, block)], slot, ring_sem.at[b % RING, 0])]

    def start_weights(b):
        for copy in weight_copies(b):
            copy.start()

    def wait_weights(b):
        for copy in weight_copies(b):
            copy.wait()

    def partner(i):
        offset, flip = pairs[i]
        chip = lax.rem(lax.div(me, CORES) + offset + n // CORES, n // CORES)
        return chip * CORES + lax.rem(lax.rem(me, CORES) + flip, CORES)

    def own_copy(c, src, land):
        return pltpu.make_async_copy(src.at[pl.ds(me * rows, rows)], land.at[:, pl.ds(me * chunk, chunk)], own_sem.at[c])

    def push(c, src, land, i):
        peer = partner(i)
        return pltpu.make_async_remote_copy(
            src_ref=src.at[pl.ds(peer * rows, rows)],
            dst_ref=land.at[:, pl.ds(me * chunk, chunk)],
            send_sem=send_sem.at[c, i], recv_sem=recv_sem.at[c, me],
            device_id=(group_id, peer), device_id_type=MESH)

    def arrival(c, land, source):
        return pltpu.make_async_remote_copy(
            src_ref=land.at[:, pl.ds(source * chunk, chunk)],
            dst_ref=land.at[:, pl.ds(source * chunk, chunk)],
            send_sem=send_sem.at[c, 0], recv_sem=recv_sem.at[c, source],
            device_id=(group_id, me), device_id_type=MESH)

    pl.semaphore_wait(barrier, n - 1)
    chips = n // CORES
    pairs = [(0, 1)]
    for d in range(1, (chips - 1) // 2 + 1):
        pairs += [(d, 0), (-d, 0), (d, 1), (-d, 1)]
    near = len(pairs)
    if chips % 2 == 0:
        pairs += [(chips // 2, 0), (chips // 2, 1)]
    outward = list(range(n - 1))
    inward = [0]
    for first in range(near, n - 1, 4):
        inward += range(first, min(first + 4, n - 1))
    for first in range(near - 4, 0, -4):
        inward += range(first, first + 4)
    for i in outward:
        push(0, k_ref, k_land, i).start()
    for i in inward:
        push(1, v_ref, v_land, i).start()
    own_copy(0, k_ref, k_land).start()
    own_copy(1, v_ref, v_land).start()
    small = [pltpu.make_async_copy(src, dst, small_sem.at[i]) for i, (src, dst) in enumerate((
        (lens_hbm, lens_ref), (x_hbm, x_ref), (gain_hbm, gain_ref), (bq_hbm, bq_ref), (bk_hbm, bk_ref), (bv_hbm, bv_ref)))]
    for copy in small:
        copy.start()
    for b in range(RING):
        start_weights(b)
    for copy in small:
        copy.wait()

    x_wide = x_ref[...].astype(jnp.float32)
    mean_sq = jnp.mean(x_wide * x_wide, axis=-1, keepdims=True)
    normed = x_wide * lax.rsqrt(mean_sq + RMS_EPS) * gain_ref[...].astype(jnp.float32).reshape(1, depth)
    h_ref[...] = jnp.concatenate([normed, jnp.zeros((LHS_ROWS - rows, depth), jnp.float32)], axis=0).astype(jnp.bfloat16)
    acc[...] = jnp.zeros_like(acc)
    acc_kv[...] = jnp.zeros_like(acc_kv)

    def multiply(lhs, slot, out, tile_count):
        def tile(t, carry):
            cols = pl.ds(pl.multiple_of(t * TILE, TILE), TILE)
            out[:, cols] += jnp.dot(lhs, ring[slot, :, cols], preferred_element_type=jnp.float32)
            return carry
        lax.fori_loop(0, tile_count, tile, 0)

    def multiply_kv(b):
        base = (b % 2) * PACK
        out = (b // 2) * kv_width
        slot = b % RING
        def part(c, carry):
            lhs = h_ref[:, pl.ds(pl.multiple_of((base + c) * block, block), block)]
            for t in range(kv_width // TILE):
                cols = pl.ds(out + t * TILE, TILE)
                src = pl.ds(pl.multiple_of(c * kv_width + t * TILE, TILE), TILE)
                acc_kv[:, cols] += jnp.dot(lhs, ring[slot, :, src], preferred_element_type=jnp.float32)
            return carry
        lax.fori_loop(0, PACK, part, 0)

    for b in range(4):
        wait_weights(b)
        multiply_kv(b)
        start_weights(b + RING)
    for b in range(4, 14):
        wait_weights(b)
        multiply(h_ref[:, pl.ds((b - 4) * block, block)], b % RING, acc, width // TILE)
        if b + RING < 14 + RING:
            start_weights(b + RING)

    lane = lax.broadcasted_iota(jnp.int32, (1, head_dim), 1)
    freq_idx = jnp.where(lane < half_dim, lane, lane - half_dim).astype(jnp.float32)
    inv_freq = jnp.exp(freq_idx * (-2.0 * math.log(ROPE_THETA) / head_dim))
    sign = jnp.where(lane < half_dim, -1.0, 1.0)
    q_bias = bq_ref[...].astype(jnp.float32).reshape(heads, head_dim)
    k_bias = bk_ref[...].astype(jnp.float32).reshape(kv_heads, head_dim)
    v_bias = bv_ref[...].astype(jnp.float32).reshape(kv_heads, head_dim)
    for s in range(rows):
        for j in range(heads):
            q_raw[s, pl.ds(j, 1), :] = acc[pl.ds(s, 1), j * head_dim:(j + 1) * head_dim]
        for j in range(kv_heads):
            k_raw[s, pl.ds(j, 1), :] = acc_kv[pl.ds(s, 1), j * head_dim:(j + 1) * head_dim]
            v_raw[s, pl.ds(j, 1), :] = acc_kv[pl.ds(s, 1), kv_width + j * head_dim:kv_width + (j + 1) * head_dim]
    for s in range(rows):
        angle = lens_ref[me * rows + s].astype(jnp.float32) * inv_freq
        cos_t = jnp.cos(angle)
        sin_t = jnp.sin(angle) * sign
        q_one = q_raw[s] + q_bias
        q_rot[s] = (q_one * cos_t + pltpu.roll(q_one, half_dim, 1) * sin_t).astype(jnp.bfloat16)
        k_one = k_raw[s] + k_bias
        k_raw[s] = (k_one * cos_t + pltpu.roll(k_one, half_dim, 1) * sin_t).astype(jnp.bfloat16).astype(jnp.float32)
        v_raw[s] = (v_raw[s] + v_bias).astype(jnp.bfloat16).astype(jnp.float32)

    row_idx = lax.broadcasted_iota(jnp.int32, (span, kv_heads, head_dim), 0)
    col = lax.broadcasted_iota(jnp.int32, (heads, chunk), 1)
    head = lax.broadcasted_iota(jnp.int32, (heads, chunk), 0)
    own_head = (col % kv_heads) == (head // group)
    col_slot = col // kv_heads
    scale = head_dim ** -0.5

    def settle(land, s, source, fresh):
        place = pl.ds(pl.multiple_of(source * chunk, chunk), chunk)
        limit = lens_ref[me * rows + s] - source * span
        old = land[s, place, :].astype(jnp.float32).reshape(span, kv_heads, head_dim)
        kept = jnp.where(row_idx < limit, old, jnp.where(row_idx == limit, fresh[s][None], 0.0))
        kept = kept.reshape(chunk, head_dim).astype(jnp.bfloat16)
        land[s, place, :] = kept
        return kept, place, limit

    def lane_fold(op, values):
        out = values[:, :head_dim]
        for t in range(1, chunk // head_dim):
            out = op(out, values[:, t * head_dim:(t + 1) * head_dim])
        return out

    def score_chunk(source):
        for s in range(rows):
            keys, place, limit = settle(k_land, s, source, k_raw)
            sc = lax.dot_general(q_rot[s], keys, (((1,), (1,)), ((), ())), preferred_element_type=jnp.float32) * scale
            sc = jnp.where(own_head & (col_slot <= limit), sc, MASKED)
            scores[s, :, place] = sc
            m_acc[s] = jnp.maximum(m_acc[s], lane_fold(jnp.maximum, sc))

    def value_chunk(source):
        for s in range(rows):
            vals, place, limit = settle(v_land, s, source, v_raw)
            e = jnp.exp(scores[s, :, place] - m_acc[s][:, :1])
            l_acc[s] += lane_fold(jnp.add, e)
            o_acc[s] += jnp.dot(e.astype(jnp.bfloat16), vals, preferred_element_type=jnp.float32)

    m_acc[...] = jnp.full_like(m_acc, MASKED)
    l_acc[...] = jnp.zeros_like(l_acc)
    o_acc[...] = jnp.zeros_like(o_acc)

    own_copy(0, k_ref, k_land).wait()
    score_chunk(me)
    for i in outward:
        source = partner(i)
        arrival(0, k_land, source).wait_recv()
        score_chunk(source)
    for s in range(rows):
        m_acc[s] = jnp.broadcast_to(jnp.max(m_acc[s], axis=-1, keepdims=True), (heads, head_dim))
    own_copy(1, v_ref, v_land).wait()
    value_chunk(me)
    for i in inward:
        source = partner(i)
        arrival(1, v_land, source).wait_recv()
        value_chunk(source)

    o_row[...] = jnp.zeros_like(o_row)
    for s in range(rows):
        l_all = jnp.sum(l_acc[s], axis=-1, keepdims=True)
        q_raw[s] = o_acc[s] / l_all
        for j in range(heads):
            o_row[pl.ds(s, 1), j * head_dim:(j + 1) * head_dim] = q_raw[s, pl.ds(j, 1), :]
    o_ref[...] = o_row[...].astype(jnp.bfloat16)
    for b in range(14, 14 + RING):
        wait_weights(b)
    for c, (src, land) in enumerate(((k_ref, k_land), (v_ref, v_land))):
        for i in range(n - 1):
            push(c, src, land, i).wait_send()


def output_kernel(first, o_ref, k_land, v_land, ring, x_hbm, wo_ref, y_ref, k_out, v_out, x_ref, extra, acc, sem):
    rows, depth = x_ref.shape
    block, width = extra.shape[1:]
    resident = ring.shape[0]
    tail = [pltpu.make_async_copy(wo_ref.at[pl.ds((resident + i) * block, block)], extra.at[i], sem.at[i])
            for i in range(extra.shape[0])]
    rest = [pltpu.make_async_copy(x_hbm, x_ref, sem.at[len(tail)]),
            pltpu.make_async_copy(k_land, k_out, sem.at[len(tail) + 1]),
            pltpu.make_async_copy(v_land, v_out, sem.at[len(tail) + 2])]
    for copy in tail + rest:
        copy.start()
    acc[...] = jnp.zeros_like(acc)

    def multiply(r, weights):
        lhs = o_ref[:, r * block:(r + 1) * block]

        for t in range(width // OUT_TILE):
            cols = slice(t * OUT_TILE, (t + 1) * OUT_TILE)
            acc[:, cols] += jnp.dot(lhs, weights[:, cols], preferred_element_type=jnp.float32)

    for r in range(resident):
        multiply(r, ring.at[(first + r) % resident])
    for i, copy in enumerate(tail):
        copy.wait()
        multiply(resident + i, extra.at[i])
    for copy in rest:
        copy.wait()
    y_ref[...] = (x_ref[...].astype(jnp.float32) + acc[:rows, :]).astype(jnp.bfloat16)


def solution(mesh):
    batch_spec = P(('dp', 'cp'))
    seq_spec = P('dp', 'cp')
    whole = P()
    n = mesh.shape['cp']

    def per_device(x_tok, prompt_lens, k_cache, v_cache, norm_gain, w_q, b_q, w_k, b_k, w_v, b_v, w_o):
        rows, depth = x_tok.shape
        batch, span, kv_heads, head_dim = k_cache.shape
        width = w_q.shape[1]
        heads = width // head_dim
        chunk = span * kv_heads
        kv_width = kv_heads * head_dim
        block = depth // 10
        dims = (n, rows, span, kv_heads, head_dim, heads)
        vmem = pl.BlockSpec(memory_space=pltpu.VMEM)
        smem = pl.BlockSpec(memory_space=pltpu.SMEM)
        hbm = pl.BlockSpec(memory_space=pl.ANY)
        bf16, f32 = jnp.bfloat16, jnp.float32
        land = (rows, n * chunk, head_dim)
        o_rows, k_all, v_all, ring = pl.pallas_call(
            functools.partial(exchange_kernel, dims),
            out_shape=(pltpu.VMEM((LHS_ROWS, width), bf16), pltpu.VMEM(land, bf16), pltpu.VMEM(land, bf16),
                       pltpu.VMEM((RING, block, width), bf16)),
            in_specs=[hbm] * 12,
            out_specs=(vmem,) * 4,
            scratch_shapes=[
                pltpu.SMEM((batch,), jnp.int32),
                pltpu.VMEM((rows, depth), bf16),
                pltpu.VMEM((depth,), bf16),
                pltpu.VMEM((width,), bf16),
                pltpu.VMEM((kv_width,), bf16),
                pltpu.VMEM((kv_width,), bf16),
                pltpu.VMEM((rows, heads, n * chunk), f32),
                pltpu.VMEM((LHS_ROWS, depth), bf16),
                pltpu.VMEM((LHS_ROWS, width), f32),
                pltpu.VMEM((LHS_ROWS, 2 * kv_width), f32),
                pltpu.VMEM((rows, heads, head_dim), f32),
                pltpu.VMEM((rows, heads, head_dim), bf16),
                pltpu.VMEM((rows, kv_heads, head_dim), f32),
                pltpu.VMEM((rows, kv_heads, head_dim), f32),
                pltpu.VMEM((rows, heads, head_dim), f32),
                pltpu.VMEM((rows, heads, head_dim), f32),
                pltpu.VMEM((rows, heads, head_dim), f32),
                pltpu.VMEM((LHS_ROWS, width), f32),
                pltpu.SemaphoreType.DMA((6,)),
                pltpu.SemaphoreType.DMA((RING, PACK)),
                pltpu.SemaphoreType.DMA((2,)),
                pltpu.SemaphoreType.DMA((2, n)),
                pltpu.SemaphoreType.DMA((2, n)),
            ],
            compiler_params=pltpu.CompilerParams(collective_id=0, has_side_effects=True, vmem_limit_bytes=8 * 1024 * 1024),
            cost_estimate=pl.CostEstimate(flops=1 << 30, bytes_accessed=1 << 27, transcendentals=0),
        )(prompt_lens, x_tok, norm_gain, b_q, b_k, b_v,
          k_cache.reshape(batch, chunk, head_dim), v_cache.reshape(batch, chunk, head_dim), w_q, w_k, w_v, w_o)
        extra = depth // block - RING
        y, k_out, v_out = pl.pallas_call(
            functools.partial(output_kernel, 14),
            out_shape=(jax.ShapeDtypeStruct((rows, depth), bf16), jax.ShapeDtypeStruct(land, bf16), jax.ShapeDtypeStruct(land, bf16)),
            in_specs=[vmem] * 4 + [hbm] * 2,
            out_specs=(vmem, hbm, hbm),
            scratch_shapes=[
                pltpu.VMEM((rows, depth), bf16),
                pltpu.VMEM((extra, block, width), bf16),
                pltpu.VMEM((LHS_ROWS, depth), f32),
                pltpu.SemaphoreType.DMA((extra + 3,)),
            ],
            compiler_params=pltpu.CompilerParams(vmem_limit_bytes=(extra * 6 + 2) * 1024 * 1024),
            cost_estimate=pl.CostEstimate(flops=1 << 30, bytes_accessed=1 << 25, transcendentals=0),
        )(*[pltpu.with_memory_space_constraint(a, pltpu.VMEM) for a in (o_rows, k_all, v_all, ring)], x_tok, w_o)
        shape = (rows, n * span, kv_heads, head_dim)
        return y, k_out.reshape(shape), v_out.reshape(shape)

    return jax.shard_map(per_device, mesh=mesh, in_specs=(batch_spec, P('dp'), seq_spec, seq_spec, whole, whole, whole, whole, whole, whole, whole, whole), out_specs=(batch_spec, batch_spec, batch_spec), check_vma=False)
```

```python
import functools
import math
import jax
import jax.numpy as jnp
from jax import lax
from jax.experimental import pallas as pl
from jax.experimental.pallas import tpu as pltpu
from jax.sharding import PartitionSpec as P

RMS_EPS = 1e-6
ROPE_THETA = 1000000.0
MASKED = -1e30
RING = 9
PACK = 5
TILE = 512
OUT_TILE = 512
LHS_ROWS = 16
CORES = 2
MESH = pl.DeviceIdType.MESH


def exchange_kernel(dims, lens_hbm, x_hbm, gain_hbm, bq_hbm, bk_hbm, bv_hbm, k_ref, v_ref, wq_ref, wk_ref, wv_ref, wo_ref,
                    o_ref, k_land, v_land, ring,
                    lens_ref, x_ref, gain_ref, bq_ref, bk_ref, bv_ref,
                    scores, h_ref, acc, acc_kv, q_raw, q_rot, k_raw, v_raw, o_acc, m_acc, l_acc, o_row,
                    small_sem, ring_sem, own_sem, send_sem, recv_sem, hop_sem):
    n, rows, span, kv_heads, head_dim, heads = dims
    group = heads // kv_heads
    width = heads * head_dim
    kv_width = kv_heads * head_dim
    chunk = span * kv_heads
    depth = x_ref.shape[1]
    half_dim = head_dim // 2
    block = depth // 10
    group_id = lax.axis_index("dp")
    me = lax.axis_index("cp")

    barrier = pltpu.get_barrier_semaphore()

    chips = n // CORES
    reach = (chips - 1) // 2
    pairs = [(0, 1)]
    for d in range(1, reach + 1):
        pairs += [(d, 0), (-d, 0), (d, 1), (-d, 1)]
    near = len(pairs)
    if chips % 2 == 0:
        pairs += [(chips // 2, 0), (chips // 2, 1)]

    def device(offset, flip):
        chip = lax.rem(lax.div(me, CORES) + offset + chips, chips)
        return chip * CORES + lax.rem(lax.rem(me, CORES) + flip, CORES)

    def partner(i):
        return device(*pairs[i])

    first = 1 + 4
    for i in range(first):
        pl.semaphore_signal(barrier, inc=1, device_id=(group_id, partner(i)), device_id_type=MESH)

    def pass_on(stage):
        for way, offset in ((0, -1), (1, 1)):
            pl.semaphore_signal(hop_sem.at[stage, way], inc=1, device_id=(group_id, device(offset, 0)), device_id_type=MESH)

    def await_stage(stage):
        for way in range(2):
            pl.semaphore_wait(hop_sem.at[stage, way], 1)

    def weight_copies(b):
        slot = ring.at[b % RING]
        if b < 4:
            src = wk_ref if b < 2 else wv_ref
            base = (b % 2) * PACK
            return [pltpu.make_async_copy(src.at[pl.ds((base + c) * block, block)],
                                          slot.at[:, pl.ds(c * kv_width, kv_width)], ring_sem.at[b % RING, c])
                    for c in range(PACK)]
        src, r = (wq_ref, b - 4) if b < 14 else (wo_ref, b - 14)
        return [pltpu.make_async_copy(src.at[pl.ds(r * block, block)], slot, ring_sem.at[b % RING, 0])]

    def start_weights(b):
        for copy in weight_copies(b):
            copy.start()

    def wait_weights(b):
        for copy in weight_copies(b):
            copy.wait()

    def own_copy(c, src, land):
        return pltpu.make_async_copy(src.at[pl.ds(me * rows, rows)], land.at[:, pl.ds(me * chunk, chunk)], own_sem.at[c])

    def push(c, src, land, i):
        peer = partner(i)
        return pltpu.make_async_remote_copy(
            src_ref=src.at[pl.ds(peer * rows, rows)],
            dst_ref=land.at[:, pl.ds(me * chunk, chunk)],
            send_sem=send_sem.at[c, i], recv_sem=recv_sem.at[c, me],
            device_id=(group_id, peer), device_id_type=MESH)

    def arrival(c, land, source):
        return pltpu.make_async_remote_copy(
            src_ref=land.at[:, pl.ds(source * chunk, chunk)],
            dst_ref=land.at[:, pl.ds(source * chunk, chunk)],
            send_sem=send_sem.at[c, 0], recv_sem=recv_sem.at[c, source],
            device_id=(group_id, me), device_id_type=MESH)

    outward = list(range(n - 1))
    inward = [0] + outward[near:]
    for d in range(reach, 0, -1):
        inward += range(1 + 4 * (d - 1), 1 + 4 * d)

    def push_all(c, peers):
        src, land = ((k_ref, k_land), (v_ref, v_land))[c]
        for i in peers:
            push(c, src, land, i).start()

    pl.semaphore_wait(barrier, first)
    push_all(0, range(first))
    pass_on(2)
    own_copy(0, k_ref, k_land).start()
    own_copy(1, v_ref, v_land).start()
    small = [pltpu.make_async_copy(src, dst, small_sem.at[i]) for i, (src, dst) in enumerate((
        (lens_hbm, lens_ref), (x_hbm, x_ref), (gain_hbm, gain_ref), (bq_hbm, bq_ref), (bk_hbm, bk_ref), (bv_hbm, bv_ref)))]
    for copy in small:
        copy.start()
    for b in range(RING):
        start_weights(b)
    for stage in range(2, chips // 2 + 1):
        await_stage(stage)
        if stage < chips // 2:
            pass_on(stage + 1)
        if stage <= reach:
            push_all(0, range(1 + 4 * (stage - 1), 1 + 4 * stage))
    push_all(0, outward[near:])
    push_all(1, inward)
    for copy in small:
        copy.wait()

    x_wide = x_ref[...].astype(jnp.float32)
    mean_sq = jnp.mean(x_wide * x_wide, axis=-1, keepdims=True)
    normed = x_wide * lax.rsqrt(mean_sq + RMS_EPS) * gain_ref[...].astype(jnp.float32).reshape(1, depth)
    h_ref[...] = jnp.concatenate([normed, jnp.zeros((LHS_ROWS - rows, depth), jnp.float32)], axis=0).astype(jnp.bfloat16)
    acc[...] = jnp.zeros_like(acc)
    acc_kv[...] = jnp.zeros_like(acc_kv)

    def multiply(lhs, slot, out, tile_count):
        def tile(t, carry):
            cols = pl.ds(pl.multiple_of(t * TILE, TILE), TILE)
            out[:, cols] += jnp.dot(lhs, ring[slot, :, cols], preferred_element_type=jnp.float32)
            return carry
        lax.fori_loop(0, tile_count, tile, 0)

    def multiply_kv(b):
        base = (b % 2) * PACK
        out = (b // 2) * kv_width
        slot = b % RING
        def part(c, carry):
            lhs = h_ref[:, pl.ds(pl.multiple_of((base + c) * block, block), block)]
            for t in range(kv_width // TILE):
                cols = pl.ds(out + t * TILE, TILE)
                src = pl.ds(pl.multiple_of(c * kv_width + t * TILE, TILE), TILE)
                acc_kv[:, cols] += jnp.dot(lhs, ring[slot, :, src], preferred_element_type=jnp.float32)
            return carry
        lax.fori_loop(0, PACK, part, 0)

    for b in range(4):
        wait_weights(b)
        multiply_kv(b)
        start_weights(b + RING)
    for b in range(4, 14):
        wait_weights(b)
        multiply(h_ref[:, pl.ds((b - 4) * block, block)], b % RING, acc, width // TILE)
        if b + RING < 14 + RING:
            start_weights(b + RING)

    lane = lax.broadcasted_iota(jnp.int32, (1, head_dim), 1)
    freq_idx = jnp.where(lane < half_dim, lane, lane - half_dim).astype(jnp.float32)
    inv_freq = jnp.exp(freq_idx * (-2.0 * math.log(ROPE_THETA) / head_dim))
    sign = jnp.where(lane < half_dim, -1.0, 1.0)
    q_bias = bq_ref[...].astype(jnp.float32).reshape(heads, head_dim)
    k_bias = bk_ref[...].astype(jnp.float32).reshape(kv_heads, head_dim)
    v_bias = bv_ref[...].astype(jnp.float32).reshape(kv_heads, head_dim)
    for s in range(rows):
        for j in range(heads):
            q_raw[s, pl.ds(j, 1), :] = acc[pl.ds(s, 1), j * head_dim:(j + 1) * head_dim]
        for j in range(kv_heads):
            k_raw[s, pl.ds(j, 1), :] = acc_kv[pl.ds(s, 1), j * head_dim:(j + 1) * head_dim]
            v_raw[s, pl.ds(j, 1), :] = acc_kv[pl.ds(s, 1), kv_width + j * head_dim:kv_width + (j + 1) * head_dim]
    for s in range(rows):
        angle = lens_ref[me * rows + s].astype(jnp.float32) * inv_freq
        cos_t = jnp.cos(angle)
        sin_t = jnp.sin(angle) * sign
        q_one = q_raw[s] + q_bias
        q_rot[s] = (q_one * cos_t + pltpu.roll(q_one, half_dim, 1) * sin_t).astype(jnp.bfloat16)
        k_one = k_raw[s] + k_bias
        k_raw[s] = (k_one * cos_t + pltpu.roll(k_one, half_dim, 1) * sin_t).astype(jnp.bfloat16).astype(jnp.float32)
        v_raw[s] = (v_raw[s] + v_bias).astype(jnp.bfloat16).astype(jnp.float32)

    row_idx = lax.broadcasted_iota(jnp.int32, (span, kv_heads, head_dim), 0)
    col = lax.broadcasted_iota(jnp.int32, (heads, chunk), 1)
    head = lax.broadcasted_iota(jnp.int32, (heads, chunk), 0)
    own_head = (col % kv_heads) == (head // group)
    col_slot = col // kv_heads
    scale = head_dim ** -0.5

    def settle(land, s, source, fresh):
        place = pl.ds(pl.multiple_of(source * chunk, chunk), chunk)
        limit = lens_ref[me * rows + s] - source * span
        old = land[s, place, :].astype(jnp.float32).reshape(span, kv_heads, head_dim)
        kept = jnp.where(row_idx < limit, old, jnp.where(row_idx == limit, fresh[s][None], 0.0))
        kept = kept.reshape(chunk, head_dim).astype(jnp.bfloat16)
        land[s, place, :] = kept
        return kept, place, limit

    def lane_fold(op, values):
        out = values[:, :head_dim]
        for t in range(1, chunk // head_dim):
            out = op(out, values[:, t * head_dim:(t + 1) * head_dim])
        return out

    def score_chunk(source):
        for s in range(rows):
            keys, place, limit = settle(k_land, s, source, k_raw)
            sc = lax.dot_general(q_rot[s], keys, (((1,), (1,)), ((), ())), preferred_element_type=jnp.float32) * scale
            sc = jnp.where(own_head & (col_slot <= limit), sc, MASKED)
            scores[s, :, place] = sc
            m_acc[s] = jnp.maximum(m_acc[s], lane_fold(jnp.maximum, sc))

    def value_chunk(source):
        for s in range(rows):
            vals, place, limit = settle(v_land, s, source, v_raw)
            e = jnp.exp(scores[s, :, place] - m_acc[s][:, :1])
            l_acc[s] += lane_fold(jnp.add, e)
            o_acc[s] += jnp.dot(e.astype(jnp.bfloat16), vals, preferred_element_type=jnp.float32)

    m_acc[...] = jnp.full_like(m_acc, MASKED)
    l_acc[...] = jnp.zeros_like(l_acc)
    o_acc[...] = jnp.zeros_like(o_acc)

    own_copy(0, k_ref, k_land).wait()
    score_chunk(me)
    for i in outward:
        source = partner(i)
        arrival(0, k_land, source).wait_recv()
        score_chunk(source)
    for s in range(rows):
        m_acc[s] = jnp.broadcast_to(jnp.max(m_acc[s], axis=-1, keepdims=True), (heads, head_dim))
    own_copy(1, v_ref, v_land).wait()
    value_chunk(me)
    for i in inward:
        source = partner(i)
        arrival(1, v_land, source).wait_recv()
        value_chunk(source)

    o_row[...] = jnp.zeros_like(o_row)
    for s in range(rows):
        l_all = jnp.sum(l_acc[s], axis=-1, keepdims=True)
        q_raw[s] = o_acc[s] / l_all
        for j in range(heads):
            o_row[pl.ds(s, 1), j * head_dim:(j + 1) * head_dim] = q_raw[s, pl.ds(j, 1), :]
    o_ref[...] = o_row[...].astype(jnp.bfloat16)
    for b in range(14, 14 + RING):
        wait_weights(b)
    for c, (src, land) in enumerate(((k_ref, k_land), (v_ref, v_land))):
        for i in range(n - 1):
            push(c, src, land, i).wait_send()


def output_kernel(first, o_ref, k_land, v_land, ring, x_hbm, wo_ref, y_ref, k_out, v_out, x_ref, extra, acc, sem):
    rows, depth = x_ref.shape
    block, width = extra.shape[1:]
    resident = ring.shape[0]
    tail = [pltpu.make_async_copy(wo_ref.at[pl.ds((resident + i) * block, block)], extra.at[i], sem.at[i])
            for i in range(extra.shape[0])]
    rest = [pltpu.make_async_copy(x_hbm, x_ref, sem.at[len(tail)]),
            pltpu.make_async_copy(k_land, k_out, sem.at[len(tail) + 1]),
            pltpu.make_async_copy(v_land, v_out, sem.at[len(tail) + 2])]
    for copy in tail + rest:
        copy.start()
    acc[...] = jnp.zeros_like(acc)

    def multiply(r, weights):
        lhs = o_ref[:, r * block:(r + 1) * block]

        for t in range(width // OUT_TILE):
            cols = slice(t * OUT_TILE, (t + 1) * OUT_TILE)
            acc[:, cols] += jnp.dot(lhs, weights[:, cols], preferred_element_type=jnp.float32)

    for r in range(resident):
        multiply(r, ring.at[(first + r) % resident])
    for i, copy in enumerate(tail):
        copy.wait()
        multiply(resident + i, extra.at[i])
    for copy in rest:
        copy.wait()
    y_ref[...] = (x_ref[...].astype(jnp.float32) + acc[:rows, :]).astype(jnp.bfloat16)


def solution(mesh):
    batch_spec = P(('dp', 'cp'))
    seq_spec = P('dp', 'cp')
    whole = P()
    n = mesh.shape['cp']

    def per_device(x_tok, prompt_lens, k_cache, v_cache, norm_gain, w_q, b_q, w_k, b_k, w_v, b_v, w_o):
        rows, depth = x_tok.shape
        batch, span, kv_heads, head_dim = k_cache.shape
        width = w_q.shape[1]
        heads = width // head_dim
        chunk = span * kv_heads
        kv_width = kv_heads * head_dim
        block = depth // 10
        dims = (n, rows, span, kv_heads, head_dim, heads)
        vmem = pl.BlockSpec(memory_space=pltpu.VMEM)
        smem = pl.BlockSpec(memory_space=pltpu.SMEM)
        hbm = pl.BlockSpec(memory_space=pl.ANY)
        bf16, f32 = jnp.bfloat16, jnp.float32
        land = (rows, n * chunk, head_dim)
        o_rows, k_all, v_all, ring = pl.pallas_call(
            functools.partial(exchange_kernel, dims),
            out_shape=(pltpu.VMEM((LHS_ROWS, width), bf16), pltpu.VMEM(land, bf16), pltpu.VMEM(land, bf16),
                       pltpu.VMEM((RING, block, width), bf16)),
            in_specs=[hbm] * 12,
            out_specs=(vmem,) * 4,
            scratch_shapes=[
                pltpu.SMEM((batch,), jnp.int32),
                pltpu.VMEM((rows, depth), bf16),
                pltpu.VMEM((depth,), bf16),
                pltpu.VMEM((width,), bf16),
                pltpu.VMEM((kv_width,), bf16),
                pltpu.VMEM((kv_width,), bf16),
                pltpu.VMEM((rows, heads, n * chunk), f32),
                pltpu.VMEM((LHS_ROWS, depth), bf16),
                pltpu.VMEM((LHS_ROWS, width), f32),
                pltpu.VMEM((LHS_ROWS, 2 * kv_width), f32),
                pltpu.VMEM((rows, heads, head_dim), f32),
                pltpu.VMEM((rows, heads, head_dim), bf16),
                pltpu.VMEM((rows, kv_heads, head_dim), f32),
                pltpu.VMEM((rows, kv_heads, head_dim), f32),
                pltpu.VMEM((rows, heads, head_dim), f32),
                pltpu.VMEM((rows, heads, head_dim), f32),
                pltpu.VMEM((rows, heads, head_dim), f32),
                pltpu.VMEM((LHS_ROWS, width), f32),
                pltpu.SemaphoreType.DMA((6,)),
                pltpu.SemaphoreType.DMA((RING, PACK)),
                pltpu.SemaphoreType.DMA((2,)),
                pltpu.SemaphoreType.DMA((2, n)),
                pltpu.SemaphoreType.DMA((2, n)),
                pltpu.SemaphoreType.REGULAR((n // CORES // 2 + 1, 2)),
            ],
            compiler_params=pltpu.CompilerParams(collective_id=0, has_side_effects=True, vmem_limit_bytes=8 * 1024 * 1024),
            cost_estimate=pl.CostEstimate(flops=1 << 30, bytes_accessed=1 << 27, transcendentals=0),
        )(prompt_lens, x_tok, norm_gain, b_q, b_k, b_v,
          k_cache.reshape(batch, chunk, head_dim), v_cache.reshape(batch, chunk, head_dim), w_q, w_k, w_v, w_o)
        extra = depth // block - RING
        y, k_out, v_out = pl.pallas_call(
            functools.partial(output_kernel, 14),
            out_shape=(jax.ShapeDtypeStruct((rows, depth), bf16), jax.ShapeDtypeStruct(land, bf16), jax.ShapeDtypeStruct(land, bf16)),
            in_specs=[vmem] * 4 + [hbm] * 2,
            out_specs=(vmem, hbm, hbm),
            scratch_shapes=[
                pltpu.VMEM((rows, depth), bf16),
                pltpu.VMEM((extra, block, width), bf16),
                pltpu.VMEM((LHS_ROWS, depth), f32),
                pltpu.SemaphoreType.DMA((extra + 3,)),
            ],
            compiler_params=pltpu.CompilerParams(vmem_limit_bytes=(extra * 6 + 2) * 1024 * 1024),
            cost_estimate=pl.CostEstimate(flops=1 << 30, bytes_accessed=1 << 25, transcendentals=0),
        )(*[pltpu.with_memory_space_constraint(a, pltpu.VMEM) for a in (o_rows, k_all, v_all, ring)], x_tok, w_o)
        shape = (rows, n * span, kv_heads, head_dim)
        return y, k_out.reshape(shape), v_out.reshape(shape)

    return jax.shard_map(per_device, mesh=mesh, in_specs=(batch_spec, P('dp'), seq_spec, seq_spec, whole, whole, whole, whole, whole, whole, whole, whole), out_specs=(batch_spec, batch_spec, batch_spec), check_vma=False)
```

```python
import functools
import math
import jax
import jax.numpy as jnp
from jax import lax
from jax.experimental import pallas as pl
from jax.experimental.pallas import tpu as pltpu
from jax.sharding import PartitionSpec as P

RMS_EPS = 1e-6
ROPE_THETA = 1000000.0
MASKED = -1e30
RING = 9
PACK = 5
TILE = 512
OUT_TILE = 512
LHS_ROWS = 16
CORES = 2
MESH = pl.DeviceIdType.MESH


def exchange_kernel(dims, lens_hbm, x_hbm, gain_hbm, bq_hbm, bk_hbm, bv_hbm, k_ref, v_ref, wq_ref, wk_ref, wv_ref, wo_ref,
                    o_ref, k_land, v_land, ring,
                    lens_ref, x_ref, gain_ref, bq_ref, bk_ref, bv_ref,
                    scores, h_ref, acc, acc_kv, q_raw, q_rot, k_raw, v_raw, o_acc, m_acc, l_acc, o_row,
                    small_sem, ring_sem, own_sem, send_sem, recv_sem):
    n, rows, span, kv_heads, head_dim, heads = dims
    group = heads // kv_heads
    width = heads * head_dim
    kv_width = kv_heads * head_dim
    chunk = span * kv_heads
    depth = x_ref.shape[1]
    half_dim = head_dim // 2
    block = depth // 10
    group_id = lax.axis_index("dp")
    me = lax.axis_index("cp")

    barrier = pltpu.get_barrier_semaphore()

    def greet(d, carry):
        peer = lax.rem(me + d, n)
        pl.semaphore_signal(barrier, inc=1, device_id=(group_id, peer), device_id_type=MESH)
        return carry

    lax.fori_loop(1, n, greet, 0)

    def weight_copies(b):
        slot = ring.at[b % RING]
        if b < 4:
            src = wk_ref if b < 2 else wv_ref
            base = (b % 2) * PACK
            return [pltpu.make_async_copy(src.at[pl.ds((base + c) * block, block)],
                                          slot.at[:, pl.ds(c * kv_width, kv_width)], ring_sem.at[b % RING, c])
                    for c in range(PACK)]
        src, r = (wq_ref, b - 4) if b < 14 else (wo_ref, b - 14)
        return [pltpu.make_async_copy(src.at[pl.ds(r * block, block)], slot, ring_sem.at[b % RING, 0])]

    def start_weights(b):
        for copy in weight_copies(b):
            copy.start()

    def wait_weights(b):
        for copy in weight_copies(b):
            copy.wait()

    def partner(i):
        offset, flip = pairs[i]
        chip = lax.rem(lax.div(me, CORES) + offset + n // CORES, n // CORES)
        return chip * CORES + lax.rem(lax.rem(me, CORES) + flip, CORES)

    def own_copy(c, src, land):
        return pltpu.make_async_copy(src.at[pl.ds(me * rows, rows)], land.at[:, pl.ds(me * chunk, chunk)], own_sem.at[c])

    sides = ((k_ref, k_land), (v_ref, v_land))

    def seqs(part):
        return pl.ds(0, rows) if part is None else pl.ds(part, 1)

    def push(c, i, part=None):
        src, land = sides[c]
        peer = partner(i)
        lane = 0 if part is None else part
        first, count = (peer * rows, rows) if part is None else (peer * rows + part, 1)
        return pltpu.make_async_remote_copy(
            src_ref=src.at[pl.ds(first, count)],
            dst_ref=land.at[seqs(part), pl.ds(me * chunk, chunk)],
            send_sem=send_sem.at[lane, c, i], recv_sem=recv_sem.at[lane, c, me],
            device_id=(group_id, peer), device_id_type=MESH)

    def arrival(c, i, part=None):
        land = sides[c][1]
        source = partner(i)
        lane = 0 if part is None else part
        place = land.at[seqs(part), pl.ds(source * chunk, chunk)]
        return pltpu.make_async_remote_copy(
            src_ref=place, dst_ref=place,
            send_sem=send_sem.at[lane, c, i], recv_sem=recv_sem.at[lane, c, source],
            device_id=(group_id, me), device_id_type=MESH)

    pl.semaphore_wait(barrier, n - 1)
    chips = n // CORES
    pairs = [(0, 1)]
    for d in range(1, (chips - 1) // 2 + 1):
        pairs += [(d, 0), (-d, 0), (d, 1), (-d, 1)]
    near = len(pairs)
    if chips % 2 == 0:
        pairs += [(chips // 2, 0), (chips // 2, 1)]
    cut = ((1, 2), (1, 2, near))
    halves = tuple(range(rows))

    def parts(c, i):
        return halves if i in cut[c] else (None,)

    stretches = []
    for todo in ([(0, i) for i in range(near)], [(1, i) for i in range(near)],
                 [(0, i) for i in range(near, n - 1)] + [(1, i) for i in range(near, n - 1)]):
        even = [(c, i, part) for c, i in todo for part in parts(c, i)]
        odd = [e for e in even if e[2] in (None, 0)] + [e for e in even if e[2] not in (None, 0)]
        stretches.append((even, odd))
    core = lax.rem(me, CORES)
    for which in range(CORES):
        @pl.when(core == which)
        def _():
            for stretch in stretches:
                for c, i, part in stretch[which]:
                    push(c, i, part).start()
    own_copy(0, k_ref, k_land).start()
    own_copy(1, v_ref, v_land).start()
    small = [pltpu.make_async_copy(src, dst, small_sem.at[i]) for i, (src, dst) in enumerate((
        (lens_hbm, lens_ref), (x_hbm, x_ref), (gain_hbm, gain_ref), (bq_hbm, bq_ref), (bk_hbm, bk_ref), (bv_hbm, bv_ref)))]
    for copy in small:
        copy.start()
    for b in range(RING):
        start_weights(b)
    for copy in small:
        copy.wait()

    x_wide = x_ref[...].astype(jnp.float32)
    mean_sq = jnp.mean(x_wide * x_wide, axis=-1, keepdims=True)
    normed = x_wide * lax.rsqrt(mean_sq + RMS_EPS) * gain_ref[...].astype(jnp.float32).reshape(1, depth)
    h_ref[...] = jnp.concatenate([normed, jnp.zeros((LHS_ROWS - rows, depth), jnp.float32)], axis=0).astype(jnp.bfloat16)
    acc[...] = jnp.zeros_like(acc)
    acc_kv[...] = jnp.zeros_like(acc_kv)

    def multiply(lhs, slot, out, tile_count):
        def tile(t, carry):
            cols = pl.ds(pl.multiple_of(t * TILE, TILE), TILE)
            out[:, cols] += jnp.dot(lhs, ring[slot, :, cols], preferred_element_type=jnp.float32)
            return carry
        lax.fori_loop(0, tile_count, tile, 0)

    def multiply_kv(b):
        base = (b % 2) * PACK
        out = (b // 2) * kv_width
        slot = b % RING
        def part(c, carry):
            lhs = h_ref[:, pl.ds(pl.multiple_of((base + c) * block, block), block)]
            for t in range(kv_width // TILE):
                cols = pl.ds(out + t * TILE, TILE)
                src = pl.ds(pl.multiple_of(c * kv_width + t * TILE, TILE), TILE)
                acc_kv[:, cols] += jnp.dot(lhs, ring[slot, :, src], preferred_element_type=jnp.float32)
            return carry
        lax.fori_loop(0, PACK, part, 0)

    for b in range(4):
        wait_weights(b)
        multiply_kv(b)
        start_weights(b + RING)
    for b in range(4, 14):
        wait_weights(b)
        multiply(h_ref[:, pl.ds((b - 4) * block, block)], b % RING, acc, width // TILE)
        if b + RING < 14 + RING:
            start_weights(b + RING)

    lane = lax.broadcasted_iota(jnp.int32, (1, head_dim), 1)
    freq_idx = jnp.where(lane < half_dim, lane, lane - half_dim).astype(jnp.float32)
    inv_freq = jnp.exp(freq_idx * (-2.0 * math.log(ROPE_THETA) / head_dim))
    sign = jnp.where(lane < half_dim, -1.0, 1.0)
    q_bias = bq_ref[...].astype(jnp.float32).reshape(heads, head_dim)
    k_bias = bk_ref[...].astype(jnp.float32).reshape(kv_heads, head_dim)
    v_bias = bv_ref[...].astype(jnp.float32).reshape(kv_heads, head_dim)
    for s in range(rows):
        for j in range(heads):
            q_raw[s, pl.ds(j, 1), :] = acc[pl.ds(s, 1), j * head_dim:(j + 1) * head_dim]
        for j in range(kv_heads):
            k_raw[s, pl.ds(j, 1), :] = acc_kv[pl.ds(s, 1), j * head_dim:(j + 1) * head_dim]
            v_raw[s, pl.ds(j, 1), :] = acc_kv[pl.ds(s, 1), kv_width + j * head_dim:kv_width + (j + 1) * head_dim]
    for s in range(rows):
        angle = lens_ref[me * rows + s].astype(jnp.float32) * inv_freq
        cos_t = jnp.cos(angle)
        sin_t = jnp.sin(angle) * sign
        q_one = q_raw[s] + q_bias
        q_rot[s] = (q_one * cos_t + pltpu.roll(q_one, half_dim, 1) * sin_t).astype(jnp.bfloat16)
        k_one = k_raw[s] + k_bias
        k_raw[s] = (k_one * cos_t + pltpu.roll(k_one, half_dim, 1) * sin_t).astype(jnp.bfloat16).astype(jnp.float32)
        v_raw[s] = (v_raw[s] + v_bias).astype(jnp.bfloat16).astype(jnp.float32)

    row_idx = lax.broadcasted_iota(jnp.int32, (span, kv_heads, head_dim), 0)
    col = lax.broadcasted_iota(jnp.int32, (heads, chunk), 1)
    head = lax.broadcasted_iota(jnp.int32, (heads, chunk), 0)
    own_head = (col % kv_heads) == (head // group)
    col_slot = col // kv_heads
    scale = head_dim ** -0.5

    def settle(land, s, source, fresh):
        place = pl.ds(pl.multiple_of(source * chunk, chunk), chunk)
        limit = lens_ref[me * rows + s] - source * span
        old = land[s, place, :].astype(jnp.float32).reshape(span, kv_heads, head_dim)
        kept = jnp.where(row_idx < limit, old, jnp.where(row_idx == limit, fresh[s][None], 0.0))
        kept = kept.reshape(chunk, head_dim).astype(jnp.bfloat16)
        land[s, place, :] = kept
        return kept, place, limit

    def lane_fold(op, values):
        out = values[:, :head_dim]
        for t in range(1, chunk // head_dim):
            out = op(out, values[:, t * head_dim:(t + 1) * head_dim])
        return out

    def score_chunk(source):
        for s in range(rows):
            keys, place, limit = settle(k_land, s, source, k_raw)
            sc = lax.dot_general(q_rot[s], keys, (((1,), (1,)), ((), ())), preferred_element_type=jnp.float32) * scale
            sc = jnp.where(own_head & (col_slot <= limit), sc, MASKED)
            scores[s, :, place] = sc
            m_acc[s] = jnp.maximum(m_acc[s], lane_fold(jnp.maximum, sc))

    def value_chunk(source):
        for s in range(rows):
            vals, place, limit = settle(v_land, s, source, v_raw)
            e = jnp.exp(scores[s, :, place] - m_acc[s][:, :1])
            l_acc[s] += lane_fold(jnp.add, e)
            o_acc[s] += jnp.dot(e.astype(jnp.bfloat16), vals, preferred_element_type=jnp.float32)

    m_acc[...] = jnp.full_like(m_acc, MASKED)
    l_acc[...] = jnp.zeros_like(l_acc)
    o_acc[...] = jnp.zeros_like(o_acc)

    own_copy(0, k_ref, k_land).wait()
    score_chunk(me)
    for i in range(n - 1):
        source = partner(i)
        for part in parts(0, i):
            arrival(0, i, part).wait_recv()
        score_chunk(source)
    for s in range(rows):
        m_acc[s] = jnp.broadcast_to(jnp.max(m_acc[s], axis=-1, keepdims=True), (heads, head_dim))
    own_copy(1, v_ref, v_land).wait()
    value_chunk(me)
    for i in range(n - 1):
        source = partner(i)
        for part in parts(1, i):
            arrival(1, i, part).wait_recv()
        value_chunk(source)

    o_row[...] = jnp.zeros_like(o_row)
    for s in range(rows):
        l_all = jnp.sum(l_acc[s], axis=-1, keepdims=True)
        q_raw[s] = o_acc[s] / l_all
        for j in range(heads):
            o_row[pl.ds(s, 1), j * head_dim:(j + 1) * head_dim] = q_raw[s, pl.ds(j, 1), :]
    o_ref[...] = o_row[...].astype(jnp.bfloat16)
    for b in range(14, 14 + RING):
        wait_weights(b)
    for c in range(2):
        for i in range(n - 1):
            for part in parts(c, i):
                push(c, i, part).wait_send()


def output_kernel(first, o_ref, k_land, v_land, ring, x_hbm, wo_ref, y_ref, k_out, v_out, x_ref, extra, acc, sem):
    rows, depth = x_ref.shape
    block, width = extra.shape[1:]
    resident = ring.shape[0]
    tail = [pltpu.make_async_copy(wo_ref.at[pl.ds((resident + i) * block, block)], extra.at[i], sem.at[i])
            for i in range(extra.shape[0])]
    rest = [pltpu.make_async_copy(x_hbm, x_ref, sem.at[len(tail)]),
            pltpu.make_async_copy(k_land, k_out, sem.at[len(tail) + 1]),
            pltpu.make_async_copy(v_land, v_out, sem.at[len(tail) + 2])]
    for copy in tail + rest:
        copy.start()
    acc[...] = jnp.zeros_like(acc)

    def multiply(r, weights):
        lhs = o_ref[:, r * block:(r + 1) * block]

        for t in range(width // OUT_TILE):
            cols = slice(t * OUT_TILE, (t + 1) * OUT_TILE)
            acc[:, cols] += jnp.dot(lhs, weights[:, cols], preferred_element_type=jnp.float32)

    for r in range(resident):
        multiply(r, ring.at[(first + r) % resident])
    for i, copy in enumerate(tail):
        copy.wait()
        multiply(resident + i, extra.at[i])
    for copy in rest:
        copy.wait()
    y_ref[...] = (x_ref[...].astype(jnp.float32) + acc[:rows, :]).astype(jnp.bfloat16)


def solution(mesh):
    batch_spec = P(('dp', 'cp'))
    seq_spec = P('dp', 'cp')
    whole = P()
    n = mesh.shape['cp']

    def per_device(x_tok, prompt_lens, k_cache, v_cache, norm_gain, w_q, b_q, w_k, b_k, w_v, b_v, w_o):
        rows, depth = x_tok.shape
        batch, span, kv_heads, head_dim = k_cache.shape
        width = w_q.shape[1]
        heads = width // head_dim
        chunk = span * kv_heads
        kv_width = kv_heads * head_dim
        block = depth // 10
        dims = (n, rows, span, kv_heads, head_dim, heads)
        vmem = pl.BlockSpec(memory_space=pltpu.VMEM)
        smem = pl.BlockSpec(memory_space=pltpu.SMEM)
        hbm = pl.BlockSpec(memory_space=pl.ANY)
        bf16, f32 = jnp.bfloat16, jnp.float32
        land = (rows, n * chunk, head_dim)
        o_rows, k_all, v_all, ring = pl.pallas_call(
            functools.partial(exchange_kernel, dims),
            out_shape=(pltpu.VMEM((LHS_ROWS, width), bf16), pltpu.VMEM(land, bf16), pltpu.VMEM(land, bf16),
                       pltpu.VMEM((RING, block, width), bf16)),
            in_specs=[hbm] * 12,
            out_specs=(vmem,) * 4,
            scratch_shapes=[
                pltpu.SMEM((batch,), jnp.int32),
                pltpu.VMEM((rows, depth), bf16),
                pltpu.VMEM((depth,), bf16),
                pltpu.VMEM((width,), bf16),
                pltpu.VMEM((kv_width,), bf16),
                pltpu.VMEM((kv_width,), bf16),
                pltpu.VMEM((rows, heads, n * chunk), f32),
                pltpu.VMEM((LHS_ROWS, depth), bf16),
                pltpu.VMEM((LHS_ROWS, width), f32),
                pltpu.VMEM((LHS_ROWS, 2 * kv_width), f32),
                pltpu.VMEM((rows, heads, head_dim), f32),
                pltpu.VMEM((rows, heads, head_dim), bf16),
                pltpu.VMEM((rows, kv_heads, head_dim), f32),
                pltpu.VMEM((rows, kv_heads, head_dim), f32),
                pltpu.VMEM((rows, heads, head_dim), f32),
                pltpu.VMEM((rows, heads, head_dim), f32),
                pltpu.VMEM((rows, heads, head_dim), f32),
                pltpu.VMEM((LHS_ROWS, width), f32),
                pltpu.SemaphoreType.DMA((6,)),
                pltpu.SemaphoreType.DMA((RING, PACK)),
                pltpu.SemaphoreType.DMA((2,)),
                pltpu.SemaphoreType.DMA((rows, 2, n)),
                pltpu.SemaphoreType.DMA((rows, 2, n)),
            ],
            compiler_params=pltpu.CompilerParams(collective_id=0, has_side_effects=True, vmem_limit_bytes=8 * 1024 * 1024),
            cost_estimate=pl.CostEstimate(flops=1 << 30, bytes_accessed=1 << 27, transcendentals=0),
        )(prompt_lens, x_tok, norm_gain, b_q, b_k, b_v,
          k_cache.reshape(batch, chunk, head_dim), v_cache.reshape(batch, chunk, head_dim), w_q, w_k, w_v, w_o)
        extra = depth // block - RING
        y, k_out, v_out = pl.pallas_call(
            functools.partial(output_kernel, 14),
            out_shape=(jax.ShapeDtypeStruct((rows, depth), bf16), jax.ShapeDtypeStruct(land, bf16), jax.ShapeDtypeStruct(land, bf16)),
            in_specs=[vmem] * 4 + [hbm] * 2,
            out_specs=(vmem, hbm, hbm),
            scratch_shapes=[
                pltpu.VMEM((rows, depth), bf16),
                pltpu.VMEM((extra, block, width), bf16),
                pltpu.VMEM((LHS_ROWS, depth), f32),
                pltpu.SemaphoreType.DMA((extra + 3,)),
            ],
            compiler_params=pltpu.CompilerParams(vmem_limit_bytes=(extra * 6 + 2) * 1024 * 1024),
            cost_estimate=pl.CostEstimate(flops=1 << 30, bytes_accessed=1 << 25, transcendentals=0),
        )(*[pltpu.with_memory_space_constraint(a, pltpu.VMEM) for a in (o_rows, k_all, v_all, ring)], x_tok, w_o)
        shape = (rows, n * span, kv_heads, head_dim)
        return y, k_out.reshape(shape), v_out.reshape(shape)

    return jax.shard_map(per_device, mesh=mesh, in_specs=(batch_spec, P('dp'), seq_spec, seq_spec, whole, whole, whole, whole, whole, whole, whole, whole), out_specs=(batch_spec, batch_spec, batch_spec), check_vma=False)
```

```python
import functools
import math
import jax
import jax.numpy as jnp
from jax import lax
from jax.experimental import pallas as pl
from jax.experimental.pallas import tpu as pltpu
from jax.sharding import PartitionSpec as P

RMS_EPS = 1e-6
ROPE_THETA = 1000000.0
MASKED = -1e30
RING = 8
PACK = 5
TILE = 512
OUT_TILE = 512
LHS_ROWS = 16
CORES = 2
MESH = pl.DeviceIdType.MESH


def multiply_block(o_ref, r, weights, out):
    block, width = weights.shape
    lhs = o_ref[:, r * block:(r + 1) * block]
    for t in range(width // OUT_TILE):
        cols = slice(t * OUT_TILE, (t + 1) * OUT_TILE)
        out[:, cols] += jnp.dot(lhs, weights[:, cols], preferred_element_type=jnp.float32)


def exchange_kernel(dims, lens_hbm, x_hbm, gain_hbm, bq_hbm, bk_hbm, bv_hbm, k_ref, v_ref, wq_ref, wk_ref, wv_ref, wo_ref,
                    o_ref, k_land, v_land, ring, y_part,
                    lens_ref, x_ref, gain_ref, bq_ref, bk_ref, bv_ref,
                    scores, h_ref, acc, acc_kv, q_raw, q_rot, k_raw, v_raw, o_acc, m_acc, l_acc, o_row,
                    staged, packed, half_land, small_sem, ring_sem, own_sem, send_sem, recv_sem, stage_sem, half_send, half_recv):
    n, rows, span, kv_heads, head_dim, heads = dims
    group = heads // kv_heads
    width = heads * head_dim
    kv_width = kv_heads * head_dim
    chunk = span * kv_heads
    depth = x_ref.shape[1]
    half_dim = head_dim // 2
    block = depth // 10
    group_id = lax.axis_index("dp")
    me = lax.axis_index("cp")

    barrier = pltpu.get_barrier_semaphore()

    def greet(d, carry):
        peer = lax.rem(me + d, n)
        pl.semaphore_signal(barrier, inc=1, device_id=(group_id, peer), device_id_type=MESH)
        return carry

    lax.fori_loop(1, n, greet, 0)

    def weight_copies(b):
        slot = ring.at[b % RING]
        if b < 4:
            src = wk_ref if b < 2 else wv_ref
            base = (b % 2) * PACK
            return [pltpu.make_async_copy(src.at[pl.ds((base + c) * block, block)],
                                          slot.at[:, pl.ds(c * kv_width, kv_width)], ring_sem.at[b % RING, c])
                    for c in range(PACK)]
        src, r = (wq_ref, b - 4) if b < 14 else (wo_ref, b - 14)
        return [pltpu.make_async_copy(src.at[pl.ds(r * block, block)], slot, ring_sem.at[b % RING, 0])]

    def start_weights(b):
        for copy in weight_copies(b):
            copy.start()

    def wait_weights(b):
        for copy in weight_copies(b):
            copy.wait()

    def partner(i):
        offset, flip = pairs[i]
        chip = lax.rem(lax.div(me, CORES) + offset + n // CORES, n // CORES)
        return chip * CORES + lax.rem(lax.rem(me, CORES) + flip, CORES)

    def own_copy(c, src, land):
        return pltpu.make_async_copy(src.at[pl.ds(me * rows, rows)], land.at[:, pl.ds(me * chunk, chunk)], own_sem.at[c])

    def push(c, src, land, i):
        peer = partner(i)
        return pltpu.make_async_remote_copy(
            src_ref=src.at[pl.ds(peer * rows, rows)],
            dst_ref=land.at[:, pl.ds(me * chunk, chunk)],
            send_sem=send_sem.at[c, i], recv_sem=recv_sem.at[c, me],
            device_id=(group_id, peer), device_id_type=MESH)

    def arrival(c, land, source):
        return pltpu.make_async_remote_copy(
            src_ref=land.at[:, pl.ds(source * chunk, chunk)],
            dst_ref=land.at[:, pl.ds(source * chunk, chunk)],
            send_sem=send_sem.at[c, 0], recv_sem=recv_sem.at[c, source],
            device_id=(group_id, me), device_id_type=MESH)

    pl.semaphore_wait(barrier, n - 1)
    chips = n // CORES
    pairs = [(0, 1)]
    for d in range(1, (chips - 1) // 2 + 1):
        pairs += [(d, 0), (-d, 0), (d, 1), (-d, 1)]
    near = len(pairs)
    if chips % 2 == 0:
        pairs += [(chips // 2, 0), (chips // 2, 1)]
    for c, src, land, peers in ((0, k_ref, k_land, range(near)), (1, v_ref, v_land, range(near)),
                                (0, k_ref, k_land, range(near, n - 1))):
        for i in peers:
            push(c, src, land, i).start()
    own_copy(0, k_ref, k_land).start()
    own_copy(1, v_ref, v_land).start()

    last = range(n - 1 - near)

    def stage_copy(f):
        return pltpu.make_async_copy(v_ref.at[pl.ds(partner(near + f) * rows, rows)], staged.at[f], stage_sem.at[f])

    def push_half(part, f):
        return pltpu.make_async_remote_copy(
            src_ref=packed.at[part, f], dst_ref=half_land.at[part, f],
            send_sem=half_send.at[part, f], recv_sem=half_recv.at[part, f],
            device_id=(group_id, partner(near + f)), device_id_type=MESH)

    for f in last:
        stage_copy(f).start()
    small = [pltpu.make_async_copy(src, dst, small_sem.at[i]) for i, (src, dst) in enumerate((
        (lens_hbm, lens_ref), (x_hbm, x_ref), (gain_hbm, gain_ref), (bq_hbm, bq_ref), (bk_hbm, bk_ref), (bv_hbm, bv_ref)))]
    for copy in small:
        copy.start()
    for b in range(RING):
        start_weights(b)
    for copy in small:
        copy.wait()

    x_wide = x_ref[...].astype(jnp.float32)
    mean_sq = jnp.mean(x_wide * x_wide, axis=-1, keepdims=True)
    normed = x_wide * lax.rsqrt(mean_sq + RMS_EPS) * gain_ref[...].astype(jnp.float32).reshape(1, depth)
    h_ref[...] = jnp.concatenate([normed, jnp.zeros((LHS_ROWS - rows, depth), jnp.float32)], axis=0).astype(jnp.bfloat16)
    acc[...] = jnp.zeros_like(acc)
    acc_kv[...] = jnp.zeros_like(acc_kv)

    def multiply(lhs, slot, out, tile_count):
        def tile(t, carry):
            cols = pl.ds(pl.multiple_of(t * TILE, TILE), TILE)
            out[:, cols] += jnp.dot(lhs, ring[slot, :, cols], preferred_element_type=jnp.float32)
            return carry
        lax.fori_loop(0, tile_count, tile, 0)

    def multiply_kv(b):
        base = (b % 2) * PACK
        out = (b // 2) * kv_width
        slot = b % RING
        def part(c, carry):
            lhs = h_ref[:, pl.ds(pl.multiple_of((base + c) * block, block), block)]
            for t in range(kv_width // TILE):
                cols = pl.ds(out + t * TILE, TILE)
                src = pl.ds(pl.multiple_of(c * kv_width + t * TILE, TILE), TILE)
                acc_kv[:, cols] += jnp.dot(lhs, ring[slot, :, src], preferred_element_type=jnp.float32)
            return carry
        lax.fori_loop(0, PACK, part, 0)

    half = kv_heads // 2
    tile_row = lax.broadcasted_iota(jnp.int32, (span // 2, kv_heads, head_dim), 1)
    for f in last:
        stage_copy(f).wait()
        for s in range(rows):
            pair = staged[f, s].astype(jnp.float32).reshape(span // 2, 2, kv_heads, head_dim)
            even, odd = pair[:, 0], pair[:, 1]
            for part, both in enumerate((jnp.where(tile_row < half, even, pltpu.roll(odd, half, 1)),
                                         jnp.where(tile_row < half, pltpu.roll(even, half, 1), odd))):
                packed[part, f, s] = both.reshape(chunk // 2, head_dim).astype(jnp.bfloat16)

    for b in range(4):
        wait_weights(b)
        multiply_kv(b)
        start_weights(b + RING)
    for b in range(4, 14):
        wait_weights(b)
        multiply(h_ref[:, pl.ds((b - 4) * block, block)], b % RING, acc, width // TILE)
        if b + RING < 14 + RING:
            start_weights(b + RING)

    for part in range(2):
        for f in last:
            push_half(part, f).start()

    lane = lax.broadcasted_iota(jnp.int32, (1, head_dim), 1)
    freq_idx = jnp.where(lane < half_dim, lane, lane - half_dim).astype(jnp.float32)
    inv_freq = jnp.exp(freq_idx * (-2.0 * math.log(ROPE_THETA) / head_dim))
    sign = jnp.where(lane < half_dim, -1.0, 1.0)
    q_bias = bq_ref[...].astype(jnp.float32).reshape(heads, head_dim)
    k_bias = bk_ref[...].astype(jnp.float32).reshape(kv_heads, head_dim)
    v_bias = bv_ref[...].astype(jnp.float32).reshape(kv_heads, head_dim)
    for s in range(rows):
        for j in range(heads):
            q_raw[s, pl.ds(j, 1), :] = acc[pl.ds(s, 1), j * head_dim:(j + 1) * head_dim]
        for j in range(kv_heads):
            k_raw[s, pl.ds(j, 1), :] = acc_kv[pl.ds(s, 1), j * head_dim:(j + 1) * head_dim]
            v_raw[s, pl.ds(j, 1), :] = acc_kv[pl.ds(s, 1), kv_width + j * head_dim:kv_width + (j + 1) * head_dim]
    for s in range(rows):
        angle = lens_ref[me * rows + s].astype(jnp.float32) * inv_freq
        cos_t = jnp.cos(angle)
        sin_t = jnp.sin(angle) * sign
        q_one = q_raw[s] + q_bias
        q_rot[s] = (q_one * cos_t + pltpu.roll(q_one, half_dim, 1) * sin_t).astype(jnp.bfloat16)
        k_one = k_raw[s] + k_bias
        k_raw[s] = (k_one * cos_t + pltpu.roll(k_one, half_dim, 1) * sin_t).astype(jnp.bfloat16).astype(jnp.float32)
        v_raw[s] = (v_raw[s] + v_bias).astype(jnp.bfloat16).astype(jnp.float32)

    row_idx = lax.broadcasted_iota(jnp.int32, (span, kv_heads, head_dim), 0)
    col = lax.broadcasted_iota(jnp.int32, (heads, chunk), 1)
    head = lax.broadcasted_iota(jnp.int32, (heads, chunk), 0)
    own_head = (col % kv_heads) == (head // group)
    col_slot = col // kv_heads
    scale = head_dim ** -0.5

    def settle(land, s, source, fresh):
        place = pl.ds(pl.multiple_of(source * chunk, chunk), chunk)
        limit = lens_ref[me * rows + s] - source * span
        old = land[s, place, :].astype(jnp.float32).reshape(span, kv_heads, head_dim)
        kept = jnp.where(row_idx < limit, old, jnp.where(row_idx == limit, fresh[s][None], 0.0))
        kept = kept.reshape(chunk, head_dim).astype(jnp.bfloat16)
        land[s, place, :] = kept
        return kept, place, limit

    def lane_fold(op, values):
        out = values[:, :head_dim]
        for t in range(1, chunk // head_dim):
            out = op(out, values[:, t * head_dim:(t + 1) * head_dim])
        return out

    def score_chunk(source):
        for s in range(rows):
            keys, place, limit = settle(k_land, s, source, k_raw)
            sc = lax.dot_general(q_rot[s], keys, (((1,), (1,)), ((), ())), preferred_element_type=jnp.float32) * scale
            sc = jnp.where(own_head & (col_slot <= limit), sc, MASKED)
            scores[s, :, place] = sc
            m_acc[s] = jnp.maximum(m_acc[s], lane_fold(jnp.maximum, sc))

    head_row = lax.broadcasted_iota(jnp.int32, (span, kv_heads, head_dim), 1)

    def settle_half(s, f, source, part):
        place = pl.ds(pl.multiple_of(source * chunk, chunk), chunk)
        limit = lens_ref[me * rows + s] - source * span
        both = half_land[part, f, s].astype(jnp.float32).reshape(span // 2, kv_heads, head_dim)
        turned = pltpu.roll(both, half, 1)
        even, odd = (both, turned) if part == 0 else (turned, both)
        old = jnp.stack([even, odd], axis=1).reshape(span, kv_heads, head_dim)
        kept = jnp.where(row_idx < limit, old, jnp.where(row_idx == limit, v_raw[s][None], 0.0))
        mine = head_row < half if part == 0 else head_row >= half
        kept = jnp.where(mine, kept, 0.0)
        full = kept
        if part:
            full = jnp.where(mine, kept, v_land[s, place, :].astype(jnp.float32).reshape(span, kv_heads, head_dim))
        v_land[s, place, :] = full.reshape(chunk, head_dim).astype(jnp.bfloat16)
        return kept.reshape(chunk, head_dim).astype(jnp.bfloat16), place

    def weigh(s, place, vals, count):
        e = jnp.exp(scores[s, :, place] - m_acc[s][:, :1])
        if count:
            l_acc[s] += lane_fold(jnp.add, e)
        o_acc[s] += jnp.dot(e.astype(jnp.bfloat16), vals, preferred_element_type=jnp.float32)

    def value_chunk(source):
        for s in range(rows):
            vals, place, _ = settle(v_land, s, source, v_raw)
            weigh(s, place, vals, True)

    def value_half(part):
        for f in last:
            push_half(part, f).wait_recv()
            for s in range(rows):
                vals, place = settle_half(s, f, partner(near + f), part)
                weigh(s, place, vals, part == 0)

    def finish_heads(part):
        start, stop = part * heads // 2, (part + 1) * heads // 2
        for s in range(rows):
            l_all = jnp.sum(l_acc[s, pl.ds(start, stop - start), :], axis=-1, keepdims=True)
            q_raw[s, pl.ds(start, stop - start), :] = o_acc[s, pl.ds(start, stop - start), :] / l_all
            for j in range(start, stop):
                o_row[pl.ds(s, 1), j * head_dim:(j + 1) * head_dim] = q_raw[s, pl.ds(j, 1), :]
        cols = slice(start * head_dim, stop * head_dim)
        o_ref[:, cols] = o_row[:, cols].astype(jnp.bfloat16)

    m_acc[...] = jnp.full_like(m_acc, MASKED)
    l_acc[...] = jnp.zeros_like(l_acc)
    o_acc[...] = jnp.zeros_like(o_acc)

    own_copy(0, k_ref, k_land).wait()
    score_chunk(me)
    for i in range(n - 1):
        source = partner(i)
        arrival(0, k_land, source).wait_recv()
        score_chunk(source)
    for s in range(rows):
        m_acc[s] = jnp.broadcast_to(jnp.max(m_acc[s], axis=-1, keepdims=True), (heads, head_dim))
    own_copy(1, v_ref, v_land).wait()
    value_chunk(me)
    for i in range(near):
        source = partner(i)
        arrival(1, v_land, source).wait_recv()
        value_chunk(source)
    o_row[...] = jnp.zeros_like(o_row)
    y_part[...] = jnp.zeros_like(y_part)
    value_half(0)
    finish_heads(0)
    for r in range(depth // block // 2):
        wait_weights(14 + r)
        multiply_block(o_ref, r, ring.at[(14 + r) % RING], y_part)
        if 14 + r + RING < 24:
            start_weights(14 + r + RING)
    value_half(1)
    finish_heads(1)
    for r in range(depth // block // 2, depth // block):
        wait_weights(14 + r)
    for c, (src, land) in enumerate(((k_ref, k_land), (v_ref, v_land))):
        for i in range(n - 1 if c == 0 else near):
            push(c, src, land, i).wait_send()
    for part in range(2):
        for f in last:
            push_half(part, f).wait_send()


def output_kernel(first, start, o_ref, k_land, v_land, ring, y_part, x_hbm, y_ref, k_out, v_out, x_ref, acc, sem):
    rows, depth = x_ref.shape
    block = ring.shape[1]
    copies = [pltpu.make_async_copy(k_land, k_out, sem.at[0]),
              pltpu.make_async_copy(v_land, v_out, sem.at[1]),
              pltpu.make_async_copy(x_hbm, x_ref, sem.at[2])]
    for copy in copies:
        copy.start()
    acc[...] = y_part[...]
    for r in range(start, depth // block):
        multiply_block(o_ref, r, ring.at[(first + r) % ring.shape[0]], acc)
    for copy in copies:
        copy.wait()
    y_ref[...] = (x_ref[...].astype(jnp.float32) + acc[:rows, :]).astype(jnp.bfloat16)


def solution(mesh):
    batch_spec = P(('dp', 'cp'))
    seq_spec = P('dp', 'cp')
    whole = P()
    n = mesh.shape['cp']

    def per_device(x_tok, prompt_lens, k_cache, v_cache, norm_gain, w_q, b_q, w_k, b_k, w_v, b_v, w_o):
        rows, depth = x_tok.shape
        batch, span, kv_heads, head_dim = k_cache.shape
        width = w_q.shape[1]
        heads = width // head_dim
        chunk = span * kv_heads
        kv_width = kv_heads * head_dim
        block = depth // 10
        dims = (n, rows, span, kv_heads, head_dim, heads)
        vmem = pl.BlockSpec(memory_space=pltpu.VMEM)
        smem = pl.BlockSpec(memory_space=pltpu.SMEM)
        hbm = pl.BlockSpec(memory_space=pl.ANY)
        bf16, f32 = jnp.bfloat16, jnp.float32
        land = (rows, n * chunk, head_dim)
        o_rows, k_all, v_all, ring, y_part = pl.pallas_call(
            functools.partial(exchange_kernel, dims),
            out_shape=(pltpu.VMEM((LHS_ROWS, width), bf16), pltpu.VMEM(land, bf16), pltpu.VMEM(land, bf16),
                       pltpu.VMEM((RING, block, width), bf16), pltpu.VMEM((LHS_ROWS, depth), f32)),
            in_specs=[hbm] * 12,
            out_specs=(vmem,) * 5,
            scratch_shapes=[
                pltpu.SMEM((batch,), jnp.int32),
                pltpu.VMEM((rows, depth), bf16),
                pltpu.VMEM((depth,), bf16),
                pltpu.VMEM((width,), bf16),
                pltpu.VMEM((kv_width,), bf16),
                pltpu.VMEM((kv_width,), bf16),
                pltpu.VMEM((rows, heads, n * chunk), f32),
                pltpu.VMEM((LHS_ROWS, depth), bf16),
                pltpu.VMEM((LHS_ROWS, width), f32),
                pltpu.VMEM((LHS_ROWS, 2 * kv_width), f32),
                pltpu.VMEM((rows, heads, head_dim), f32),
                pltpu.VMEM((rows, heads, head_dim), bf16),
                pltpu.VMEM((rows, kv_heads, head_dim), f32),
                pltpu.VMEM((rows, kv_heads, head_dim), f32),
                pltpu.VMEM((rows, heads, head_dim), f32),
                pltpu.VMEM((rows, heads, head_dim), f32),
                pltpu.VMEM((rows, heads, head_dim), f32),
                pltpu.VMEM((LHS_ROWS, width), f32),
                pltpu.VMEM((CORES, rows, chunk, head_dim), bf16),
                pltpu.VMEM((2, CORES, rows, chunk // 2, head_dim), bf16),
                pltpu.VMEM((2, CORES, rows, chunk // 2, head_dim), bf16),
                pltpu.SemaphoreType.DMA((6,)),
                pltpu.SemaphoreType.DMA((RING, PACK)),
                pltpu.SemaphoreType.DMA((2,)),
                pltpu.SemaphoreType.DMA((2, n)),
                pltpu.SemaphoreType.DMA((2, n)),
                pltpu.SemaphoreType.DMA((CORES,)),
                pltpu.SemaphoreType.DMA((2, CORES)),
                pltpu.SemaphoreType.DMA((2, CORES)),
            ],
            compiler_params=pltpu.CompilerParams(collective_id=0, has_side_effects=True, vmem_limit_bytes=8 * 1024 * 1024),
            cost_estimate=pl.CostEstimate(flops=1 << 30, bytes_accessed=1 << 27, transcendentals=0),
        )(prompt_lens, x_tok, norm_gain, b_q, b_k, b_v,
          k_cache.reshape(batch, chunk, head_dim), v_cache.reshape(batch, chunk, head_dim), w_q, w_k, w_v, w_o)
        y, k_out, v_out = pl.pallas_call(
            functools.partial(output_kernel, 14, depth // block // 2),
            out_shape=(jax.ShapeDtypeStruct((rows, depth), bf16), jax.ShapeDtypeStruct(land, bf16), jax.ShapeDtypeStruct(land, bf16)),
            in_specs=[vmem] * 5 + [hbm],
            out_specs=(vmem, hbm, hbm),
            scratch_shapes=[
                pltpu.VMEM((rows, depth), bf16),
                pltpu.VMEM((LHS_ROWS, depth), f32),
                pltpu.SemaphoreType.DMA((3,)),
            ],
            compiler_params=pltpu.CompilerParams(vmem_limit_bytes=3 * 1024 * 1024),
            cost_estimate=pl.CostEstimate(flops=1 << 30, bytes_accessed=1 << 25, transcendentals=0),
        )(*[pltpu.with_memory_space_constraint(a, pltpu.VMEM) for a in (o_rows, k_all, v_all, ring, y_part)], x_tok)
        shape = (rows, n * span, kv_heads, head_dim)
        return y, k_out.reshape(shape), v_out.reshape(shape)

    return jax.shard_map(per_device, mesh=mesh, in_specs=(batch_spec, P('dp'), seq_spec, seq_spec, whole, whole, whole, whole, whole, whole, whole, whole), out_specs=(batch_spec, batch_spec, batch_spec), check_vma=False)
```

```python
import functools
import math
import jax
import jax.numpy as jnp
from jax import lax
from jax.experimental import pallas as pl
from jax.experimental.pallas import tpu as pltpu
from jax.sharding import PartitionSpec as P

RMS_EPS = 1e-6
ROPE_THETA = 1000000.0
MASKED = -1e30
RING = 8
PACK = 5
TILE = 512
OUT_TILE = 512
LHS_ROWS = 16
CORES = 2
MESH = pl.DeviceIdType.MESH


def multiply_block(o_ref, r, weights, out):
    block, width = weights.shape
    lhs = o_ref[:, r * block:(r + 1) * block]
    for t in range(width // OUT_TILE):
        cols = slice(t * OUT_TILE, (t + 1) * OUT_TILE)
        out[:, cols] += jnp.dot(lhs, weights[:, cols], preferred_element_type=jnp.float32)


def exchange_kernel(dims, lens_hbm, x_hbm, gain_hbm, bq_hbm, bk_hbm, bv_hbm, k_ref, v_ref, wq_ref, wk_ref, wv_ref, wo_ref,
                    o_ref, k_land, v_land, ring, y_part,
                    lens_ref, x_ref, gain_ref, bq_ref, bk_ref, bv_ref,
                    scores, h_ref, acc, acc_kv, q_raw, q_rot, k_raw, v_raw, o_acc, m_acc, l_acc, o_row,
                    staged, packed, half_land, small_sem, ring_sem, own_sem, send_sem, recv_sem, stage_sem, half_send, half_recv):
    n, rows, span, kv_heads, head_dim, heads = dims
    group = heads // kv_heads
    width = heads * head_dim
    kv_width = kv_heads * head_dim
    chunk = span * kv_heads
    depth = x_ref.shape[1]
    half_dim = head_dim // 2
    block = depth // 10
    group_id = lax.axis_index("dp")
    me = lax.axis_index("cp")

    barrier = pltpu.get_barrier_semaphore()

    def greet(d, carry):
        peer = lax.rem(me + d, n)
        pl.semaphore_signal(barrier, inc=1, device_id=(group_id, peer), device_id_type=MESH)
        return carry

    lax.fori_loop(1, n, greet, 0)

    def weight_copies(b):
        slot = ring.at[b % RING]
        if b < 4:
            src = wk_ref if b < 2 else wv_ref
            base = (b % 2) * PACK
            return [pltpu.make_async_copy(src.at[pl.ds((base + c) * block, block)],
                                          slot.at[:, pl.ds(c * kv_width, kv_width)], ring_sem.at[b % RING, c])
                    for c in range(PACK)]
        src, r = (wq_ref, b - 4) if b < 14 else (wo_ref, b - 14)
        return [pltpu.make_async_copy(src.at[pl.ds(r * block, block)], slot, ring_sem.at[b % RING, 0])]

    def start_weights(b):
        for copy in weight_copies(b):
            copy.start()

    def wait_weights(b):
        for copy in weight_copies(b):
            copy.wait()

    def partner(i):
        offset, flip = pairs[i]
        chip = lax.rem(lax.div(me, CORES) + offset + n // CORES, n // CORES)
        return chip * CORES + lax.rem(lax.rem(me, CORES) + flip, CORES)

    def own_copy(c, src, land):
        return pltpu.make_async_copy(src.at[pl.ds(me * rows, rows)], land.at[:, pl.ds(me * chunk, chunk)], own_sem.at[c])

    def push(c, src, land, i):
        peer = partner(i)
        return pltpu.make_async_remote_copy(
            src_ref=src.at[pl.ds(peer * rows, rows)],
            dst_ref=land.at[:, pl.ds(me * chunk, chunk)],
            send_sem=send_sem.at[c, i], recv_sem=recv_sem.at[c, me],
            device_id=(group_id, peer), device_id_type=MESH)

    def arrival(c, land, source):
        return pltpu.make_async_remote_copy(
            src_ref=land.at[:, pl.ds(source * chunk, chunk)],
            dst_ref=land.at[:, pl.ds(source * chunk, chunk)],
            send_sem=send_sem.at[c, 0], recv_sem=recv_sem.at[c, source],
            device_id=(group_id, me), device_id_type=MESH)

    pl.semaphore_wait(barrier, n - 1)
    chips = n // CORES
    pairs = [(0, 1)]
    for d in range(1, (chips - 1) // 2 + 1):
        pairs += [(d, 0), (-d, 0), (d, 1), (-d, 1)]
    near = len(pairs)
    if chips % 2 == 0:
        pairs += [(chips // 2, 0), (chips // 2, 1)]
    for c, src, land, peers in ((0, k_ref, k_land, range(near)), (1, v_ref, v_land, range(near)),
                                (0, k_ref, k_land, range(near, n - 1))):
        for i in peers:
            push(c, src, land, i).start()
    own_copy(0, k_ref, k_land).start()
    own_copy(1, v_ref, v_land).start()

    last = range(n - 1 - near)

    def stage_copy(f):
        return pltpu.make_async_copy(v_ref.at[pl.ds(partner(near + f) * rows, rows)], staged.at[f], stage_sem.at[f])

    def push_half(part, f):
        return pltpu.make_async_remote_copy(
            src_ref=packed.at[part, f], dst_ref=half_land.at[part, f],
            send_sem=half_send.at[part, f], recv_sem=half_recv.at[part, f],
            device_id=(group_id, partner(near + f)), device_id_type=MESH)

    for f in last:
        stage_copy(f).start()
    small = [pltpu.make_async_copy(src, dst, small_sem.at[i]) for i, (src, dst) in enumerate((
        (lens_hbm, lens_ref), (x_hbm, x_ref), (gain_hbm, gain_ref), (bq_hbm, bq_ref), (bk_hbm, bk_ref), (bv_hbm, bv_ref)))]
    for copy in small:
        copy.start()
    for b in range(RING):
        start_weights(b)
    for copy in small:
        copy.wait()

    x_wide = x_ref[...].astype(jnp.float32)
    mean_sq = jnp.mean(x_wide * x_wide, axis=-1, keepdims=True)
    normed = x_wide * lax.rsqrt(mean_sq + RMS_EPS) * gain_ref[...].astype(jnp.float32).reshape(1, depth)
    h_ref[...] = jnp.concatenate([normed, jnp.zeros((LHS_ROWS - rows, depth), jnp.float32)], axis=0).astype(jnp.bfloat16)
    acc[...] = jnp.zeros_like(acc)
    acc_kv[...] = jnp.zeros_like(acc_kv)

    def multiply(lhs, slot, out, tile_count):
        def tile(t, carry):
            cols = pl.ds(pl.multiple_of(t * TILE, TILE), TILE)
            out[:, cols] += jnp.dot(lhs, ring[slot, :, cols], preferred_element_type=jnp.float32)
            return carry
        lax.fori_loop(0, tile_count, tile, 0)

    def multiply_kv(b):
        base = (b % 2) * PACK
        out = (b // 2) * kv_width
        slot = b % RING
        def part(c, carry):
            lhs = h_ref[:, pl.ds(pl.multiple_of((base + c) * block, block), block)]
            for t in range(kv_width // TILE):
                cols = pl.ds(out + t * TILE, TILE)
                src = pl.ds(pl.multiple_of(c * kv_width + t * TILE, TILE), TILE)
                acc_kv[:, cols] += jnp.dot(lhs, ring[slot, :, src], preferred_element_type=jnp.float32)
            return carry
        lax.fori_loop(0, PACK, part, 0)

    half = kv_heads // 2
    tile_row = lax.broadcasted_iota(jnp.int32, (span // 2, kv_heads, head_dim), 1)
    for f in last:
        stage_copy(f).wait()
        for s in range(rows):
            pair = staged[f, s].astype(jnp.float32).reshape(span // 2, 2, kv_heads, head_dim)
            even, odd = pair[:, 0], pair[:, 1]
            for part, both in enumerate((jnp.where(tile_row < half, even, pltpu.roll(odd, half, 1)),
                                         jnp.where(tile_row < half, pltpu.roll(even, half, 1), odd))):
                packed[part, f, s] = both.reshape(chunk // 2, head_dim).astype(jnp.bfloat16)

    for b in range(4):
        wait_weights(b)
        multiply_kv(b)
        start_weights(b + RING)
    for b in range(4, 14):
        wait_weights(b)
        multiply(h_ref[:, pl.ds((b - 4) * block, block)], b % RING, acc, width // TILE)
        if b + RING < 14 + RING:
            start_weights(b + RING)

    for part in range(2):
        for f in last:
            push_half(part, f).start()

    lane = lax.broadcasted_iota(jnp.int32, (1, head_dim), 1)
    freq_idx = jnp.where(lane < half_dim, lane, lane - half_dim).astype(jnp.float32)
    inv_freq = jnp.exp(freq_idx * (-2.0 * math.log(ROPE_THETA) / head_dim))
    sign = jnp.where(lane < half_dim, -1.0, 1.0)
    q_bias = bq_ref[...].astype(jnp.float32).reshape(heads, head_dim)
    k_bias = bk_ref[...].astype(jnp.float32).reshape(kv_heads, head_dim)
    v_bias = bv_ref[...].astype(jnp.float32).reshape(kv_heads, head_dim)
    for s in range(rows):
        for j in range(heads):
            q_raw[s, pl.ds(j, 1), :] = acc[pl.ds(s, 1), j * head_dim:(j + 1) * head_dim]
        for j in range(kv_heads):
            k_raw[s, pl.ds(j, 1), :] = acc_kv[pl.ds(s, 1), j * head_dim:(j + 1) * head_dim]
            v_raw[s, pl.ds(j, 1), :] = acc_kv[pl.ds(s, 1), kv_width + j * head_dim:kv_width + (j + 1) * head_dim]
    for s in range(rows):
        angle = lens_ref[me * rows + s].astype(jnp.float32) * inv_freq
        cos_t = jnp.cos(angle)
        sin_t = jnp.sin(angle) * sign
        q_one = q_raw[s] + q_bias
        q_rot[s] = (q_one * cos_t + pltpu.roll(q_one, half_dim, 1) * sin_t).astype(jnp.bfloat16)
        k_one = k_raw[s] + k_bias
        k_raw[s] = (k_one * cos_t + pltpu.roll(k_one, half_dim, 1) * sin_t).astype(jnp.bfloat16).astype(jnp.float32)
        v_raw[s] = (v_raw[s] + v_bias).astype(jnp.bfloat16).astype(jnp.float32)

    row_idx = lax.broadcasted_iota(jnp.int32, (span, kv_heads, head_dim), 0)
    col = lax.broadcasted_iota(jnp.int32, (heads, chunk), 1)
    head = lax.broadcasted_iota(jnp.int32, (heads, chunk), 0)
    own_head = (col % kv_heads) == (head // group)
    col_slot = col // kv_heads
    scale = head_dim ** -0.5

    def settle(land, s, source, fresh):
        place = pl.ds(pl.multiple_of(source * chunk, chunk), chunk)
        limit = lens_ref[me * rows + s] - source * span
        old = land[s, place, :].astype(jnp.float32).reshape(span, kv_heads, head_dim)
        kept = jnp.where(row_idx < limit, old, jnp.where(row_idx == limit, fresh[s][None], 0.0))
        kept = kept.reshape(chunk, head_dim).astype(jnp.bfloat16)
        land[s, place, :] = kept
        return kept, place, limit

    def lane_fold(op, values):
        out = values[:, :head_dim]
        for t in range(1, chunk // head_dim):
            out = op(out, values[:, t * head_dim:(t + 1) * head_dim])
        return out

    def score_chunk(source):
        for s in range(rows):
            keys, place, limit = settle(k_land, s, source, k_raw)
            sc = lax.dot_general(q_rot[s], keys, (((1,), (1,)), ((), ())), preferred_element_type=jnp.float32) * scale
            sc = jnp.where(own_head & (col_slot <= limit), sc, MASKED)
            scores[s, :, place] = sc
            m_acc[s] = jnp.maximum(m_acc[s], lane_fold(jnp.maximum, sc))

    head_row = lax.broadcasted_iota(jnp.int32, (span, kv_heads, head_dim), 1)

    def settle_half(s, f, source, part):
        place = pl.ds(pl.multiple_of(source * chunk, chunk), chunk)
        limit = lens_ref[me * rows + s] - source * span
        both = half_land[part, f, s].astype(jnp.float32).reshape(span // 2, kv_heads, head_dim)
        turned = pltpu.roll(both, half, 1)
        even, odd = (both, turned) if part == 0 else (turned, both)
        old = jnp.stack([even, odd], axis=1).reshape(span, kv_heads, head_dim)
        kept = jnp.where(row_idx < limit, old, jnp.where(row_idx == limit, v_raw[s][None], 0.0))
        mine = head_row < half if part == 0 else head_row >= half
        kept = jnp.where(mine, kept, 0.0)
        full = kept
        if part:
            full = jnp.where(mine, kept, v_land[s, place, :].astype(jnp.float32).reshape(span, kv_heads, head_dim))
        v_land[s, place, :] = full.reshape(chunk, head_dim).astype(jnp.bfloat16)
        return kept.reshape(chunk, head_dim).astype(jnp.bfloat16), place

    def weigh(s, place, vals, count):
        e = jnp.exp(scores[s, :, place] - m_acc[s][:, :1])
        if count:
            l_acc[s] += lane_fold(jnp.add, e)
        o_acc[s] += jnp.dot(e.astype(jnp.bfloat16), vals, preferred_element_type=jnp.float32)

    def value_chunk(source):
        for s in range(rows):
            vals, place, _ = settle(v_land, s, source, v_raw)
            weigh(s, place, vals, True)

    def value_half(part):
        for f in last:
            push_half(part, f).wait_recv()
            for s in range(rows):
                vals, place = settle_half(s, f, partner(near + f), part)
                weigh(s, place, vals, part == 0)

    def finish_heads(part):
        start, stop = part * heads // 2, (part + 1) * heads // 2
        for s in range(rows):
            l_all = jnp.sum(l_acc[s, pl.ds(start, stop - start), :], axis=-1, keepdims=True)
            q_raw[s, pl.ds(start, stop - start), :] = o_acc[s, pl.ds(start, stop - start), :] / l_all
            for j in range(start, stop):
                o_row[pl.ds(s, 1), j * head_dim:(j + 1) * head_dim] = q_raw[s, pl.ds(j, 1), :]
        cols = slice(start * head_dim, stop * head_dim)
        o_ref[:, cols] = o_row[:, cols].astype(jnp.bfloat16)

    m_acc[...] = jnp.full_like(m_acc, MASKED)
    l_acc[...] = jnp.zeros_like(l_acc)
    o_acc[...] = jnp.zeros_like(o_acc)

    own_copy(0, k_ref, k_land).wait()
    score_chunk(me)
    for i in range(n - 1):
        source = partner(i)
        arrival(0, k_land, source).wait_recv()
        score_chunk(source)
    for s in range(rows):
        m_acc[s] = jnp.broadcast_to(jnp.max(m_acc[s], axis=-1, keepdims=True), (heads, head_dim))
    own_copy(1, v_ref, v_land).wait()
    value_chunk(me)
    for i in range(near):
        source = partner(i)
        arrival(1, v_land, source).wait_recv()
        value_chunk(source)
    o_row[...] = jnp.zeros_like(o_row)
    y_part[...] = jnp.zeros_like(y_part)
    value_half(0)
    finish_heads(0)
    for r in range(depth // block // 2):
        wait_weights(14 + r)
        multiply_block(o_ref, r, ring.at[(14 + r) % RING], y_part)
        if 14 + r + RING < 24:
            start_weights(14 + r + RING)
    value_half(1)
    finish_heads(1)
    for r in range(depth // block // 2, depth // block):
        wait_weights(14 + r)
    for c, (src, land) in enumerate(((k_ref, k_land), (v_ref, v_land))):
        for i in range(n - 1 if c == 0 else near):
            push(c, src, land, i).wait_send()
    for part in range(2):
        for f in last:
            push_half(part, f).wait_send()


def output_kernel(first, start, o_ref, k_land, v_land, ring, y_part, x_hbm, y_ref, k_out, v_out, x_ref, acc, sem):
    rows, depth = x_ref.shape
    block = ring.shape[1]
    copies = [pltpu.make_async_copy(k_land, k_out, sem.at[0]),
              pltpu.make_async_copy(v_land, v_out, sem.at[1]),
              pltpu.make_async_copy(x_hbm, x_ref, sem.at[2])]
    for copy in copies:
        copy.start()
    acc[...] = y_part[...]
    for r in range(start, depth // block):
        multiply_block(o_ref, r, ring.at[(first + r) % ring.shape[0]], acc)
    for copy in copies:
        copy.wait()
    y_ref[...] = (x_ref[...].astype(jnp.float32) + acc[:rows, :]).astype(jnp.bfloat16)


def solution(mesh):
    batch_spec = P(('dp', 'cp'))
    seq_spec = P('dp', 'cp')
    whole = P()
    n = mesh.shape['cp']

    def per_device(x_tok, prompt_lens, k_cache, v_cache, norm_gain, w_q, b_q, w_k, b_k, w_v, b_v, w_o):
        rows, depth = x_tok.shape
        batch, span, kv_heads, head_dim = k_cache.shape
        width = w_q.shape[1]
        heads = width // head_dim
        chunk = span * kv_heads
        kv_width = kv_heads * head_dim
        block = depth // 10
        dims = (n, rows, span, kv_heads, head_dim, heads)
        vmem = pl.BlockSpec(memory_space=pltpu.VMEM)
        smem = pl.BlockSpec(memory_space=pltpu.SMEM)
        hbm = pl.BlockSpec(memory_space=pl.ANY)
        bf16, f32 = jnp.bfloat16, jnp.float32
        land = (rows, n * chunk, head_dim)
        o_rows, k_all, v_all, ring, y_part = pl.pallas_call(
            functools.partial(exchange_kernel, dims),
            out_shape=(pltpu.VMEM((LHS_ROWS, width), bf16), pltpu.VMEM(land, bf16), pltpu.VMEM(land, bf16),
                       pltpu.VMEM((RING, block, width), bf16), pltpu.VMEM((LHS_ROWS, depth), f32)),
            in_specs=[hbm] * 12,
            out_specs=(vmem,) * 5,
            scratch_shapes=[
                pltpu.SMEM((batch,), jnp.int32),
                pltpu.VMEM((rows, depth), bf16),
                pltpu.VMEM((depth,), bf16),
                pltpu.VMEM((width,), bf16),
                pltpu.VMEM((kv_width,), bf16),
                pltpu.VMEM((kv_width,), bf16),
                pltpu.VMEM((rows, heads, n * chunk), f32),
                pltpu.VMEM((LHS_ROWS, depth), bf16),
                pltpu.VMEM((LHS_ROWS, width), f32),
                pltpu.VMEM((LHS_ROWS, 2 * kv_width), f32),
                pltpu.VMEM((rows, heads, head_dim), f32),
                pltpu.VMEM((rows, heads, head_dim), bf16),
                pltpu.VMEM((rows, kv_heads, head_dim), f32),
                pltpu.VMEM((rows, kv_heads, head_dim), f32),
                pltpu.VMEM((rows, heads, head_dim), f32),
                pltpu.VMEM((rows, heads, head_dim), f32),
                pltpu.VMEM((rows, heads, head_dim), f32),
                pltpu.VMEM((LHS_ROWS, width), f32),
                pltpu.VMEM((CORES, rows, chunk, head_dim), bf16),
                pltpu.VMEM((2, CORES, rows, chunk // 2, head_dim), bf16),
                pltpu.VMEM((2, CORES, rows, chunk // 2, head_dim), bf16),
                pltpu.SemaphoreType.DMA((6,)),
                pltpu.SemaphoreType.DMA((RING, PACK)),
                pltpu.SemaphoreType.DMA((2,)),
                pltpu.SemaphoreType.DMA((2, n)),
                pltpu.SemaphoreType.DMA((2, n)),
                pltpu.SemaphoreType.DMA((CORES,)),
                pltpu.SemaphoreType.DMA((2, CORES)),
                pltpu.SemaphoreType.DMA((2, CORES)),
            ],
            compiler_params=pltpu.CompilerParams(collective_id=0, has_side_effects=True, vmem_limit_bytes=8 * 1024 * 1024),
            cost_estimate=pl.CostEstimate(flops=1 << 30, bytes_accessed=1 << 27, transcendentals=0),
        )(prompt_lens, x_tok, norm_gain, b_q, b_k, b_v,
          k_cache.reshape(batch, chunk, head_dim), v_cache.reshape(batch, chunk, head_dim), w_q, w_k, w_v, w_o)
        y, k_out, v_out = pl.pallas_call(
            functools.partial(output_kernel, 14, depth // block // 2),
            out_shape=(jax.ShapeDtypeStruct((rows, depth), bf16), jax.ShapeDtypeStruct(land, bf16), jax.ShapeDtypeStruct(land, bf16)),
            in_specs=[vmem] * 5 + [hbm],
            out_specs=(vmem, hbm, hbm),
            scratch_shapes=[
                pltpu.VMEM((rows, depth), bf16),
                pltpu.VMEM((LHS_ROWS, depth), f32),
                pltpu.SemaphoreType.DMA((3,)),
            ],
            compiler_params=pltpu.CompilerParams(vmem_limit_bytes=8 * 1024 * 1024),
            cost_estimate=pl.CostEstimate(flops=1 << 30, bytes_accessed=1 << 25, transcendentals=0),
        )(*[pltpu.with_memory_space_constraint(a, pltpu.VMEM) for a in (o_rows, k_all, v_all, ring, y_part)], x_tok)
        shape = (rows, n * span, kv_heads, head_dim)
        return y, k_out.reshape(shape), v_out.reshape(shape)

    return jax.shard_map(per_device, mesh=mesh, in_specs=(batch_spec, P('dp'), seq_spec, seq_spec, whole, whole, whole, whole, whole, whole, whole, whole), out_specs=(batch_spec, batch_spec, batch_spec), check_vma=False)
```

```python
import functools
import math
import jax
import jax.numpy as jnp
from jax import lax
from jax.experimental import pallas as pl
from jax.experimental.pallas import tpu as pltpu
from jax.sharding import PartitionSpec as P

RMS_EPS = 1e-6
ROPE_THETA = 1000000.0
MASKED = -1e30
RING = 8
PACK = 5
TILE = 512
OUT_TILE = 512
LHS_ROWS = 16
CORES = 2
LAST = 3 * CORES
MESH = pl.DeviceIdType.MESH


def multiply_block(o_ref, r, weights, out):
    block, width = weights.shape
    lhs = o_ref[:, r * block:(r + 1) * block]
    for t in range(width // OUT_TILE):
        cols = slice(t * OUT_TILE, (t + 1) * OUT_TILE)
        out[:, cols] += jnp.dot(lhs, weights[:, cols], preferred_element_type=jnp.float32)


def exchange_kernel(dims, lens_hbm, x_hbm, gain_hbm, bq_hbm, bk_hbm, bv_hbm, k_ref, v_ref, wq_ref, wk_ref, wv_ref, wo_ref,
                    o_ref, k_land, v_land, ring, y_part,
                    lens_ref, x_ref, gain_ref, bq_ref, bk_ref, bv_ref,
                    scores, h_ref, acc, acc_kv, q_raw, q_rot, k_raw, v_raw, o_acc, m_acc, l_acc, o_row,
                    staged, packed, half_land, small_sem, ring_sem, own_sem, send_sem, recv_sem, stage_sem, half_send, half_recv):
    n, rows, span, kv_heads, head_dim, heads = dims
    group = heads // kv_heads
    width = heads * head_dim
    kv_width = kv_heads * head_dim
    chunk = span * kv_heads
    depth = x_ref.shape[1]
    half_dim = head_dim // 2
    block = depth // 10
    group_id = lax.axis_index("dp")
    me = lax.axis_index("cp")

    barrier = pltpu.get_barrier_semaphore()

    def greet(d, carry):
        peer = lax.rem(me + d, n)
        pl.semaphore_signal(barrier, inc=1, device_id=(group_id, peer), device_id_type=MESH)
        return carry

    lax.fori_loop(1, n, greet, 0)

    def weight_copies(b):
        slot = ring.at[b % RING]
        if b < 4:
            src = wk_ref if b < 2 else wv_ref
            base = (b % 2) * PACK
            return [pltpu.make_async_copy(src.at[pl.ds((base + c) * block, block)],
                                          slot.at[:, pl.ds(c * kv_width, kv_width)], ring_sem.at[b % RING, c])
                    for c in range(PACK)]
        src, r = (wq_ref, b - 4) if b < 14 else (wo_ref, b - 14)
        return [pltpu.make_async_copy(src.at[pl.ds(r * block, block)], slot, ring_sem.at[b % RING, 0])]

    def start_weights(b):
        for copy in weight_copies(b):
            copy.start()

    def wait_weights(b):
        for copy in weight_copies(b):
            copy.wait()

    def partner(i):
        offset, flip = pairs[i]
        chip = lax.rem(lax.div(me, CORES) + offset + n // CORES, n // CORES)
        return chip * CORES + lax.rem(lax.rem(me, CORES) + flip, CORES)

    def own_copy(c, src, land):
        return pltpu.make_async_copy(src.at[pl.ds(me * rows, rows)], land.at[:, pl.ds(me * chunk, chunk)], own_sem.at[c])

    def push(c, src, land, i):
        peer = partner(i)
        return pltpu.make_async_remote_copy(
            src_ref=src.at[pl.ds(peer * rows, rows)],
            dst_ref=land.at[:, pl.ds(me * chunk, chunk)],
            send_sem=send_sem.at[c, i], recv_sem=recv_sem.at[c, me],
            device_id=(group_id, peer), device_id_type=MESH)

    def arrival(c, land, source):
        return pltpu.make_async_remote_copy(
            src_ref=land.at[:, pl.ds(source * chunk, chunk)],
            dst_ref=land.at[:, pl.ds(source * chunk, chunk)],
            send_sem=send_sem.at[c, 0], recv_sem=recv_sem.at[c, source],
            device_id=(group_id, me), device_id_type=MESH)

    pl.semaphore_wait(barrier, n - 1)
    chips = n // CORES
    pairs = [(0, 1)]
    for d in range(1, (chips - 1) // 2 + 1):
        pairs += [(d, 0), (-d, 0), (d, 1), (-d, 1)]
    near = len(pairs)
    split = near - 2 * CORES
    if chips % 2 == 0:
        pairs += [(chips // 2, 0), (chips // 2, 1)]
    for c, src, land, peers in ((0, k_ref, k_land, range(near)), (1, v_ref, v_land, range(split)),
                                (0, k_ref, k_land, range(near, n - 1))):
        for i in peers:
            push(c, src, land, i).start()
    own_copy(0, k_ref, k_land).start()
    own_copy(1, v_ref, v_land).start()

    last = range(n - 1 - split)

    def mirrored(f):
        offset, flip = pairs[split + f]
        return pairs.index((-offset, flip)) - split if (-offset, flip) in pairs else f

    def stage_copy(f):
        return pltpu.make_async_copy(v_ref.at[pl.ds(partner(split + f) * rows, rows)], staged.at[f], stage_sem.at[f])

    def push_half(part, f):
        return pltpu.make_async_remote_copy(
            src_ref=packed.at[part, f], dst_ref=half_land.at[part, mirrored(f)],
            send_sem=half_send.at[part, f], recv_sem=half_recv.at[part, mirrored(f)],
            device_id=(group_id, partner(split + f)), device_id_type=MESH)

    def half_arrival(part, f):
        return pltpu.make_async_remote_copy(
            src_ref=half_land.at[part, f], dst_ref=half_land.at[part, f],
            send_sem=half_send.at[part, f], recv_sem=half_recv.at[part, f],
            device_id=(group_id, me), device_id_type=MESH)

    for f in last:
        stage_copy(f).start()
    small = [pltpu.make_async_copy(src, dst, small_sem.at[i]) for i, (src, dst) in enumerate((
        (lens_hbm, lens_ref), (x_hbm, x_ref), (gain_hbm, gain_ref), (bq_hbm, bq_ref), (bk_hbm, bk_ref), (bv_hbm, bv_ref)))]
    for copy in small:
        copy.start()
    for b in range(RING):
        start_weights(b)
    for copy in small:
        copy.wait()

    x_wide = x_ref[...].astype(jnp.float32)
    mean_sq = jnp.mean(x_wide * x_wide, axis=-1, keepdims=True)
    normed = x_wide * lax.rsqrt(mean_sq + RMS_EPS) * gain_ref[...].astype(jnp.float32).reshape(1, depth)
    h_ref[...] = jnp.concatenate([normed, jnp.zeros((LHS_ROWS - rows, depth), jnp.float32)], axis=0).astype(jnp.bfloat16)
    acc[...] = jnp.zeros_like(acc)
    acc_kv[...] = jnp.zeros_like(acc_kv)

    def multiply(lhs, slot, out, tile_count):
        def tile(t, carry):
            cols = pl.ds(pl.multiple_of(t * TILE, TILE), TILE)
            out[:, cols] += jnp.dot(lhs, ring[slot, :, cols], preferred_element_type=jnp.float32)
            return carry
        lax.fori_loop(0, tile_count, tile, 0)

    def multiply_kv(b):
        base = (b % 2) * PACK
        out = (b // 2) * kv_width
        slot = b % RING
        def part(c, carry):
            lhs = h_ref[:, pl.ds(pl.multiple_of((base + c) * block, block), block)]
            for t in range(kv_width // TILE):
                cols = pl.ds(out + t * TILE, TILE)
                src = pl.ds(pl.multiple_of(c * kv_width + t * TILE, TILE), TILE)
                acc_kv[:, cols] += jnp.dot(lhs, ring[slot, :, src], preferred_element_type=jnp.float32)
            return carry
        lax.fori_loop(0, PACK, part, 0)

    half = kv_heads // 2
    tile_row = lax.broadcasted_iota(jnp.int32, (span // 2, kv_heads, head_dim), 1)
    for f in last:
        stage_copy(f).wait()
        for s in range(rows):
            pair = staged[f, s].astype(jnp.float32).reshape(span // 2, 2, kv_heads, head_dim)
            even, odd = pair[:, 0], pair[:, 1]
            for part, both in enumerate((jnp.where(tile_row < half, even, pltpu.roll(odd, half, 1)),
                                         jnp.where(tile_row < half, pltpu.roll(even, half, 1), odd))):
                packed[part, f, s] = both.reshape(chunk // 2, head_dim).astype(jnp.bfloat16)

    for b in range(4):
        wait_weights(b)
        multiply_kv(b)
        start_weights(b + RING)
    for b in range(4, 14):
        wait_weights(b)
        multiply(h_ref[:, pl.ds((b - 4) * block, block)], b % RING, acc, width // TILE)
        if b + RING < 14 + RING:
            start_weights(b + RING)

    for part in range(2):
        for f in last:
            push_half(part, f).start()

    lane = lax.broadcasted_iota(jnp.int32, (1, head_dim), 1)
    freq_idx = jnp.where(lane < half_dim, lane, lane - half_dim).astype(jnp.float32)
    inv_freq = jnp.exp(freq_idx * (-2.0 * math.log(ROPE_THETA) / head_dim))
    sign = jnp.where(lane < half_dim, -1.0, 1.0)
    q_bias = bq_ref[...].astype(jnp.float32).reshape(heads, head_dim)
    k_bias = bk_ref[...].astype(jnp.float32).reshape(kv_heads, head_dim)
    v_bias = bv_ref[...].astype(jnp.float32).reshape(kv_heads, head_dim)
    for s in range(rows):
        for j in range(heads):
            q_raw[s, pl.ds(j, 1), :] = acc[pl.ds(s, 1), j * head_dim:(j + 1) * head_dim]
        for j in range(kv_heads):
            k_raw[s, pl.ds(j, 1), :] = acc_kv[pl.ds(s, 1), j * head_dim:(j + 1) * head_dim]
            v_raw[s, pl.ds(j, 1), :] = acc_kv[pl.ds(s, 1), kv_width + j * head_dim:kv_width + (j + 1) * head_dim]
    for s in range(rows):
        angle = lens_ref[me * rows + s].astype(jnp.float32) * inv_freq
        cos_t = jnp.cos(angle)
        sin_t = jnp.sin(angle) * sign
        q_one = q_raw[s] + q_bias
        q_rot[s] = (q_one * cos_t + pltpu.roll(q_one, half_dim, 1) * sin_t).astype(jnp.bfloat16)
        k_one = k_raw[s] + k_bias
        k_raw[s] = (k_one * cos_t + pltpu.roll(k_one, half_dim, 1) * sin_t).astype(jnp.bfloat16).astype(jnp.float32)
        v_raw[s] = (v_raw[s] + v_bias).astype(jnp.bfloat16).astype(jnp.float32)

    row_idx = lax.broadcasted_iota(jnp.int32, (span, kv_heads, head_dim), 0)
    col = lax.broadcasted_iota(jnp.int32, (heads, chunk), 1)
    head = lax.broadcasted_iota(jnp.int32, (heads, chunk), 0)
    own_head = (col % kv_heads) == (head // group)
    col_slot = col // kv_heads
    scale = head_dim ** -0.5

    def settle(land, s, source, fresh):
        place = pl.ds(pl.multiple_of(source * chunk, chunk), chunk)
        limit = lens_ref[me * rows + s] - source * span
        old = land[s, place, :].astype(jnp.float32).reshape(span, kv_heads, head_dim)
        kept = jnp.where(row_idx < limit, old, jnp.where(row_idx == limit, fresh[s][None], 0.0))
        kept = kept.reshape(chunk, head_dim).astype(jnp.bfloat16)
        land[s, place, :] = kept
        return kept, place, limit

    def lane_fold(op, values):
        out = values[:, :head_dim]
        for t in range(1, chunk // head_dim):
            out = op(out, values[:, t * head_dim:(t + 1) * head_dim])
        return out

    def score_chunk(source):
        for s in range(rows):
            keys, place, limit = settle(k_land, s, source, k_raw)
            sc = lax.dot_general(q_rot[s], keys, (((1,), (1,)), ((), ())), preferred_element_type=jnp.float32) * scale
            sc = jnp.where(own_head & (col_slot <= limit), sc, MASKED)
            scores[s, :, place] = sc
            m_acc[s] = jnp.maximum(m_acc[s], lane_fold(jnp.maximum, sc))

    head_row = lax.broadcasted_iota(jnp.int32, (span, kv_heads, head_dim), 1)

    def settle_half(s, f, source, part):
        place = pl.ds(pl.multiple_of(source * chunk, chunk), chunk)
        limit = lens_ref[me * rows + s] - source * span
        both = half_land[part, f, s].astype(jnp.float32).reshape(span // 2, kv_heads, head_dim)
        turned = pltpu.roll(both, half, 1)
        even, odd = (both, turned) if part == 0 else (turned, both)
        old = jnp.stack([even, odd], axis=1).reshape(span, kv_heads, head_dim)
        kept = jnp.where(row_idx < limit, old, jnp.where(row_idx == limit, v_raw[s][None], 0.0))
        mine = head_row < half if part == 0 else head_row >= half
        kept = jnp.where(mine, kept, 0.0)
        full = kept
        if part:
            full = jnp.where(mine, kept, v_land[s, place, :].astype(jnp.float32).reshape(span, kv_heads, head_dim))
        v_land[s, place, :] = full.reshape(chunk, head_dim).astype(jnp.bfloat16)
        return kept.reshape(chunk, head_dim).astype(jnp.bfloat16), place

    def weigh(s, place, vals, count):
        e = jnp.exp(scores[s, :, place] - m_acc[s][:, :1])
        if count:
            l_acc[s] += lane_fold(jnp.add, e)
        o_acc[s] += jnp.dot(e.astype(jnp.bfloat16), vals, preferred_element_type=jnp.float32)

    def value_chunk(source):
        for s in range(rows):
            vals, place, _ = settle(v_land, s, source, v_raw)
            weigh(s, place, vals, True)

    def value_half(part):
        for f in last:
            half_arrival(part, f).wait_recv()
            for s in range(rows):
                vals, place = settle_half(s, f, partner(split + f), part)
                weigh(s, place, vals, part == 0)

    def finish_heads(part):
        start, stop = part * heads // 2, (part + 1) * heads // 2
        for s in range(rows):
            l_all = jnp.sum(l_acc[s, pl.ds(start, stop - start), :], axis=-1, keepdims=True)
            q_raw[s, pl.ds(start, stop - start), :] = o_acc[s, pl.ds(start, stop - start), :] / l_all
            for j in range(start, stop):
                o_row[pl.ds(s, 1), j * head_dim:(j + 1) * head_dim] = q_raw[s, pl.ds(j, 1), :]
        cols = slice(start * head_dim, stop * head_dim)
        o_ref[:, cols] = o_row[:, cols].astype(jnp.bfloat16)

    m_acc[...] = jnp.full_like(m_acc, MASKED)
    l_acc[...] = jnp.zeros_like(l_acc)
    o_acc[...] = jnp.zeros_like(o_acc)

    own_copy(0, k_ref, k_land).wait()
    score_chunk(me)
    for i in range(n - 1):
        source = partner(i)
        arrival(0, k_land, source).wait_recv()
        score_chunk(source)
    for s in range(rows):
        m_acc[s] = jnp.broadcast_to(jnp.max(m_acc[s], axis=-1, keepdims=True), (heads, head_dim))
    own_copy(1, v_ref, v_land).wait()
    value_chunk(me)
    for i in range(split):
        source = partner(i)
        arrival(1, v_land, source).wait_recv()
        value_chunk(source)
    o_row[...] = jnp.zeros_like(o_row)
    y_part[...] = jnp.zeros_like(y_part)
    value_half(0)
    finish_heads(0)
    for r in range(depth // block // 2):
        wait_weights(14 + r)
        multiply_block(o_ref, r, ring.at[(14 + r) % RING], y_part)
        if 14 + r + RING < 24:
            start_weights(14 + r + RING)
    value_half(1)
    finish_heads(1)
    for r in range(depth // block // 2, depth // block):
        wait_weights(14 + r)
    for c, (src, land) in enumerate(((k_ref, k_land), (v_ref, v_land))):
        for i in range(n - 1 if c == 0 else split):
            push(c, src, land, i).wait_send()
    for part in range(2):
        for f in last:
            push_half(part, f).wait_send()


def output_kernel(first, start, o_ref, k_land, v_land, ring, y_part, x_hbm, y_ref, k_out, v_out, x_ref, acc, sem):
    rows, depth = x_ref.shape
    block = ring.shape[1]
    copies = [pltpu.make_async_copy(k_land, k_out, sem.at[0]),
              pltpu.make_async_copy(v_land, v_out, sem.at[1]),
              pltpu.make_async_copy(x_hbm, x_ref, sem.at[2])]
    for copy in copies:
        copy.start()
    acc[...] = y_part[...]
    for r in range(start, depth // block):
        multiply_block(o_ref, r, ring.at[(first + r) % ring.shape[0]], acc)
    for copy in copies:
        copy.wait()
    y_ref[...] = (x_ref[...].astype(jnp.float32) + acc[:rows, :]).astype(jnp.bfloat16)


def solution(mesh):
    batch_spec = P(('dp', 'cp'))
    seq_spec = P('dp', 'cp')
    whole = P()
    n = mesh.shape['cp']

    def per_device(x_tok, prompt_lens, k_cache, v_cache, norm_gain, w_q, b_q, w_k, b_k, w_v, b_v, w_o):
        rows, depth = x_tok.shape
        batch, span, kv_heads, head_dim = k_cache.shape
        width = w_q.shape[1]
        heads = width // head_dim
        chunk = span * kv_heads
        kv_width = kv_heads * head_dim
        block = depth // 10
        dims = (n, rows, span, kv_heads, head_dim, heads)
        vmem = pl.BlockSpec(memory_space=pltpu.VMEM)
        smem = pl.BlockSpec(memory_space=pltpu.SMEM)
        hbm = pl.BlockSpec(memory_space=pl.ANY)
        bf16, f32 = jnp.bfloat16, jnp.float32
        land = (rows, n * chunk, head_dim)
        o_rows, k_all, v_all, ring, y_part = pl.pallas_call(
            functools.partial(exchange_kernel, dims),
            out_shape=(pltpu.VMEM((LHS_ROWS, width), bf16), pltpu.VMEM(land, bf16), pltpu.VMEM(land, bf16),
                       pltpu.VMEM((RING, block, width), bf16), pltpu.VMEM((LHS_ROWS, depth), f32)),
            in_specs=[hbm] * 12,
            out_specs=(vmem,) * 5,
            scratch_shapes=[
                pltpu.SMEM((batch,), jnp.int32),
                pltpu.VMEM((rows, depth), bf16),
                pltpu.VMEM((depth,), bf16),
                pltpu.VMEM((width,), bf16),
                pltpu.VMEM((kv_width,), bf16),
                pltpu.VMEM((kv_width,), bf16),
                pltpu.VMEM((rows, heads, n * chunk), f32),
                pltpu.VMEM((LHS_ROWS, depth), bf16),
                pltpu.VMEM((LHS_ROWS, width), f32),
                pltpu.VMEM((LHS_ROWS, 2 * kv_width), f32),
                pltpu.VMEM((rows, heads, head_dim), f32),
                pltpu.VMEM((rows, heads, head_dim), bf16),
                pltpu.VMEM((rows, kv_heads, head_dim), f32),
                pltpu.VMEM((rows, kv_heads, head_dim), f32),
                pltpu.VMEM((rows, heads, head_dim), f32),
                pltpu.VMEM((rows, heads, head_dim), f32),
                pltpu.VMEM((rows, heads, head_dim), f32),
                pltpu.VMEM((LHS_ROWS, width), f32),
                pltpu.VMEM((LAST, rows, chunk, head_dim), bf16),
                pltpu.VMEM((2, LAST, rows, chunk // 2, head_dim), bf16),
                pltpu.VMEM((2, LAST, rows, chunk // 2, head_dim), bf16),
                pltpu.SemaphoreType.DMA((6,)),
                pltpu.SemaphoreType.DMA((RING, PACK)),
                pltpu.SemaphoreType.DMA((2,)),
                pltpu.SemaphoreType.DMA((2, n)),
                pltpu.SemaphoreType.DMA((2, n)),
                pltpu.SemaphoreType.DMA((LAST,)),
                pltpu.SemaphoreType.DMA((2, LAST)),
                pltpu.SemaphoreType.DMA((2, LAST)),
            ],
            compiler_params=pltpu.CompilerParams(collective_id=0, has_side_effects=True, vmem_limit_bytes=9 * 1024 * 1024),
            cost_estimate=pl.CostEstimate(flops=1 << 30, bytes_accessed=1 << 27, transcendentals=0),
        )(prompt_lens, x_tok, norm_gain, b_q, b_k, b_v,
          k_cache.reshape(batch, chunk, head_dim), v_cache.reshape(batch, chunk, head_dim), w_q, w_k, w_v, w_o)
        y, k_out, v_out = pl.pallas_call(
            functools.partial(output_kernel, 14, depth // block // 2),
            out_shape=(jax.ShapeDtypeStruct((rows, depth), bf16), jax.ShapeDtypeStruct(land, bf16), jax.ShapeDtypeStruct(land, bf16)),
            in_specs=[vmem] * 5 + [hbm],
            out_specs=(vmem, hbm, hbm),
            scratch_shapes=[
                pltpu.VMEM((rows, depth), bf16),
                pltpu.VMEM((LHS_ROWS, depth), f32),
                pltpu.SemaphoreType.DMA((3,)),
            ],
            compiler_params=pltpu.CompilerParams(vmem_limit_bytes=9 * 1024 * 1024),
            cost_estimate=pl.CostEstimate(flops=1 << 30, bytes_accessed=1 << 25, transcendentals=0),
        )(*[pltpu.with_memory_space_constraint(a, pltpu.VMEM) for a in (o_rows, k_all, v_all, ring, y_part)], x_tok)
        shape = (rows, n * span, kv_heads, head_dim)
        return y, k_out.reshape(shape), v_out.reshape(shape)

    return jax.shard_map(per_device, mesh=mesh, in_specs=(batch_spec, P('dp'), seq_spec, seq_spec, whole, whole, whole, whole, whole, whole, whole, whole), out_specs=(batch_spec, batch_spec, batch_spec), check_vma=False)
```

```python
import functools
import math
import jax
import jax.numpy as jnp
from jax import lax
from jax.experimental import pallas as pl
from jax.experimental.pallas import tpu as pltpu
from jax.sharding import PartitionSpec as P

RMS_EPS = 1e-6
ROPE_THETA = 1000000.0
MASKED = -1e30
RING = 8
PACK = 5
TILE = 512
OUT_TILE = 512
LHS_ROWS = 16
CORES = 2
MESH = pl.DeviceIdType.MESH


def multiply_block(o_ref, r, weights, out):
    block, width = weights.shape
    lhs = o_ref[:, r * block:(r + 1) * block]
    for t in range(width // OUT_TILE):
        cols = slice(t * OUT_TILE, (t + 1) * OUT_TILE)
        out[:, cols] += jnp.dot(lhs, weights[:, cols], preferred_element_type=jnp.float32)


def exchange_kernel(dims, lens_hbm, x_hbm, gain_hbm, bq_hbm, bk_hbm, bv_hbm, k_ref, v_ref, wq_ref, wk_ref, wv_ref, wo_ref,
                    o_ref, k_land, v_land, ring, y_part,
                    lens_ref, x_ref, gain_ref, bq_ref, bk_ref, bv_ref,
                    scores, h_ref, acc, acc_kv, q_raw, q_rot, k_raw, v_raw, o_acc, m_acc, l_acc, o_row,
                    staged, packed, half_land, small_sem, ring_sem, own_sem, send_sem, recv_sem, stage_sem, half_send, half_recv):
    n, rows, span, kv_heads, head_dim, heads = dims
    group = heads // kv_heads
    width = heads * head_dim
    kv_width = kv_heads * head_dim
    chunk = span * kv_heads
    depth = x_ref.shape[1]
    half_dim = head_dim // 2
    block = depth // 10
    group_id = lax.axis_index("dp")
    me = lax.axis_index("cp")

    barrier = pltpu.get_barrier_semaphore()

    def greet(d, carry):
        peer = lax.rem(me + d, n)
        pl.semaphore_signal(barrier, inc=1, device_id=(group_id, peer), device_id_type=MESH)
        return carry

    lax.fori_loop(1, n, greet, 0)

    def weight_copies(b):
        slot = ring.at[b % RING]
        if b < 4:
            src = wk_ref if b < 2 else wv_ref
            base = (b % 2) * PACK
            return [pltpu.make_async_copy(src.at[pl.ds((base + c) * block, block)],
                                          slot.at[:, pl.ds(c * kv_width, kv_width)], ring_sem.at[b % RING, c])
                    for c in range(PACK)]
        src, r = (wq_ref, b - 4) if b < 14 else (wo_ref, b - 14)
        return [pltpu.make_async_copy(src.at[pl.ds(r * block, block)], slot, ring_sem.at[b % RING, 0])]

    def start_weights(b):
        for copy in weight_copies(b):
            copy.start()

    def wait_weights(b):
        for copy in weight_copies(b):
            copy.wait()

    def partner(i):
        offset, flip = pairs[i]
        chip = lax.rem(lax.div(me, CORES) + offset + n // CORES, n // CORES)
        return chip * CORES + lax.rem(lax.rem(me, CORES) + flip, CORES)

    def own_copy(c, src, land):
        return pltpu.make_async_copy(src.at[pl.ds(me * rows, rows)], land.at[:, pl.ds(me * chunk, chunk)], own_sem.at[c])

    def push(c, src, land, i):
        peer = partner(i)
        return pltpu.make_async_remote_copy(
            src_ref=src.at[pl.ds(peer * rows, rows)],
            dst_ref=land.at[:, pl.ds(me * chunk, chunk)],
            send_sem=send_sem.at[c, i], recv_sem=recv_sem.at[c, me],
            device_id=(group_id, peer), device_id_type=MESH)

    def arrival(c, land, source):
        return pltpu.make_async_remote_copy(
            src_ref=land.at[:, pl.ds(source * chunk, chunk)],
            dst_ref=land.at[:, pl.ds(source * chunk, chunk)],
            send_sem=send_sem.at[c, 0], recv_sem=recv_sem.at[c, source],
            device_id=(group_id, me), device_id_type=MESH)

    pl.semaphore_wait(barrier, n - 1)
    chips = n // CORES
    pairs = [(0, 1)]
    for d in range(1, (chips - 1) // 2 + 1):
        pairs += [(d, 0), (-d, 0), (d, 1), (-d, 1)]
    near = len(pairs)
    if chips % 2 == 0:
        pairs += [(chips // 2, 0), (chips // 2, 1)]
    for c, src, land, peers in ((0, k_ref, k_land, range(n - 1)), (1, v_ref, v_land, range(near))):
        for i in peers:
            push(c, src, land, i).start()
    own_copy(0, k_ref, k_land).start()
    own_copy(1, v_ref, v_land).start()

    last = range(n - 1 - near)

    def stage_copy(f):
        return pltpu.make_async_copy(v_ref.at[pl.ds(partner(near + f) * rows, rows)], staged.at[f], stage_sem.at[f])

    def push_half(part, f):
        return pltpu.make_async_remote_copy(
            src_ref=packed.at[part, f], dst_ref=half_land.at[part, f],
            send_sem=half_send.at[part, f], recv_sem=half_recv.at[part, f],
            device_id=(group_id, partner(near + f)), device_id_type=MESH)

    for f in last:
        stage_copy(f).start()
    small = [pltpu.make_async_copy(src, dst, small_sem.at[i]) for i, (src, dst) in enumerate((
        (lens_hbm, lens_ref), (x_hbm, x_ref), (gain_hbm, gain_ref), (bq_hbm, bq_ref), (bk_hbm, bk_ref), (bv_hbm, bv_ref)))]
    for copy in small:
        copy.start()
    for b in range(RING):
        start_weights(b)
    for copy in small:
        copy.wait()

    x_wide = x_ref[...].astype(jnp.float32)
    mean_sq = jnp.mean(x_wide * x_wide, axis=-1, keepdims=True)
    normed = x_wide * lax.rsqrt(mean_sq + RMS_EPS) * gain_ref[...].astype(jnp.float32).reshape(1, depth)
    h_ref[...] = jnp.concatenate([normed, jnp.zeros((LHS_ROWS - rows, depth), jnp.float32)], axis=0).astype(jnp.bfloat16)
    acc[...] = jnp.zeros_like(acc)
    acc_kv[...] = jnp.zeros_like(acc_kv)

    def multiply(lhs, slot, out, tile_count):
        def tile(t, carry):
            cols = pl.ds(pl.multiple_of(t * TILE, TILE), TILE)
            out[:, cols] += jnp.dot(lhs, ring[slot, :, cols], preferred_element_type=jnp.float32)
            return carry
        lax.fori_loop(0, tile_count, tile, 0)

    def multiply_kv(b):
        base = (b % 2) * PACK
        out = (b // 2) * kv_width
        slot = b % RING
        def part(c, carry):
            lhs = h_ref[:, pl.ds(pl.multiple_of((base + c) * block, block), block)]
            for t in range(kv_width // TILE):
                cols = pl.ds(out + t * TILE, TILE)
                src = pl.ds(pl.multiple_of(c * kv_width + t * TILE, TILE), TILE)
                acc_kv[:, cols] += jnp.dot(lhs, ring[slot, :, src], preferred_element_type=jnp.float32)
            return carry
        lax.fori_loop(0, PACK, part, 0)

    half = kv_heads // 2
    tile_row = lax.broadcasted_iota(jnp.int32, (span // 2, kv_heads, head_dim), 1)
    for f in last:
        stage_copy(f).wait()
        for s in range(rows):
            pair = staged[f, s].astype(jnp.float32).reshape(span // 2, 2, kv_heads, head_dim)
            even, odd = pair[:, 0], pair[:, 1]
            for part, both in enumerate((jnp.where(tile_row < half, even, pltpu.roll(odd, half, 1)),
                                         jnp.where(tile_row < half, pltpu.roll(even, half, 1), odd))):
                packed[part, f, s] = both.reshape(chunk // 2, head_dim).astype(jnp.bfloat16)

    for b in range(4):
        wait_weights(b)
        multiply_kv(b)
        start_weights(b + RING)
    for b in range(4, 14):
        wait_weights(b)
        multiply(h_ref[:, pl.ds((b - 4) * block, block)], b % RING, acc, width // TILE)
        if b + RING < 14 + RING:
            start_weights(b + RING)

    for part in range(2):
        for f in last:
            push_half(part, f).start()

    lane = lax.broadcasted_iota(jnp.int32, (1, head_dim), 1)
    freq_idx = jnp.where(lane < half_dim, lane, lane - half_dim).astype(jnp.float32)
    inv_freq = jnp.exp(freq_idx * (-2.0 * math.log(ROPE_THETA) / head_dim))
    sign = jnp.where(lane < half_dim, -1.0, 1.0)
    q_bias = bq_ref[...].astype(jnp.float32).reshape(heads, head_dim)
    k_bias = bk_ref[...].astype(jnp.float32).reshape(kv_heads, head_dim)
    v_bias = bv_ref[...].astype(jnp.float32).reshape(kv_heads, head_dim)
    for s in range(rows):
        for j in range(heads):
            q_raw[s, pl.ds(j, 1), :] = acc[pl.ds(s, 1), j * head_dim:(j + 1) * head_dim]
        for j in range(kv_heads):
            k_raw[s, pl.ds(j, 1), :] = acc_kv[pl.ds(s, 1), j * head_dim:(j + 1) * head_dim]
            v_raw[s, pl.ds(j, 1), :] = acc_kv[pl.ds(s, 1), kv_width + j * head_dim:kv_width + (j + 1) * head_dim]
    for s in range(rows):
        angle = lens_ref[me * rows + s].astype(jnp.float32) * inv_freq
        cos_t = jnp.cos(angle)
        sin_t = jnp.sin(angle) * sign
        q_one = q_raw[s] + q_bias
        q_rot[s] = (q_one * cos_t + pltpu.roll(q_one, half_dim, 1) * sin_t).astype(jnp.bfloat16)
        k_one = k_raw[s] + k_bias
        k_raw[s] = (k_one * cos_t + pltpu.roll(k_one, half_dim, 1) * sin_t).astype(jnp.bfloat16).astype(jnp.float32)
        v_raw[s] = (v_raw[s] + v_bias).astype(jnp.bfloat16).astype(jnp.float32)

    row_idx = lax.broadcasted_iota(jnp.int32, (span, kv_heads, head_dim), 0)
    col = lax.broadcasted_iota(jnp.int32, (heads, chunk), 1)
    head = lax.broadcasted_iota(jnp.int32, (heads, chunk), 0)
    own_head = (col % kv_heads) == (head // group)
    col_slot = col // kv_heads
    scale = head_dim ** -0.5

    def settle(land, s, source, fresh):
        place = pl.ds(pl.multiple_of(source * chunk, chunk), chunk)
        limit = lens_ref[me * rows + s] - source * span
        old = land[s, place, :].astype(jnp.float32).reshape(span, kv_heads, head_dim)
        kept = jnp.where(row_idx < limit, old, jnp.where(row_idx == limit, fresh[s][None], 0.0))
        kept = kept.reshape(chunk, head_dim).astype(jnp.bfloat16)
        land[s, place, :] = kept
        return kept, place, limit

    def lane_fold(op, values):
        out = values[:, :head_dim]
        for t in range(1, chunk // head_dim):
            out = op(out, values[:, t * head_dim:(t + 1) * head_dim])
        return out

    def score_chunk(source):
        for s in range(rows):
            keys, place, limit = settle(k_land, s, source, k_raw)
            sc = lax.dot_general(q_rot[s], keys, (((1,), (1,)), ((), ())), preferred_element_type=jnp.float32) * scale
            sc = jnp.where(own_head & (col_slot <= limit), sc, MASKED)
            scores[s, :, place] = sc
            m_acc[s] = jnp.maximum(m_acc[s], lane_fold(jnp.maximum, sc))

    head_row = lax.broadcasted_iota(jnp.int32, (span, kv_heads, head_dim), 1)

    def settle_half(s, f, source, part):
        place = pl.ds(pl.multiple_of(source * chunk, chunk), chunk)
        limit = lens_ref[me * rows + s] - source * span
        both = half_land[part, f, s].astype(jnp.float32).reshape(span // 2, kv_heads, head_dim)
        turned = pltpu.roll(both, half, 1)
        even, odd = (both, turned) if part == 0 else (turned, both)
        old = jnp.stack([even, odd], axis=1).reshape(span, kv_heads, head_dim)
        kept = jnp.where(row_idx < limit, old, jnp.where(row_idx == limit, v_raw[s][None], 0.0))
        mine = head_row < half if part == 0 else head_row >= half
        kept = jnp.where(mine, kept, 0.0)
        full = kept
        if part:
            full = jnp.where(mine, kept, v_land[s, place, :].astype(jnp.float32).reshape(span, kv_heads, head_dim))
        v_land[s, place, :] = full.reshape(chunk, head_dim).astype(jnp.bfloat16)
        return kept.reshape(chunk, head_dim).astype(jnp.bfloat16), place

    def weigh(s, place, vals, count):
        e = jnp.exp(scores[s, :, place] - m_acc[s][:, :1])
        if count:
            l_acc[s] += lane_fold(jnp.add, e)
        o_acc[s] += jnp.dot(e.astype(jnp.bfloat16), vals, preferred_element_type=jnp.float32)

    def value_chunk(source):
        for s in range(rows):
            vals, place, _ = settle(v_land, s, source, v_raw)
            weigh(s, place, vals, True)

    def value_half(part):
        for f in last:
            push_half(part, f).wait_recv()
            for s in range(rows):
                vals, place = settle_half(s, f, partner(near + f), part)
                weigh(s, place, vals, part == 0)

    def finish_heads(part):
        start, stop = part * heads // 2, (part + 1) * heads // 2
        for s in range(rows):
            l_all = jnp.sum(l_acc[s, pl.ds(start, stop - start), :], axis=-1, keepdims=True)
            q_raw[s, pl.ds(start, stop - start), :] = o_acc[s, pl.ds(start, stop - start), :] / l_all
            for j in range(start, stop):
                o_row[pl.ds(s, 1), j * head_dim:(j + 1) * head_dim] = q_raw[s, pl.ds(j, 1), :]
        cols = slice(start * head_dim, stop * head_dim)
        o_ref[:, cols] = o_row[:, cols].astype(jnp.bfloat16)

    m_acc[...] = jnp.full_like(m_acc, MASKED)
    l_acc[...] = jnp.zeros_like(l_acc)
    o_acc[...] = jnp.zeros_like(o_acc)

    own_copy(0, k_ref, k_land).wait()
    score_chunk(me)
    for i in range(n - 1):
        source = partner(i)
        arrival(0, k_land, source).wait_recv()
        score_chunk(source)
    for s in range(rows):
        m_acc[s] = jnp.broadcast_to(jnp.max(m_acc[s], axis=-1, keepdims=True), (heads, head_dim))
    own_copy(1, v_ref, v_land).wait()
    value_chunk(me)
    for i in range(near):
        source = partner(i)
        arrival(1, v_land, source).wait_recv()
        value_chunk(source)
    o_row[...] = jnp.zeros_like(o_row)
    y_part[...] = jnp.zeros_like(y_part)
    value_half(0)
    finish_heads(0)
    for r in range(depth // block // 2):
        wait_weights(14 + r)
        multiply_block(o_ref, r, ring.at[(14 + r) % RING], y_part)
        if 14 + r + RING < 24:
            start_weights(14 + r + RING)
    value_half(1)
    finish_heads(1)
    for r in range(depth // block // 2, depth // block):
        wait_weights(14 + r)
    for c, (src, land) in enumerate(((k_ref, k_land), (v_ref, v_land))):
        for i in range(n - 1 if c == 0 else near):
            push(c, src, land, i).wait_send()
    for part in range(2):
        for f in last:
            push_half(part, f).wait_send()


def output_kernel(first, start, o_ref, k_land, v_land, ring, y_part, x_hbm, y_ref, k_out, v_out, x_ref, acc, sem):
    rows, depth = x_ref.shape
    block = ring.shape[1]
    copies = [pltpu.make_async_copy(k_land, k_out, sem.at[0]),
              pltpu.make_async_copy(v_land, v_out, sem.at[1]),
              pltpu.make_async_copy(x_hbm, x_ref, sem.at[2])]
    for copy in copies:
        copy.start()
    acc[...] = y_part[...]
    for r in range(start, depth // block):
        multiply_block(o_ref, r, ring.at[(first + r) % ring.shape[0]], acc)
    for copy in copies:
        copy.wait()
    y_ref[...] = (x_ref[...].astype(jnp.float32) + acc[:rows, :]).astype(jnp.bfloat16)


def solution(mesh):
    batch_spec = P(('dp', 'cp'))
    seq_spec = P('dp', 'cp')
    whole = P()
    n = mesh.shape['cp']

    def per_device(x_tok, prompt_lens, k_cache, v_cache, norm_gain, w_q, b_q, w_k, b_k, w_v, b_v, w_o):
        rows, depth = x_tok.shape
        batch, span, kv_heads, head_dim = k_cache.shape
        width = w_q.shape[1]
        heads = width // head_dim
        chunk = span * kv_heads
        kv_width = kv_heads * head_dim
        block = depth // 10
        dims = (n, rows, span, kv_heads, head_dim, heads)
        vmem = pl.BlockSpec(memory_space=pltpu.VMEM)
        smem = pl.BlockSpec(memory_space=pltpu.SMEM)
        hbm = pl.BlockSpec(memory_space=pl.ANY)
        bf16, f32 = jnp.bfloat16, jnp.float32
        land = (rows, n * chunk, head_dim)
        o_rows, k_all, v_all, ring, y_part = pl.pallas_call(
            functools.partial(exchange_kernel, dims),
            out_shape=(pltpu.VMEM((LHS_ROWS, width), bf16), pltpu.VMEM(land, bf16), pltpu.VMEM(land, bf16),
                       pltpu.VMEM((RING, block, width), bf16), pltpu.VMEM((LHS_ROWS, depth), f32)),
            in_specs=[hbm] * 12,
            out_specs=(vmem,) * 5,
            scratch_shapes=[
                pltpu.SMEM((batch,), jnp.int32),
                pltpu.VMEM((rows, depth), bf16),
                pltpu.VMEM((depth,), bf16),
                pltpu.VMEM((width,), bf16),
                pltpu.VMEM((kv_width,), bf16),
                pltpu.VMEM((kv_width,), bf16),
                pltpu.VMEM((rows, heads, n * chunk), f32),
                pltpu.VMEM((LHS_ROWS, depth), bf16),
                pltpu.VMEM((LHS_ROWS, width), f32),
                pltpu.VMEM((LHS_ROWS, 2 * kv_width), f32),
                pltpu.VMEM((rows, heads, head_dim), f32),
                pltpu.VMEM((rows, heads, head_dim), bf16),
                pltpu.VMEM((rows, kv_heads, head_dim), f32),
                pltpu.VMEM((rows, kv_heads, head_dim), f32),
                pltpu.VMEM((rows, heads, head_dim), f32),
                pltpu.VMEM((rows, heads, head_dim), f32),
                pltpu.VMEM((rows, heads, head_dim), f32),
                pltpu.VMEM((LHS_ROWS, width), f32),
                pltpu.VMEM((CORES, rows, chunk, head_dim), bf16),
                pltpu.VMEM((2, CORES, rows, chunk // 2, head_dim), bf16),
                pltpu.VMEM((2, CORES, rows, chunk // 2, head_dim), bf16),
                pltpu.SemaphoreType.DMA((6,)),
                pltpu.SemaphoreType.DMA((RING, PACK)),
                pltpu.SemaphoreType.DMA((2,)),
                pltpu.SemaphoreType.DMA((2, n)),
                pltpu.SemaphoreType.DMA((2, n)),
                pltpu.SemaphoreType.DMA((CORES,)),
                pltpu.SemaphoreType.DMA((2, CORES)),
                pltpu.SemaphoreType.DMA((2, CORES)),
            ],
            compiler_params=pltpu.CompilerParams(collective_id=0, has_side_effects=True, vmem_limit_bytes=8 * 1024 * 1024),
            cost_estimate=pl.CostEstimate(flops=1 << 30, bytes_accessed=1 << 27, transcendentals=0),
        )(prompt_lens, x_tok, norm_gain, b_q, b_k, b_v,
          k_cache.reshape(batch, chunk, head_dim), v_cache.reshape(batch, chunk, head_dim), w_q, w_k, w_v, w_o)
        y, k_out, v_out = pl.pallas_call(
            functools.partial(output_kernel, 14, depth // block // 2),
            out_shape=(jax.ShapeDtypeStruct((rows, depth), bf16), jax.ShapeDtypeStruct(land, bf16), jax.ShapeDtypeStruct(land, bf16)),
            in_specs=[vmem] * 5 + [hbm],
            out_specs=(vmem, hbm, hbm),
            scratch_shapes=[
                pltpu.VMEM((rows, depth), bf16),
                pltpu.VMEM((LHS_ROWS, depth), f32),
                pltpu.SemaphoreType.DMA((3,)),
            ],
            compiler_params=pltpu.CompilerParams(vmem_limit_bytes=8 * 1024 * 1024),
            cost_estimate=pl.CostEstimate(flops=1 << 30, bytes_accessed=1 << 25, transcendentals=0),
        )(*[pltpu.with_memory_space_constraint(a, pltpu.VMEM) for a in (o_rows, k_all, v_all, ring, y_part)], x_tok)
        shape = (rows, n * span, kv_heads, head_dim)
        return y, k_out.reshape(shape), v_out.reshape(shape)

    return jax.shard_map(per_device, mesh=mesh, in_specs=(batch_spec, P('dp'), seq_spec, seq_spec, whole, whole, whole, whole, whole, whole, whole, whole), out_specs=(batch_spec, batch_spec, batch_spec), check_vma=False)
```

```python
import functools
import math
import jax
import jax.numpy as jnp
from jax import lax
from jax.experimental import pallas as pl
from jax.experimental.pallas import tpu as pltpu
from jax.sharding import PartitionSpec as P

RMS_EPS = 1e-6
ROPE_THETA = 1000000.0
MASKED = -1e30
RING = 8
PACK = 5
TILE = 512
OUT_TILE = 512
LHS_ROWS = 16
CORES = 2
MESH = pl.DeviceIdType.MESH


def multiply_block(o_ref, r, weights, out):
    block, width = weights.shape
    lhs = o_ref[:, r * block:(r + 1) * block]
    for t in range(width // OUT_TILE):
        cols = slice(t * OUT_TILE, (t + 1) * OUT_TILE)
        out[:, cols] += jnp.dot(lhs, weights[:, cols], preferred_element_type=jnp.float32)


def exchange_kernel(dims, lens_hbm, x_hbm, gain_hbm, bq_hbm, bk_hbm, bv_hbm, k_ref, v_ref, wq_ref, wk_ref, wv_ref, wo_ref,
                    o_ref, k_land, v_land, ring, y_part,
                    lens_ref, x_ref, gain_ref, bq_ref, bk_ref, bv_ref,
                    scores, h_ref, acc, acc_kv, q_raw, q_rot, k_raw, v_raw, o_acc, m_acc, l_acc, o_row,
                    staged, packed, half_land, small_sem, ring_sem, own_sem, send_sem, recv_sem, stage_sem, half_send, half_recv):
    n, rows, span, kv_heads, head_dim, heads = dims
    group = heads // kv_heads
    width = heads * head_dim
    kv_width = kv_heads * head_dim
    chunk = span * kv_heads
    depth = x_ref.shape[1]
    half_dim = head_dim // 2
    block = depth // 10
    group_id = lax.axis_index("dp")
    me = lax.axis_index("cp")

    barrier = pltpu.get_barrier_semaphore()

    def greet(d, carry):
        peer = lax.rem(me + d, n)
        pl.semaphore_signal(barrier, inc=1, device_id=(group_id, peer), device_id_type=MESH)
        return carry

    lax.fori_loop(1, n, greet, 0)

    def weight_copies(b):
        slot = ring.at[b % RING]
        if b < 4:
            src = wk_ref if b < 2 else wv_ref
            base = (b % 2) * PACK
            return [pltpu.make_async_copy(src.at[pl.ds((base + c) * block, block)],
                                          slot.at[:, pl.ds(c * kv_width, kv_width)], ring_sem.at[b % RING, c])
                    for c in range(PACK)]
        src, r = (wq_ref, b - 4) if b < 14 else (wo_ref, b - 14)
        return [pltpu.make_async_copy(src.at[pl.ds(r * block, block)], slot, ring_sem.at[b % RING, 0])]

    def start_weights(b):
        for copy in weight_copies(b):
            copy.start()

    def wait_weights(b):
        for copy in weight_copies(b):
            copy.wait()

    def partner(i):
        offset, flip = pairs[i]
        chip = lax.rem(lax.div(me, CORES) + offset + n // CORES, n // CORES)
        return chip * CORES + lax.rem(lax.rem(me, CORES) + flip, CORES)

    def own_copy(c, src, land):
        return pltpu.make_async_copy(src.at[pl.ds(me * rows, rows)], land.at[:, pl.ds(me * chunk, chunk)], own_sem.at[c])

    def push(c, src, land, i):
        peer = partner(i)
        return pltpu.make_async_remote_copy(
            src_ref=src.at[pl.ds(peer * rows, rows)],
            dst_ref=land.at[:, pl.ds(me * chunk, chunk)],
            send_sem=send_sem.at[c, i], recv_sem=recv_sem.at[c, me],
            device_id=(group_id, peer), device_id_type=MESH)

    def arrival(c, land, source):
        return pltpu.make_async_remote_copy(
            src_ref=land.at[:, pl.ds(source * chunk, chunk)],
            dst_ref=land.at[:, pl.ds(source * chunk, chunk)],
            send_sem=send_sem.at[c, 0], recv_sem=recv_sem.at[c, source],
            device_id=(group_id, me), device_id_type=MESH)

    pl.semaphore_wait(barrier, n - 1)
    chips = n // CORES
    pairs = [(0, 1)]
    for d in range(1, (chips - 1) // 2 + 1):
        pairs += [(d, 0), (-d, 0), (d, 1), (-d, 1)]
    near = len(pairs)
    split = near - 2 * CORES
    if chips % 2 == 0:
        pairs += [(chips // 2, 0), (chips // 2, 1)]
    for c, src, land, peers in ((0, k_ref, k_land, range(n - 1)), (1, v_ref, v_land, range(split))):
        for i in peers:
            push(c, src, land, i).start()
    own_copy(0, k_ref, k_land).start()
    own_copy(1, v_ref, v_land).start()

    last = range(n - 1 - near)

    def stage_copy(f):
        return pltpu.make_async_copy(v_ref.at[pl.ds(partner(near + f) * rows, rows)], staged.at[f], stage_sem.at[f])

    def push_half(part, f):
        return pltpu.make_async_remote_copy(
            src_ref=packed.at[part, f], dst_ref=half_land.at[part, f],
            send_sem=half_send.at[part, f], recv_sem=half_recv.at[part, f],
            device_id=(group_id, partner(near + f)), device_id_type=MESH)

    for f in last:
        stage_copy(f).start()
    small = [pltpu.make_async_copy(src, dst, small_sem.at[i]) for i, (src, dst) in enumerate((
        (lens_hbm, lens_ref), (x_hbm, x_ref), (gain_hbm, gain_ref), (bq_hbm, bq_ref), (bk_hbm, bk_ref), (bv_hbm, bv_ref)))]
    for copy in small:
        copy.start()
    for b in range(RING):
        start_weights(b)
    for copy in small:
        copy.wait()

    x_wide = x_ref[...].astype(jnp.float32)
    mean_sq = jnp.mean(x_wide * x_wide, axis=-1, keepdims=True)
    normed = x_wide * lax.rsqrt(mean_sq + RMS_EPS) * gain_ref[...].astype(jnp.float32).reshape(1, depth)
    h_ref[...] = jnp.concatenate([normed, jnp.zeros((LHS_ROWS - rows, depth), jnp.float32)], axis=0).astype(jnp.bfloat16)
    acc[...] = jnp.zeros_like(acc)
    acc_kv[...] = jnp.zeros_like(acc_kv)

    def multiply(lhs, slot, out, tile_count):
        def tile(t, carry):
            cols = pl.ds(pl.multiple_of(t * TILE, TILE), TILE)
            out[:, cols] += jnp.dot(lhs, ring[slot, :, cols], preferred_element_type=jnp.float32)
            return carry
        lax.fori_loop(0, tile_count, tile, 0)

    def multiply_kv(b):
        base = (b % 2) * PACK
        out = (b // 2) * kv_width
        slot = b % RING
        def part(c, carry):
            lhs = h_ref[:, pl.ds(pl.multiple_of((base + c) * block, block), block)]
            for t in range(kv_width // TILE):
                cols = pl.ds(out + t * TILE, TILE)
                src = pl.ds(pl.multiple_of(c * kv_width + t * TILE, TILE), TILE)
                acc_kv[:, cols] += jnp.dot(lhs, ring[slot, :, src], preferred_element_type=jnp.float32)
            return carry
        lax.fori_loop(0, PACK, part, 0)

    half = kv_heads // 2
    tile_row = lax.broadcasted_iota(jnp.int32, (span // 2, kv_heads, head_dim), 1)
    for f in last:
        stage_copy(f).wait()
        for s in range(rows):
            pair = staged[f, s].astype(jnp.float32).reshape(span // 2, 2, kv_heads, head_dim)
            even, odd = pair[:, 0], pair[:, 1]
            for part, both in enumerate((jnp.where(tile_row < half, even, pltpu.roll(odd, half, 1)),
                                         jnp.where(tile_row < half, pltpu.roll(even, half, 1), odd))):
                packed[part, f, s] = both.reshape(chunk // 2, head_dim).astype(jnp.bfloat16)

    for b in range(4):
        wait_weights(b)
        multiply_kv(b)
        start_weights(b + RING)
    for b in range(4, 14):
        wait_weights(b)
        multiply(h_ref[:, pl.ds((b - 4) * block, block)], b % RING, acc, width // TILE)
        if b + RING < 14 + RING:
            start_weights(b + RING)

    for f in last:
        push_half(0, f).start()
    for i in range(split, near):
        push(1, v_ref, v_land, i).start()
    for f in last:
        push_half(1, f).start()

    lane = lax.broadcasted_iota(jnp.int32, (1, head_dim), 1)
    freq_idx = jnp.where(lane < half_dim, lane, lane - half_dim).astype(jnp.float32)
    inv_freq = jnp.exp(freq_idx * (-2.0 * math.log(ROPE_THETA) / head_dim))
    sign = jnp.where(lane < half_dim, -1.0, 1.0)
    q_bias = bq_ref[...].astype(jnp.float32).reshape(heads, head_dim)
    k_bias = bk_ref[...].astype(jnp.float32).reshape(kv_heads, head_dim)
    v_bias = bv_ref[...].astype(jnp.float32).reshape(kv_heads, head_dim)
    for s in range(rows):
        for j in range(heads):
            q_raw[s, pl.ds(j, 1), :] = acc[pl.ds(s, 1), j * head_dim:(j + 1) * head_dim]
        for j in range(kv_heads):
            k_raw[s, pl.ds(j, 1), :] = acc_kv[pl.ds(s, 1), j * head_dim:(j + 1) * head_dim]
            v_raw[s, pl.ds(j, 1), :] = acc_kv[pl.ds(s, 1), kv_width + j * head_dim:kv_width + (j + 1) * head_dim]
    for s in range(rows):
        angle = lens_ref[me * rows + s].astype(jnp.float32) * inv_freq
        cos_t = jnp.cos(angle)
        sin_t = jnp.sin(angle) * sign
        q_one = q_raw[s] + q_bias
        q_rot[s] = (q_one * cos_t + pltpu.roll(q_one, half_dim, 1) * sin_t).astype(jnp.bfloat16)
        k_one = k_raw[s] + k_bias
        k_raw[s] = (k_one * cos_t + pltpu.roll(k_one, half_dim, 1) * sin_t).astype(jnp.bfloat16).astype(jnp.float32)
        v_raw[s] = (v_raw[s] + v_bias).astype(jnp.bfloat16).astype(jnp.float32)

    row_idx = lax.broadcasted_iota(jnp.int32, (span, kv_heads, head_dim), 0)
    col = lax.broadcasted_iota(jnp.int32, (heads, chunk), 1)
    head = lax.broadcasted_iota(jnp.int32, (heads, chunk), 0)
    own_head = (col % kv_heads) == (head // group)
    col_slot = col // kv_heads
    scale = head_dim ** -0.5

    def settle(land, s, source, fresh):
        place = pl.ds(pl.multiple_of(source * chunk, chunk), chunk)
        limit = lens_ref[me * rows + s] - source * span
        old = land[s, place, :].astype(jnp.float32).reshape(span, kv_heads, head_dim)
        kept = jnp.where(row_idx < limit, old, jnp.where(row_idx == limit, fresh[s][None], 0.0))
        kept = kept.reshape(chunk, head_dim).astype(jnp.bfloat16)
        land[s, place, :] = kept
        return kept, place, limit

    def lane_fold(op, values):
        out = values[:, :head_dim]
        for t in range(1, chunk // head_dim):
            out = op(out, values[:, t * head_dim:(t + 1) * head_dim])
        return out

    def score_chunk(source):
        for s in range(rows):
            keys, place, limit = settle(k_land, s, source, k_raw)
            sc = lax.dot_general(q_rot[s], keys, (((1,), (1,)), ((), ())), preferred_element_type=jnp.float32) * scale
            sc = jnp.where(own_head & (col_slot <= limit), sc, MASKED)
            scores[s, :, place] = sc
            m_acc[s] = jnp.maximum(m_acc[s], lane_fold(jnp.maximum, sc))

    head_row = lax.broadcasted_iota(jnp.int32, (span, kv_heads, head_dim), 1)

    def settle_half(s, f, source, part):
        place = pl.ds(pl.multiple_of(source * chunk, chunk), chunk)
        limit = lens_ref[me * rows + s] - source * span
        both = half_land[part, f, s].astype(jnp.float32).reshape(span // 2, kv_heads, head_dim)
        turned = pltpu.roll(both, half, 1)
        even, odd = (both, turned) if part == 0 else (turned, both)
        old = jnp.stack([even, odd], axis=1).reshape(span, kv_heads, head_dim)
        kept = jnp.where(row_idx < limit, old, jnp.where(row_idx == limit, v_raw[s][None], 0.0))
        mine = head_row < half if part == 0 else head_row >= half
        kept = jnp.where(mine, kept, 0.0)
        full = kept
        if part:
            full = jnp.where(mine, kept, v_land[s, place, :].astype(jnp.float32).reshape(span, kv_heads, head_dim))
        v_land[s, place, :] = full.reshape(chunk, head_dim).astype(jnp.bfloat16)
        return kept.reshape(chunk, head_dim).astype(jnp.bfloat16), place

    def weigh(s, place, vals, count):
        e = jnp.exp(scores[s, :, place] - m_acc[s][:, :1])
        if count:
            l_acc[s] += lane_fold(jnp.add, e)
        o_acc[s] += jnp.dot(e.astype(jnp.bfloat16), vals, preferred_element_type=jnp.float32)

    def value_chunk(source):
        for s in range(rows):
            vals, place, _ = settle(v_land, s, source, v_raw)
            weigh(s, place, vals, True)

    def value_half(part):
        for f in last:
            push_half(part, f).wait_recv()
            for s in range(rows):
                vals, place = settle_half(s, f, partner(near + f), part)
                weigh(s, place, vals, part == 0)

    def finish_heads(part):
        start, stop = part * heads // 2, (part + 1) * heads // 2
        for s in range(rows):
            l_all = jnp.sum(l_acc[s, pl.ds(start, stop - start), :], axis=-1, keepdims=True)
            q_raw[s, pl.ds(start, stop - start), :] = o_acc[s, pl.ds(start, stop - start), :] / l_all
            for j in range(start, stop):
                o_row[pl.ds(s, 1), j * head_dim:(j + 1) * head_dim] = q_raw[s, pl.ds(j, 1), :]
        cols = slice(start * head_dim, stop * head_dim)
        o_ref[:, cols] = o_row[:, cols].astype(jnp.bfloat16)

    m_acc[...] = jnp.full_like(m_acc, MASKED)
    l_acc[...] = jnp.zeros_like(l_acc)
    o_acc[...] = jnp.zeros_like(o_acc)

    own_copy(0, k_ref, k_land).wait()
    score_chunk(me)
    for i in range(n - 1):
        source = partner(i)
        arrival(0, k_land, source).wait_recv()
        score_chunk(source)
    for s in range(rows):
        m_acc[s] = jnp.broadcast_to(jnp.max(m_acc[s], axis=-1, keepdims=True), (heads, head_dim))
    own_copy(1, v_ref, v_land).wait()
    value_chunk(me)
    for i in range(near):
        source = partner(i)
        arrival(1, v_land, source).wait_recv()
        value_chunk(source)
    o_row[...] = jnp.zeros_like(o_row)
    y_part[...] = jnp.zeros_like(y_part)
    value_half(0)
    finish_heads(0)
    for r in range(depth // block // 2):
        wait_weights(14 + r)
        multiply_block(o_ref, r, ring.at[(14 + r) % RING], y_part)
        if 14 + r + RING < 24:
            start_weights(14 + r + RING)
    value_half(1)
    finish_heads(1)
    for r in range(depth // block // 2, depth // block):
        wait_weights(14 + r)
    for c, (src, land) in enumerate(((k_ref, k_land), (v_ref, v_land))):
        for i in range(n - 1 if c == 0 else near):
            push(c, src, land, i).wait_send()
    for part in range(2):
        for f in last:
            push_half(part, f).wait_send()


def output_kernel(first, start, o_ref, k_land, v_land, ring, y_part, x_hbm, y_ref, k_out, v_out, x_ref, acc, sem):
    rows, depth = x_ref.shape
    block = ring.shape[1]
    copies = [pltpu.make_async_copy(k_land, k_out, sem.at[0]),
              pltpu.make_async_copy(v_land, v_out, sem.at[1]),
              pltpu.make_async_copy(x_hbm, x_ref, sem.at[2])]
    for copy in copies:
        copy.start()
    acc[...] = y_part[...]
    for r in range(start, depth // block):
        multiply_block(o_ref, r, ring.at[(first + r) % ring.shape[0]], acc)
    for copy in copies:
        copy.wait()
    y_ref[...] = (x_ref[...].astype(jnp.float32) + acc[:rows, :]).astype(jnp.bfloat16)


def solution(mesh):
    batch_spec = P(('dp', 'cp'))
    seq_spec = P('dp', 'cp')
    whole = P()
    n = mesh.shape['cp']

    def per_device(x_tok, prompt_lens, k_cache, v_cache, norm_gain, w_q, b_q, w_k, b_k, w_v, b_v, w_o):
        rows, depth = x_tok.shape
        batch, span, kv_heads, head_dim = k_cache.shape
        width = w_q.shape[1]
        heads = width // head_dim
        chunk = span * kv_heads
        kv_width = kv_heads * head_dim
        block = depth // 10
        dims = (n, rows, span, kv_heads, head_dim, heads)
        vmem = pl.BlockSpec(memory_space=pltpu.VMEM)
        smem = pl.BlockSpec(memory_space=pltpu.SMEM)
        hbm = pl.BlockSpec(memory_space=pl.ANY)
        bf16, f32 = jnp.bfloat16, jnp.float32
        land = (rows, n * chunk, head_dim)
        o_rows, k_all, v_all, ring, y_part = pl.pallas_call(
            functools.partial(exchange_kernel, dims),
            out_shape=(pltpu.VMEM((LHS_ROWS, width), bf16), pltpu.VMEM(land, bf16), pltpu.VMEM(land, bf16),
                       pltpu.VMEM((RING, block, width), bf16), pltpu.VMEM((LHS_ROWS, depth), f32)),
            in_specs=[hbm] * 12,
            out_specs=(vmem,) * 5,
            scratch_shapes=[
                pltpu.SMEM((batch,), jnp.int32),
                pltpu.VMEM((rows, depth), bf16),
                pltpu.VMEM((depth,), bf16),
                pltpu.VMEM((width,), bf16),
                pltpu.VMEM((kv_width,), bf16),
                pltpu.VMEM((kv_width,), bf16),
                pltpu.VMEM((rows, heads, n * chunk), f32),
                pltpu.VMEM((LHS_ROWS, depth), bf16),
                pltpu.VMEM((LHS_ROWS, width), f32),
                pltpu.VMEM((LHS_ROWS, 2 * kv_width), f32),
                pltpu.VMEM((rows, heads, head_dim), f32),
                pltpu.VMEM((rows, heads, head_dim), bf16),
                pltpu.VMEM((rows, kv_heads, head_dim), f32),
                pltpu.VMEM((rows, kv_heads, head_dim), f32),
                pltpu.VMEM((rows, heads, head_dim), f32),
                pltpu.VMEM((rows, heads, head_dim), f32),
                pltpu.VMEM((rows, heads, head_dim), f32),
                pltpu.VMEM((LHS_ROWS, width), f32),
                pltpu.VMEM((CORES, rows, chunk, head_dim), bf16),
                pltpu.VMEM((2, CORES, rows, chunk // 2, head_dim), bf16),
                pltpu.VMEM((2, CORES, rows, chunk // 2, head_dim), bf16),
                pltpu.SemaphoreType.DMA((6,)),
                pltpu.SemaphoreType.DMA((RING, PACK)),
                pltpu.SemaphoreType.DMA((2,)),
                pltpu.SemaphoreType.DMA((2, n)),
                pltpu.SemaphoreType.DMA((2, n)),
                pltpu.SemaphoreType.DMA((CORES,)),
                pltpu.SemaphoreType.DMA((2, CORES)),
                pltpu.SemaphoreType.DMA((2, CORES)),
            ],
            compiler_params=pltpu.CompilerParams(collective_id=0, has_side_effects=True, vmem_limit_bytes=8 * 1024 * 1024),
            cost_estimate=pl.CostEstimate(flops=1 << 30, bytes_accessed=1 << 27, transcendentals=0),
        )(prompt_lens, x_tok, norm_gain, b_q, b_k, b_v,
          k_cache.reshape(batch, chunk, head_dim), v_cache.reshape(batch, chunk, head_dim), w_q, w_k, w_v, w_o)
        y, k_out, v_out = pl.pallas_call(
            functools.partial(output_kernel, 14, depth // block // 2),
            out_shape=(jax.ShapeDtypeStruct((rows, depth), bf16), jax.ShapeDtypeStruct(land, bf16), jax.ShapeDtypeStruct(land, bf16)),
            in_specs=[vmem] * 5 + [hbm],
            out_specs=(vmem, hbm, hbm),
            scratch_shapes=[
                pltpu.VMEM((rows, depth), bf16),
                pltpu.VMEM((LHS_ROWS, depth), f32),
                pltpu.SemaphoreType.DMA((3,)),
            ],
            compiler_params=pltpu.CompilerParams(vmem_limit_bytes=8 * 1024 * 1024),
            cost_estimate=pl.CostEstimate(flops=1 << 30, bytes_accessed=1 << 25, transcendentals=0),
        )(*[pltpu.with_memory_space_constraint(a, pltpu.VMEM) for a in (o_rows, k_all, v_all, ring, y_part)], x_tok)
        shape = (rows, n * span, kv_heads, head_dim)
        return y, k_out.reshape(shape), v_out.reshape(shape)

    return jax.shard_map(per_device, mesh=mesh, in_specs=(batch_spec, P('dp'), seq_spec, seq_spec, whole, whole, whole, whole, whole, whole, whole, whole), out_specs=(batch_spec, batch_spec, batch_spec), check_vma=False)
```

```python
import functools
import math
import jax
import jax.numpy as jnp
from jax import lax
from jax.experimental import pallas as pl
from jax.experimental.pallas import tpu as pltpu
from jax.sharding import PartitionSpec as P

RMS_EPS = 1e-6
ROPE_THETA = 1000000.0
MASKED = -1e30
RING = 8
PACK = 5
TILE = 512
OUT_TILE = 512
LHS_ROWS = 16
CORES = 2
MESH = pl.DeviceIdType.MESH


def multiply_block(o_ref, r, weights, out):
    block, width = weights.shape
    lhs = o_ref[:, r * block:(r + 1) * block]
    for t in range(width // OUT_TILE):
        cols = slice(t * OUT_TILE, (t + 1) * OUT_TILE)
        out[:, cols] += jnp.dot(lhs, weights[:, cols], preferred_element_type=jnp.float32)


def exchange_kernel(dims, lens_hbm, x_hbm, gain_hbm, bq_hbm, bk_hbm, bv_hbm, k_ref, v_ref, wq_ref, wk_ref, wv_ref, wo_ref,
                    o_ref, k_land, v_land, ring, y_part,
                    lens_ref, x_ref, gain_ref, bq_ref, bk_ref, bv_ref,
                    scores, h_ref, acc, acc_kv, q_raw, q_rot, k_raw, v_raw, o_acc, m_acc, l_acc, o_row,
                    staged, packed, half_land, small_sem, ring_sem, own_sem, send_sem, recv_sem, stage_sem, half_send, half_recv):
    n, rows, span, kv_heads, head_dim, heads = dims
    group = heads // kv_heads
    width = heads * head_dim
    kv_width = kv_heads * head_dim
    chunk = span * kv_heads
    depth = x_ref.shape[1]
    half_dim = head_dim // 2
    block = depth // 10
    group_id = lax.axis_index("dp")
    me = lax.axis_index("cp")

    barrier = pltpu.get_barrier_semaphore()

    def greet(d, carry):
        peer = lax.rem(me + d, n)
        pl.semaphore_signal(barrier, inc=1, device_id=(group_id, peer), device_id_type=MESH)
        return carry

    lax.fori_loop(1, n, greet, 0)

    def weight_copies(b):
        slot = ring.at[b % RING]
        if b < 4:
            src = wk_ref if b < 2 else wv_ref
            base = (b % 2) * PACK
            return [pltpu.make_async_copy(src.at[pl.ds((base + c) * block, block)],
                                          slot.at[:, pl.ds(c * kv_width, kv_width)], ring_sem.at[b % RING, c])
                    for c in range(PACK)]
        src, r = (wq_ref, b - 4) if b < 14 else (wo_ref, b - 14)
        return [pltpu.make_async_copy(src.at[pl.ds(r * block, block)], slot, ring_sem.at[b % RING, 0])]

    def start_weights(b):
        for copy in weight_copies(b):
            copy.start()

    def wait_weights(b):
        for copy in weight_copies(b):
            copy.wait()

    def partner(i):
        offset, flip = pairs[i]
        chip = lax.rem(lax.div(me, CORES) + offset + n // CORES, n // CORES)
        return chip * CORES + lax.rem(lax.rem(me, CORES) + flip, CORES)

    def own_copy(c, src, land):
        return pltpu.make_async_copy(src.at[pl.ds(me * rows, rows)], land.at[:, pl.ds(me * chunk, chunk)], own_sem.at[c])

    def push(c, src, land, i):
        peer = partner(i)
        return pltpu.make_async_remote_copy(
            src_ref=src.at[pl.ds(peer * rows, rows)],
            dst_ref=land.at[:, pl.ds(me * chunk, chunk)],
            send_sem=send_sem.at[c, i], recv_sem=recv_sem.at[c, me],
            device_id=(group_id, peer), device_id_type=MESH)

    def arrival(c, land, source):
        return pltpu.make_async_remote_copy(
            src_ref=land.at[:, pl.ds(source * chunk, chunk)],
            dst_ref=land.at[:, pl.ds(source * chunk, chunk)],
            send_sem=send_sem.at[c, 0], recv_sem=recv_sem.at[c, source],
            device_id=(group_id, me), device_id_type=MESH)

    pl.semaphore_wait(barrier, n - 1)
    chips = n // CORES
    pairs = [(0, 1)]
    for d in range(1, (chips - 1) // 2 + 1):
        pairs += [(d, 0), (-d, 0), (d, 1), (-d, 1)]
    near = len(pairs)
    split = near - 2 * CORES
    if chips % 2 == 0:
        pairs += [(chips // 2, 0), (chips // 2, 1)]
    for c, src, land, peers in ((0, k_ref, k_land, range(near)), (1, v_ref, v_land, range(split)),
                                (0, k_ref, k_land, range(near, n - 1))):
        for i in peers:
            push(c, src, land, i).start()
    own_copy(0, k_ref, k_land).start()
    own_copy(1, v_ref, v_land).start()

    last = range(n - 1 - near)

    def stage_copy(f):
        return pltpu.make_async_copy(v_ref.at[pl.ds(partner(near + f) * rows, rows)], staged.at[f], stage_sem.at[f])

    def push_half(part, f):
        return pltpu.make_async_remote_copy(
            src_ref=packed.at[part, f], dst_ref=half_land.at[part, f],
            send_sem=half_send.at[part, f], recv_sem=half_recv.at[part, f],
            device_id=(group_id, partner(near + f)), device_id_type=MESH)

    for f in last:
        stage_copy(f).start()
    small = [pltpu.make_async_copy(src, dst, small_sem.at[i]) for i, (src, dst) in enumerate((
        (lens_hbm, lens_ref), (x_hbm, x_ref), (gain_hbm, gain_ref), (bq_hbm, bq_ref), (bk_hbm, bk_ref), (bv_hbm, bv_ref)))]
    for copy in small:
        copy.start()
    for b in range(RING):
        start_weights(b)
    for copy in small:
        copy.wait()

    x_wide = x_ref[...].astype(jnp.float32)
    mean_sq = jnp.mean(x_wide * x_wide, axis=-1, keepdims=True)
    normed = x_wide * lax.rsqrt(mean_sq + RMS_EPS) * gain_ref[...].astype(jnp.float32).reshape(1, depth)
    h_ref[...] = jnp.concatenate([normed, jnp.zeros((LHS_ROWS - rows, depth), jnp.float32)], axis=0).astype(jnp.bfloat16)
    acc[...] = jnp.zeros_like(acc)
    acc_kv[...] = jnp.zeros_like(acc_kv)

    def multiply(lhs, slot, out, tile_count):
        def tile(t, carry):
            cols = pl.ds(pl.multiple_of(t * TILE, TILE), TILE)
            out[:, cols] += jnp.dot(lhs, ring[slot, :, cols], preferred_element_type=jnp.float32)
            return carry
        lax.fori_loop(0, tile_count, tile, 0)

    def multiply_kv(b):
        base = (b % 2) * PACK
        out = (b // 2) * kv_width
        slot = b % RING
        def part(c, carry):
            lhs = h_ref[:, pl.ds(pl.multiple_of((base + c) * block, block), block)]
            for t in range(kv_width // TILE):
                cols = pl.ds(out + t * TILE, TILE)
                src = pl.ds(pl.multiple_of(c * kv_width + t * TILE, TILE), TILE)
                acc_kv[:, cols] += jnp.dot(lhs, ring[slot, :, src], preferred_element_type=jnp.float32)
            return carry
        lax.fori_loop(0, PACK, part, 0)

    half = kv_heads // 2
    tile_row = lax.broadcasted_iota(jnp.int32, (span // 2, kv_heads, head_dim), 1)
    for f in last:
        stage_copy(f).wait()
        for s in range(rows):
            pair = staged[f, s].astype(jnp.float32).reshape(span // 2, 2, kv_heads, head_dim)
            even, odd = pair[:, 0], pair[:, 1]
            for part, both in enumerate((jnp.where(tile_row < half, even, pltpu.roll(odd, half, 1)),
                                         jnp.where(tile_row < half, pltpu.roll(even, half, 1), odd))):
                packed[part, f, s] = both.reshape(chunk // 2, head_dim).astype(jnp.bfloat16)

    for b in range(4):
        wait_weights(b)
        multiply_kv(b)
        start_weights(b + RING)
    for b in range(4, 14):
        wait_weights(b)
        multiply(h_ref[:, pl.ds((b - 4) * block, block)], b % RING, acc, width // TILE)
        if b + RING < 14 + RING:
            start_weights(b + RING)

    for f in last:
        push_half(0, f).start()
    for i in range(split, near):
        push(1, v_ref, v_land, i).start()
    for f in last:
        push_half(1, f).start()

    lane = lax.broadcasted_iota(jnp.int32, (1, head_dim), 1)
    freq_idx = jnp.where(lane < half_dim, lane, lane - half_dim).astype(jnp.float32)
    inv_freq = jnp.exp(freq_idx * (-2.0 * math.log(ROPE_THETA) / head_dim))
    sign = jnp.where(lane < half_dim, -1.0, 1.0)
    q_bias = bq_ref[...].astype(jnp.float32).reshape(heads, head_dim)
    k_bias = bk_ref[...].astype(jnp.float32).reshape(kv_heads, head_dim)
    v_bias = bv_ref[...].astype(jnp.float32).reshape(kv_heads, head_dim)
    for s in range(rows):
        for j in range(heads):
            q_raw[s, pl.ds(j, 1), :] = acc[pl.ds(s, 1), j * head_dim:(j + 1) * head_dim]
        for j in range(kv_heads):
            k_raw[s, pl.ds(j, 1), :] = acc_kv[pl.ds(s, 1), j * head_dim:(j + 1) * head_dim]
            v_raw[s, pl.ds(j, 1), :] = acc_kv[pl.ds(s, 1), kv_width + j * head_dim:kv_width + (j + 1) * head_dim]
    for s in range(rows):
        angle = lens_ref[me * rows + s].astype(jnp.float32) * inv_freq
        cos_t = jnp.cos(angle)
        sin_t = jnp.sin(angle) * sign
        q_one = q_raw[s] + q_bias
        q_rot[s] = (q_one * cos_t + pltpu.roll(q_one, half_dim, 1) * sin_t).astype(jnp.bfloat16)
        k_one = k_raw[s] + k_bias
        k_raw[s] = (k_one * cos_t + pltpu.roll(k_one, half_dim, 1) * sin_t).astype(jnp.bfloat16).astype(jnp.float32)
        v_raw[s] = (v_raw[s] + v_bias).astype(jnp.bfloat16).astype(jnp.float32)

    row_idx = lax.broadcasted_iota(jnp.int32, (span, kv_heads, head_dim), 0)
    col = lax.broadcasted_iota(jnp.int32, (heads, chunk), 1)
    head = lax.broadcasted_iota(jnp.int32, (heads, chunk), 0)
    own_head = (col % kv_heads) == (head // group)
    col_slot = col // kv_heads
    scale = head_dim ** -0.5

    def settle(land, s, source, fresh):
        place = pl.ds(pl.multiple_of(source * chunk, chunk), chunk)
        limit = lens_ref[me * rows + s] - source * span
        old = land[s, place, :].astype(jnp.float32).reshape(span, kv_heads, head_dim)
        kept = jnp.where(row_idx < limit, old, jnp.where(row_idx == limit, fresh[s][None], 0.0))
        kept = kept.reshape(chunk, head_dim).astype(jnp.bfloat16)
        land[s, place, :] = kept
        return kept, place, limit

    def lane_fold(op, values):
        out = values[:, :head_dim]
        for t in range(1, chunk // head_dim):
            out = op(out, values[:, t * head_dim:(t + 1) * head_dim])
        return out

    def score_chunk(source):
        for s in range(rows):
            keys, place, limit = settle(k_land, s, source, k_raw)
            sc = lax.dot_general(q_rot[s], keys, (((1,), (1,)), ((), ())), preferred_element_type=jnp.float32) * scale
            sc = jnp.where(own_head & (col_slot <= limit), sc, MASKED)
            scores[s, :, place] = sc
            m_acc[s] = jnp.maximum(m_acc[s], lane_fold(jnp.maximum, sc))

    head_row = lax.broadcasted_iota(jnp.int32, (span, kv_heads, head_dim), 1)

    def settle_half(s, f, source, part):
        place = pl.ds(pl.multiple_of(source * chunk, chunk), chunk)
        limit = lens_ref[me * rows + s] - source * span
        both = half_land[part, f, s].astype(jnp.float32).reshape(span // 2, kv_heads, head_dim)
        turned = pltpu.roll(both, half, 1)
        even, odd = (both, turned) if part == 0 else (turned, both)
        old = jnp.stack([even, odd], axis=1).reshape(span, kv_heads, head_dim)
        kept = jnp.where(row_idx < limit, old, jnp.where(row_idx == limit, v_raw[s][None], 0.0))
        mine = head_row < half if part == 0 else head_row >= half
        kept = jnp.where(mine, kept, 0.0)
        full = kept
        if part:
            full = jnp.where(mine, kept, v_land[s, place, :].astype(jnp.float32).reshape(span, kv_heads, head_dim))
        v_land[s, place, :] = full.reshape(chunk, head_dim).astype(jnp.bfloat16)
        return kept.reshape(chunk, head_dim).astype(jnp.bfloat16), place

    def weigh(s, place, vals, count):
        e = jnp.exp(scores[s, :, place] - m_acc[s][:, :1])
        if count:
            l_acc[s] += lane_fold(jnp.add, e)
        o_acc[s] += jnp.dot(e.astype(jnp.bfloat16), vals, preferred_element_type=jnp.float32)

    def value_chunk(source):
        for s in range(rows):
            vals, place, _ = settle(v_land, s, source, v_raw)
            weigh(s, place, vals, True)

    def value_half(part):
        for f in last:
            push_half(part, f).wait_recv()
            for s in range(rows):
                vals, place = settle_half(s, f, partner(near + f), part)
                weigh(s, place, vals, part == 0)

    def finish_heads(part):
        start, stop = part * heads // 2, (part + 1) * heads // 2
        for s in range(rows):
            l_all = jnp.sum(l_acc[s, pl.ds(start, stop - start), :], axis=-1, keepdims=True)
            q_raw[s, pl.ds(start, stop - start), :] = o_acc[s, pl.ds(start, stop - start), :] / l_all
            for j in range(start, stop):
                o_row[pl.ds(s, 1), j * head_dim:(j + 1) * head_dim] = q_raw[s, pl.ds(j, 1), :]
        cols = slice(start * head_dim, stop * head_dim)
        o_ref[:, cols] = o_row[:, cols].astype(jnp.bfloat16)

    m_acc[...] = jnp.full_like(m_acc, MASKED)
    l_acc[...] = jnp.zeros_like(l_acc)
    o_acc[...] = jnp.zeros_like(o_acc)

    own_copy(0, k_ref, k_land).wait()
    score_chunk(me)
    for i in range(n - 1):
        source = partner(i)
        arrival(0, k_land, source).wait_recv()
        score_chunk(source)
    for s in range(rows):
        m_acc[s] = jnp.broadcast_to(jnp.max(m_acc[s], axis=-1, keepdims=True), (heads, head_dim))
    own_copy(1, v_ref, v_land).wait()
    value_chunk(me)
    for i in range(near):
        source = partner(i)
        arrival(1, v_land, source).wait_recv()
        value_chunk(source)
    o_row[...] = jnp.zeros_like(o_row)
    y_part[...] = jnp.zeros_like(y_part)
    value_half(0)
    finish_heads(0)
    for r in range(depth // block // 2):
        wait_weights(14 + r)
        multiply_block(o_ref, r, ring.at[(14 + r) % RING], y_part)
        if 14 + r + RING < 24:
            start_weights(14 + r + RING)
    value_half(1)
    finish_heads(1)
    for r in range(depth // block // 2, depth // block):
        wait_weights(14 + r)
    for c, (src, land) in enumerate(((k_ref, k_land), (v_ref, v_land))):
        for i in range(n - 1 if c == 0 else near):
            push(c, src, land, i).wait_send()
    for part in range(2):
        for f in last:
            push_half(part, f).wait_send()


def output_kernel(first, start, o_ref, k_land, v_land, ring, y_part, x_hbm, y_ref, k_out, v_out, x_ref, acc, sem):
    rows, depth = x_ref.shape
    block = ring.shape[1]
    copies = [pltpu.make_async_copy(k_land, k_out, sem.at[0]),
              pltpu.make_async_copy(v_land, v_out, sem.at[1]),
              pltpu.make_async_copy(x_hbm, x_ref, sem.at[2])]
    for copy in copies:
        copy.start()
    acc[...] = y_part[...]
    for r in range(start, depth // block):
        multiply_block(o_ref, r, ring.at[(first + r) % ring.shape[0]], acc)
    for copy in copies:
        copy.wait()
    y_ref[...] = (x_ref[...].astype(jnp.float32) + acc[:rows, :]).astype(jnp.bfloat16)


def solution(mesh):
    batch_spec = P(('dp', 'cp'))
    seq_spec = P('dp', 'cp')
    whole = P()
    n = mesh.shape['cp']

    def per_device(x_tok, prompt_lens, k_cache, v_cache, norm_gain, w_q, b_q, w_k, b_k, w_v, b_v, w_o):
        rows, depth = x_tok.shape
        batch, span, kv_heads, head_dim = k_cache.shape
        width = w_q.shape[1]
        heads = width // head_dim
        chunk = span * kv_heads
        kv_width = kv_heads * head_dim
        block = depth // 10
        dims = (n, rows, span, kv_heads, head_dim, heads)
        vmem = pl.BlockSpec(memory_space=pltpu.VMEM)
        smem = pl.BlockSpec(memory_space=pltpu.SMEM)
        hbm = pl.BlockSpec(memory_space=pl.ANY)
        bf16, f32 = jnp.bfloat16, jnp.float32
        land = (rows, n * chunk, head_dim)
        o_rows, k_all, v_all, ring, y_part = pl.pallas_call(
            functools.partial(exchange_kernel, dims),
            out_shape=(pltpu.VMEM((LHS_ROWS, width), bf16), pltpu.VMEM(land, bf16), pltpu.VMEM(land, bf16),
                       pltpu.VMEM((RING, block, width), bf16), pltpu.VMEM((LHS_ROWS, depth), f32)),
            in_specs=[hbm] * 12,
            out_specs=(vmem,) * 5,
            scratch_shapes=[
                pltpu.SMEM((batch,), jnp.int32),
                pltpu.VMEM((rows, depth), bf16),
                pltpu.VMEM((depth,), bf16),
                pltpu.VMEM((width,), bf16),
                pltpu.VMEM((kv_width,), bf16),
                pltpu.VMEM((kv_width,), bf16),
                pltpu.VMEM((rows, heads, n * chunk), f32),
                pltpu.VMEM((LHS_ROWS, depth), bf16),
                pltpu.VMEM((LHS_ROWS, width), f32),
                pltpu.VMEM((LHS_ROWS, 2 * kv_width), f32),
                pltpu.VMEM((rows, heads, head_dim), f32),
                pltpu.VMEM((rows, heads, head_dim), bf16),
                pltpu.VMEM((rows, kv_heads, head_dim), f32),
                pltpu.VMEM((rows, kv_heads, head_dim), f32),
                pltpu.VMEM((rows, heads, head_dim), f32),
                pltpu.VMEM((rows, heads, head_dim), f32),
                pltpu.VMEM((rows, heads, head_dim), f32),
                pltpu.VMEM((LHS_ROWS, width), f32),
                pltpu.VMEM((CORES, rows, chunk, head_dim), bf16),
                pltpu.VMEM((2, CORES, rows, chunk // 2, head_dim), bf16),
                pltpu.VMEM((2, CORES, rows, chunk // 2, head_dim), bf16),
                pltpu.SemaphoreType.DMA((6,)),
                pltpu.SemaphoreType.DMA((RING, PACK)),
                pltpu.SemaphoreType.DMA((2,)),
                pltpu.SemaphoreType.DMA((2, n)),
                pltpu.SemaphoreType.DMA((2, n)),
                pltpu.SemaphoreType.DMA((CORES,)),
                pltpu.SemaphoreType.DMA((2, CORES)),
                pltpu.SemaphoreType.DMA((2, CORES)),
            ],
            compiler_params=pltpu.CompilerParams(collective_id=0, has_side_effects=True, vmem_limit_bytes=8 * 1024 * 1024),
            cost_estimate=pl.CostEstimate(flops=1 << 30, bytes_accessed=1 << 27, transcendentals=0),
        )(prompt_lens, x_tok, norm_gain, b_q, b_k, b_v,
          k_cache.reshape(batch, chunk, head_dim), v_cache.reshape(batch, chunk, head_dim), w_q, w_k, w_v, w_o)
        y, k_out, v_out = pl.pallas_call(
            functools.partial(output_kernel, 14, depth // block // 2),
            out_shape=(jax.ShapeDtypeStruct((rows, depth), bf16), jax.ShapeDtypeStruct(land, bf16), jax.ShapeDtypeStruct(land, bf16)),
            in_specs=[vmem] * 5 + [hbm],
            out_specs=(vmem, hbm, hbm),
            scratch_shapes=[
                pltpu.VMEM((rows, depth), bf16),
                pltpu.VMEM((LHS_ROWS, depth), f32),
                pltpu.SemaphoreType.DMA((3,)),
            ],
            compiler_params=pltpu.CompilerParams(vmem_limit_bytes=8 * 1024 * 1024),
            cost_estimate=pl.CostEstimate(flops=1 << 30, bytes_accessed=1 << 25, transcendentals=0),
        )(*[pltpu.with_memory_space_constraint(a, pltpu.VMEM) for a in (o_rows, k_all, v_all, ring, y_part)], x_tok)
        shape = (rows, n * span, kv_heads, head_dim)
        return y, k_out.reshape(shape), v_out.reshape(shape)

    return jax.shard_map(per_device, mesh=mesh, in_specs=(batch_spec, P('dp'), seq_spec, seq_spec, whole, whole, whole, whole, whole, whole, whole, whole), out_specs=(batch_spec, batch_spec, batch_spec), check_vma=False)
```
